256 devices in a mesh: gx: 16 (over y_hi, z), gy: 16 (over x, y_lo, core).
Axes of the slice: x: 4, y: 4 (y_hi: 2, y_lo: 2; y = y_hi * 2 + y_lo), z: 8, core: 2. Of those that a mesh axis runs over, the one named last changes fastest.
Arguments:
- charge_density: float32 [256, 256, 256], P('gx', 'gy'), may hold values from -5080 to 5140
Outputs:
- potential: float32 [256, 256, 256], P('gx', 'gy')
- energies: float32 [2], replicated
The draws below stay inside these ranges and needn't reach their ends.
All inputs are finite; a program needn't handle non-finite values.
Results may differ from the reference program's by a relative error of at most 0.0003.
Values sent between devices are 32-bit elements.
A program may use at most 128 MiB of HBM per device.

```python
import math
import jax
import jax.numpy as jnp
import numpy as np
from jax import lax

N = 256
ORDER = 16


def draw_charge_density(key, part):
    level_key, noise_key = jax.random.split(jax.random.fold_in(key, 11))
    bound = float((N + 1) * (N + 1) // 13)
    levels = jax.random.uniform(level_key, (8, 8, 8), jnp.float32, minval=0.0, maxval=60.0)
    noise = jax.random.uniform(noise_key, (N, N, N), jnp.float32, minval=-bound, maxval=bound)
    block = N // 8
    coarse = jnp.repeat(jnp.repeat(jnp.repeat(levels, block, 0), block, 1), block, 2)
    return (coarse + noise).astype(jnp.float32)


def setup_inputs(seed: int = 0) -> dict:
    key_of = jax.random.split(jax.random.key(seed), 2)
    return {
        "charge_density": draw_charge_density(jax.random.fold_in(key_of[1], 71), 0),
    }


exact_mode = lax.Precision.HIGHEST
outer_ratio = 1.1
radius_scale = math.sqrt(3.0) / 2.0

def sine_table(length):
    counter = jnp.arange(length, dtype=jnp.int32) + 1
    product = counter[:, None] * counter[None, :] % (2 * (length + 1))
    return jnp.sin(math.pi * product.astype(jnp.float32) / (length + 1))

def eigen_line(counter, length):
    half_angle = math.pi * (counter + 1).astype(jnp.float32) / (2.0 * (length + 1))
    return 4.0 * float((length + 1) * (length + 1)) * jnp.sin(half_angle) ** 2

def recurrence_tables():
    degree_count = ORDER + 1
    near_coeff = np.zeros((degree_count, degree_count, 1), np.float32)
    far_coeff = np.zeros((degree_count, degree_count, 1), np.float32)
    sector = np.ones(degree_count, np.float32)
    for degree in range(1, degree_count):
        for azimuth in range(degree):
            divisor = math.sqrt(degree * degree - azimuth * azimuth)
            near_coeff[degree, azimuth, 0] = (2 * degree - 1) / divisor
            far_coeff[degree, azimuth, 0] = math.sqrt((degree - 1) * (degree - 1) - azimuth * azimuth) / divisor
        if degree >= 2:
            sector[degree] = math.sqrt((2 * degree - 1) / (2.0 * degree))
    return (near_coeff, far_coeff, sector)

def expansion_weights():
    degree_count = ORDER + 1
    weights = np.zeros((degree_count, degree_count), np.float32)
    for degree in range(degree_count):
        for azimuth in range(degree + 1):
            factor = 1.0 if azimuth == 0 else 2.0
            weights[degree, azimuth] = factor / (4.0 * math.pi * radius_scale * outer_ratio ** (degree + 1))
    return weights

def harmonic_sweep(unit_x, unit_y, unit_z, visitor, running):
    near_coeff, far_coeff, sector = recurrence_tables()
    degree_count = ORDER + 1
    selector = np.eye(degree_count, dtype=np.float32)[:, :, None]
    empty_rows = jnp.zeros((degree_count,) + unit_x.shape, unit_x.dtype)
    sector_cosine = jnp.ones_like(unit_x)
    sector_sine = jnp.zeros_like(unit_x)
    cosine_prev, sine_prev, cosine_old, sine_old = (empty_rows, empty_rows, empty_rows, empty_rows)
    for degree in range(degree_count):
        if degree > 0:
            sector_cosine, sector_sine = (sector[degree] * (unit_x * sector_cosine - unit_y * sector_sine), sector[degree] * (unit_x * sector_sine + unit_y * sector_cosine))
        cosine_now = near_coeff[degree] * unit_z * cosine_prev - far_coeff[degree] * cosine_old + selector[degree] * sector_cosine
        sine_now = near_coeff[degree] * unit_z * sine_prev - far_coeff[degree] * sine_old + selector[degree] * sector_sine
        running = visitor(running, degree, cosine_now, sine_now)
        cosine_old, sine_old = (cosine_prev, sine_prev)
        cosine_prev, sine_prev = (cosine_now, sine_now)
    return running

def face_moments(point_x, point_y, point_z, charge):
    radius = jnp.sqrt(point_x * point_x + point_y * point_y + point_z * point_z)
    scaled_radius = radius / radius_scale

    def visitor(running, degree, cosine_now, sine_now):
        weight, moment_cosine, moment_sine, facing_cosine, facing_sine = running
        moment_cosine = moment_cosine + [jnp.dot(cosine_now, weight, precision=exact_mode)]
        moment_sine = moment_sine + [jnp.dot(sine_now, weight, precision=exact_mode)]
        facing_cosine = facing_cosine + [jnp.dot(cosine_now, charge, precision=exact_mode)]
        facing_sine = facing_sine + [jnp.dot(sine_now, charge, precision=exact_mode)]
        return (weight * scaled_radius, moment_cosine, moment_sine, facing_cosine, facing_sine)
    result = harmonic_sweep(point_x / radius, point_y / radius, point_z / radius, visitor, (charge, [], [], [], []))
    return tuple((jnp.stack(listing) for listing in result[1:]))

def face_potential(point_x, point_y, point_z, weight_cosine, weight_sine):
    radius = jnp.sqrt(point_x * point_x + point_y * point_y + point_z * point_z)

    def visitor(accum, degree, cosine_now, sine_now):
        accum = accum + jnp.dot(weight_cosine[degree], cosine_now, precision=exact_mode)
        return accum + jnp.dot(weight_sine[degree], sine_now, precision=exact_mode)
    return harmonic_sweep(point_x / radius, point_y / radius, point_z / radius, visitor, jnp.zeros_like(point_x))

def transform(volume, sine_rows):
    volume = jnp.einsum('abc,ck->abk', volume, sine_rows, precision=exact_mode)
    volume = jnp.einsum('abk,bj->ajk', volume, sine_rows, precision=exact_mode)
    return jnp.einsum('ajk,ai->ijk', volume, sine_rows, precision=exact_mode)

def poisson_solve(volume, sine_rows, denominator):
    return transform(transform(volume, sine_rows) / denominator, sine_rows)

def reference(charge_density):
    length = N
    spacing = 1.0 / (length + 1)
    sine_rows = sine_table(length)
    eigen_rows = eigen_line(jnp.arange(length, dtype=jnp.int32), length)
    denominator = (eigen_rows[:, None, None] + eigen_rows[None, :, None] + eigen_rows[None, None, :]) * ((length + 1) / 2.0) ** 3
    first_field = poisson_solve(charge_density, sine_rows, denominator)
    coords = (jnp.arange(length, dtype=jnp.float32) - (length - 1) / 2.0) * spacing
    grid_rows = jnp.broadcast_to(coords[:, None], (length, length)).reshape(-1)
    grid_columns = jnp.broadcast_to(coords[None, :], (length, length)).reshape(-1)
    plane_half = jnp.full((length * length,), 0.5, jnp.float32)
    boundary_faces = [(grid_rows, grid_columns, -plane_half, first_field[:, :, 0]), (grid_rows, grid_columns, plane_half, first_field[:, :, -1]), (-plane_half, grid_rows, grid_columns, first_field[0]), (plane_half, grid_rows, grid_columns, first_field[-1]), (grid_rows, -plane_half, grid_columns, first_field[:, 0]), (grid_rows, plane_half, grid_columns, first_field[:, -1])]
    totals = None
    for point_x, point_y, point_z, near_cells in boundary_faces:
        face_terms = face_moments(point_x, point_y, point_z, spacing * near_cells.reshape(-1))
        if totals is None:
            totals = face_terms
        else:
            totals = tuple((earlier + later for earlier, later in zip(totals, face_terms)))
    weights = expansion_weights()
    weight_cosine = weights * totals[0]
    weight_sine = weights * totals[1]
    potentials = []
    for point_x, point_y, point_z, near_cells in boundary_faces:
        potentials.append(face_potential(point_x, point_y, point_z, weight_cosine, weight_sine).reshape(length, length) / spacing ** 2)
    source = charge_density
    source = source.at[:, :, 0].add(potentials[0])
    source = source.at[:, :, -1].add(potentials[1])
    source = source.at[0].add(potentials[2])
    source = source.at[-1].add(potentials[3])
    source = source.at[:, 0].add(potentials[4])
    source = source.at[:, -1].add(potentials[5])
    potential = poisson_solve(source, sine_rows, denominator)
    energies = spacing ** 3 * jnp.stack([jnp.sum(charge_density * first_field), jnp.sum(charge_density * potential)])
    return (potential, energies)
```

```python
import math

import jax
import jax.numpy as jnp
import numpy as np
from jax import lax
from jax.sharding import PartitionSpec as P

ORDER = 16
N = 256
SLOTS = 48
LANES = 1024
SPARE = 7 * 128 + 112
ENERGY_LANE = 1023


def harmonics(x, y, z):
    cosine = {(0, 0): np.ones_like(x)}
    sine = {(0, 0): np.zeros_like(x)}
    for l in range(1, ORDER + 1):
        scale = 1.0 if l == 1 else math.sqrt((2 * l - 1) / (2.0 * l))
        c, s = cosine[l - 1, l - 1], sine[l - 1, l - 1]
        cosine[l, l] = scale * (x * c - y * s)
        sine[l, l] = scale * (x * s + y * c)
        for m in range(l):
            near = (2 * l - 1) / math.sqrt(l * l - m * m)
            far = math.sqrt((l - 1) ** 2 - m * m) / math.sqrt(l * l - m * m)
            for table in (cosine, sine):
                older = table[l - 2, m] if l - 2 >= m else 0.0
                table[l, m] = near * z * table[l - 1, m] - far * older
    return cosine, sine


def face_point(face, t, s):
    one = np.ones_like(t)
    return ((t, s, one), (one, s, t), (t, one, s))[face]


def face_parity(face, px, py, pz):
    return ((px, py, pz), (pz, py, px), (px, pz, py))[face]


def trig(parity, odd, angle):
    if odd:
        orders = np.arange(1, 16, 2)
    else:
        orders = np.arange(0, 17, 2) if parity == 0 else np.arange(2, 17, 2)
    wave = np.cos if parity == 0 else np.sin
    return wave(orders[:, None] * angle[None, :])


def build_tables():
    span = N + 1.0
    step = 1.0 / span
    radius = math.sqrt(3.0) / 2.0
    index = np.arange(N) + 1
    sine_rows = np.sin(np.pi * (index[:, None] * index[None, :] % (2 * N + 2)) / span)
    eigen = 4.0 * span * span * np.sin(np.pi * index / (2 * span)) ** 2
    scaled = 2.0 * (np.arange(N) - (N - 1) / 2.0) * step
    angle = np.arctan(scaled)

    terms = [[] for _ in range(8)]
    for l in range(ORDER + 1):
        for m in range(l + 1):
            terms[(m % 2) * 4 + (l - m) % 2].append((l, m, 0))
            if m:
                terms[((m - 1) % 2) * 4 + 2 + (l - m) % 2].append((l, m, 1))

    nodes, quad = np.polynomial.legendre.leggauss(24)
    legendre = np.polynomial.legendre.legvander(nodes, ORDER).T
    basis = np.zeros((N, 32))
    basis[:, : ORDER + 1] = sine_rows @ np.polynomial.legendre.legvander(scaled, ORDER)
    even = (np.arange(N) % 2 == 0).astype(np.float64)
    basis[:, 17] = sine_rows[0] * even
    basis[:, 18] = sine_rows[0] * (1.0 - even)
    project = legendre * quad[None, :] * (np.arange(ORDER + 1) + 0.5)[:, None]
    turns = 64
    circle = 2.0 * np.pi * np.arange(turns) / turns
    ones_t, ones_s = np.meshgrid(nodes, nodes, indexing="ij")
    alpha, beta = np.meshgrid(circle, circle, indexing="ij")
    solid, wave = [], []
    for face in range(3):
        x, y, z = face_point(face, ones_t, ones_s)
        r = np.sqrt(x * x + y * y + z * z)
        table = harmonics(x / r, y / r, z / r)
        solid.append((table, r / math.sqrt(3.0)))
        ca, sa, cb, sb = np.cos(alpha), np.sin(alpha), np.cos(beta), np.sin(beta)
        parts = (sa * cb, ca * sb, ca * cb)
        x, y, z = (parts, (parts[2], parts[1], parts[0]), (parts[0], parts[2], parts[1]))[face]
        r = np.sqrt(x * x + y * y + z * z)
        safe = np.where(r < 1e-12, 1.0, r)
        wave.append((harmonics(x / safe, y / safe, z / safe), np.where(r < 1e-12, 0.0, r)))

    select = np.zeros((3, 32, LANES))
    gather = np.zeros((SLOTS, LANES))
    spread = np.zeros((SLOTS, 16, 256))
    columns = np.zeros((256, N))
    rows = np.zeros((8, 3, 16, N))
    spill = SPARE
    for group in range(8):
        px, py, pz = group >> 2 & 1, group >> 1 & 1, group & 1
        odd = (px + py + pz) % 2
        lane = group * 128
        for face in range(3):
            prow, pcol, normal = face_parity(face, px, py, pz)
            sign = 2.0 if normal == 0 else -2.0
            entries = [
                (i, j)
                for i in range(prow, ORDER + 1, 2)
                for j in range(pcol, ORDER + 1, 2)
                if i + j + normal <= ORDER - odd
            ]
            moments = {}
            for slot, (l, m, which) in enumerate(terms[group]):
                table, ratio = solid[face]
                values = ratio**l * table[which][l, m]
                moments[slot] = project @ values @ project.T
            for i, j in entries:
                if lane >= (group + 1) * 128 or (lane >= SPARE and group == 7):
                    position, spill = spill, spill + 1
                    assert group == 0
                else:
                    position, lane = lane, lane + 1
                axes = ((0, 1, 2), (2, 1, 0), (0, 2, 1))[face]
                select[axes[0], i, position] = 1.0
                select[axes[1], j, position] = 1.0
                select[axes[2], 17 + normal, position] = 1.0
                for slot in moments:
                    gather[slot, position] = step * sign * moments[slot][i, j]
            left = trig(prow, odd, circle)
            right = trig(pcol, odd, circle)
            left_unit = left / np.sum(left * left, axis=1, keepdims=True)
            right_unit = right / np.sum(right * right, axis=1, keepdims=True)
            base = group * 32 + face * 9
            for slot, (l, m, which) in enumerate(terms[group]):
                table, r = wave[face]
                values = r ** (ORDER - odd) * table[which][l, m]
                block = left_unit @ values @ right_unit.T
                weight = (1.0 if m == 0 else 2.0) / (4.0 * math.pi * radius * 1.1 ** (l + 1))
                block = block * weight * sign * span * span
                spread[slot, : block.shape[0], base : base + block.shape[1]] = block
            tail = trig(pcol, odd, angle)
            columns[base : base + tail.shape[0]] = tail
            head = trig(prow, odd, angle)
            rows[group, face, : head.shape[0]] = head
    assert spill < ENERGY_LANE
    root = 1.0 / np.sqrt(1.0 - np.outer(np.sin(angle) ** 2, np.sin(angle) ** 2))
    return sine_rows, eigen, basis, select, gather, spread, columns, rows, root, root**15


mode = lax.Precision.HIGH


def transform_forward(volume, sine_rows, swap_one, swap_two):
    cells_a, cells_b, length = volume.shape
    spectrum = jnp.einsum("abz,zk->kab", volume, sine_rows, precision=mode)
    spectrum = swap_one(spectrum.reshape(length, cells_a * cells_b))
    groups = spectrum.shape[1] // (cells_a * cells_b)
    pieces = spectrum.reshape(spectrum.shape[0], groups, cells_a, cells_b)
    table = sine_rows.reshape(groups, cells_a, length)
    spectrum = jnp.einsum("zpab,paj->jzb", pieces, table, precision=mode)
    depth = spectrum.shape[1]
    spectrum = swap_two(spectrum.reshape(length, depth * cells_b))
    groups = spectrum.shape[1] // (depth * cells_b)
    pieces = spectrum.reshape(spectrum.shape[0], groups, depth, cells_b)
    table = sine_rows.reshape(groups, cells_b, length)
    return jnp.einsum("kqzc,qcj->kzj", pieces, table, precision=mode)


def transform_inverse(spectrum, sine_rows, back_two, back_one, cells_a, cells_b):
    rows_one, depth, length = spectrum.shape
    table = sine_rows.reshape(length, length // cells_b, cells_b)
    pieces = jnp.einsum("kzj,jqc->kqzc", spectrum, table, precision=mode)
    pieces = back_two(pieces.reshape(rows_one, (length // cells_b) * depth * cells_b))
    pieces = pieces.reshape(length, depth, cells_b)
    table = sine_rows.reshape(length, length // cells_a, cells_a)
    volume = jnp.einsum("jzb,jpa->zpab", pieces, table, precision=mode)
    volume = back_one(volume.reshape(depth, (length // cells_a) * cells_a * cells_b))
    volume = volume.reshape(length, cells_a, cells_b)
    return jnp.einsum("kab,kz->abz", volume, sine_rows, precision=mode)


def total_over(values, axis):
    return jnp.sum(lax.all_gather(values, axis), axis=0)


def shards(charge_density):
    cells_a, cells_b, length = charge_density.shape
    tables = [jnp.asarray(table, jnp.float32) for table in build_tables()]
    sine_rows, eigen, basis, select, gather, spread, columns, rows, root, power = tables
    exact = lax.Precision.HIGHEST
    index_x = lax.axis_index("gx")
    index_y = lax.axis_index("gy")

    def swap_one(operand):
        return lax.all_to_all(operand, "gx", split_axis=0, concat_axis=1, tiled=True)

    def swap_two(operand):
        return lax.all_to_all(operand, "gy", split_axis=0, concat_axis=1, tiled=True)

    def back_two(operand):
        return lax.all_to_all(operand, "gy", split_axis=1, concat_axis=0, tiled=True)

    def back_one(operand):
        return lax.all_to_all(operand, "gx", split_axis=1, concat_axis=0, tiled=True)

    count_x = length // lax.axis_size("gy")
    count_z = length // lax.axis_size("gx")
    start_x = index_y * count_x
    start_z = index_x * count_z
    eigen_x = lax.dynamic_slice_in_dim(eigen, start_x, count_x)
    eigen_z = lax.dynamic_slice_in_dim(eigen, start_z, count_z)
    denominator = (
        eigen_x[:, None, None] + eigen_z[None, :, None] + eigen[None, None, :]
    ) * ((length + 1) / 2.0) ** 3
    charge = transform_forward(charge_density, sine_rows, swap_one, swap_two)
    field = charge / denominator

    basis_x = lax.dynamic_slice_in_dim(basis, start_x, count_x)
    basis_z = lax.dynamic_slice_in_dim(basis, start_z, count_z)
    expand_x = jnp.dot(basis_x, select[0], precision=exact)
    expand_y = jnp.dot(basis, select[1], precision=exact)
    expand_z = jnp.dot(basis_z, select[2], precision=exact)
    mixed = jnp.einsum("xzy,ye->xze", field, expand_y, precision=mode)
    entries = jnp.sum(jnp.sum(mixed * expand_z[None], axis=1) * expand_x, axis=0)
    entries = entries.at[ENERGY_LANE].set(jnp.sum(charge * field))
    entries = total_over(total_over(entries, "gx"), "gy")

    owner = np.arange(LANES) // 128
    owner[SPARE:ENERGY_LANE] = 0
    onehot = jnp.asarray(owner[:, None] == np.arange(256)[None, :] // 32, jnp.float32)
    moments = jnp.dot(gather * entries, onehot, precision=exact)
    shape = jnp.sum(moments[:, None, :] * spread, axis=0)

    source = 0.0
    parity = np.arange(length) % 2
    edge = [jnp.where(parity == normal, sine_rows[0], 0.0) for normal in range(2)]
    slab_x = lax.dynamic_slice_in_dim(sine_rows, start_x, count_x)
    slab_z = lax.dynamic_slice_in_dim(sine_rows, start_z, count_z)
    for normal in range(2):
        edge_x = lax.dynamic_slice_in_dim(edge[normal], start_x, count_x)
        edge_z = lax.dynamic_slice_in_dim(edge[normal], start_z, count_z)
        for face in range(3):
            parts = [0.0, 0.0]
            for group in range(8):
                bits = (group >> 2 & 1, group >> 1 & 1, group & 1)
                if face_parity(face, *bits)[2] != normal:
                    continue
                base = group * 32 + face * 9
                right = jnp.dot(shape[:, base : base + 9], columns[base : base + 9], precision=exact)
                parts[sum(bits) % 2] += jnp.dot(rows[group, face].T, right, precision=exact)
            plane = power * (root * parts[0] + parts[1])
            left = (slab_x, slab_z, slab_x)[face]
            half = jnp.dot(left, plane, precision=mode)
            if face == 0:
                full = jnp.dot(half, sine_rows, precision=mode)
                source += full[:, None, :] * edge_z[None, :, None]
            elif face == 1:
                full = jnp.dot(half, sine_rows, precision=mode)
                source += full[None, :, :] * edge_x[:, None, None]
            else:
                full = jnp.dot(half, slab_z.T, precision=mode)
                source += full[:, :, None] * edge[normal][None, None, :]
    total = field + source / denominator
    potential = transform_inverse(total, sine_rows, back_two, back_one, cells_a, cells_b)
    second = total_over(total_over(jnp.sum(charge * total), "gx"), "gy")
    spacing = 1.0 / (length + 1)
    scale = spacing**3
    energies = jnp.stack([scale * entries[ENERGY_LANE], scale * second])
    return potential, energies


def solution(mesh):
    return jax.shard_map(
        shards,
        mesh=mesh,
        in_specs=(P("gx", "gy", None),),
        out_specs=(P("gx", "gy", None), P()),
        check_vma=False,
    )
```

```python
import math

import jax
import jax.numpy as jnp
import numpy as np
from jax import lax
from jax.experimental import pallas as pl
from jax.experimental.pallas import tpu as pltpu
from jax.sharding import PartitionSpec as P

ORDER = 16
N = 256
SLOTS = 48
LANES = 1024
SPARE = 7 * 128 + 112
ENERGY_LANE = 1023


def harmonics(x, y, z):
    cosine = {(0, 0): np.ones_like(x)}
    sine = {(0, 0): np.zeros_like(x)}
    for l in range(1, ORDER + 1):
        scale = 1.0 if l == 1 else math.sqrt((2 * l - 1) / (2.0 * l))
        c, s = cosine[l - 1, l - 1], sine[l - 1, l - 1]
        cosine[l, l] = scale * (x * c - y * s)
        sine[l, l] = scale * (x * s + y * c)
        for m in range(l):
            near = (2 * l - 1) / math.sqrt(l * l - m * m)
            far = math.sqrt((l - 1) ** 2 - m * m) / math.sqrt(l * l - m * m)
            for table in (cosine, sine):
                older = table[l - 2, m] if l - 2 >= m else 0.0
                table[l, m] = near * z * table[l - 1, m] - far * older
    return cosine, sine


def face_point(face, t, s):
    one = np.ones_like(t)
    return ((s, t, one), (s, one, t), (one, t, s))[face]


def face_parity(face, px, py, pz):
    return ((py, px, pz), (pz, px, py), (py, pz, px))[face]


def trig(parity, odd, angle):
    if odd:
        orders = np.arange(1, 16, 2)
    else:
        orders = np.arange(0, 17, 2) if parity == 0 else np.arange(2, 17, 2)
    wave = np.cos if parity == 0 else np.sin
    return wave(orders[:, None] * angle[None, :])


def build_tables():
    span = N + 1.0
    step = 1.0 / span
    radius = math.sqrt(3.0) / 2.0
    index = np.arange(N) + 1
    sine_rows = np.sin(np.pi * (index[:, None] * index[None, :] % (2 * N + 2)) / span)
    eigen = 4.0 * span * span * np.sin(np.pi * index / (2 * span)) ** 2
    scaled = 2.0 * (np.arange(N) - (N - 1) / 2.0) * step
    angle = np.arctan(scaled)

    terms = [[] for _ in range(8)]
    for l in range(ORDER + 1):
        for m in range(l + 1):
            terms[(m % 2) * 4 + (l - m) % 2].append((l, m, 0))
            if m:
                terms[((m - 1) % 2) * 4 + 2 + (l - m) % 2].append((l, m, 1))

    nodes, quad = np.polynomial.legendre.leggauss(24)
    legendre = np.polynomial.legendre.legvander(nodes, ORDER).T
    basis = np.zeros((N, 32))
    basis[:, : ORDER + 1] = sine_rows @ np.polynomial.legendre.legvander(scaled, ORDER)
    even = (np.arange(N) % 2 == 0).astype(np.float64)
    basis[:, 17] = sine_rows[0] * even
    basis[:, 18] = sine_rows[0] * (1.0 - even)
    project = legendre * quad[None, :] * (np.arange(ORDER + 1) + 0.5)[:, None]
    turns = 64
    circle = 2.0 * np.pi * np.arange(turns) / turns
    ones_t, ones_s = np.meshgrid(nodes, nodes, indexing="ij")
    alpha, beta = np.meshgrid(circle, circle, indexing="ij")
    solid, wave = [], []
    for face in range(3):
        x, y, z = face_point(face, ones_t, ones_s)
        r = np.sqrt(x * x + y * y + z * z)
        table = harmonics(x / r, y / r, z / r)
        solid.append((table, r / math.sqrt(3.0)))
        ca, sa, cb, sb = np.cos(alpha), np.sin(alpha), np.cos(beta), np.sin(beta)
        parts = (sa * cb, ca * sb, ca * cb)
        order = ((1, 0, 2), (1, 2, 0), (2, 0, 1))[face]
        x, y, z = (parts[k] for k in order)
        r = np.sqrt(x * x + y * y + z * z)
        safe = np.where(r < 1e-12, 1.0, r)
        wave.append((harmonics(x / safe, y / safe, z / safe), np.where(r < 1e-12, 0.0, r)))

    select = np.zeros((3, 32, LANES))
    gather = np.zeros((SLOTS, LANES))
    spread = np.zeros((SLOTS, 16, 256))
    columns = np.zeros((256, N))
    rows = np.zeros((8, 3, 16, N))
    spill = SPARE
    for group in range(8):
        px, py, pz = group >> 2 & 1, group >> 1 & 1, group & 1
        odd = (px + py + pz) % 2
        lane = group * 128
        for face in range(3):
            prow, pcol, normal = face_parity(face, px, py, pz)
            sign = 2.0 if normal == 0 else -2.0
            entries = [
                (i, j)
                for i in range(prow, ORDER + 1, 2)
                for j in range(pcol, ORDER + 1, 2)
                if i + j + normal <= ORDER - odd
            ]
            moments = {}
            for slot, (l, m, which) in enumerate(terms[group]):
                table, ratio = solid[face]
                values = ratio**l * table[which][l, m]
                moments[slot] = project @ values @ project.T
            for i, j in entries:
                if lane >= (group + 1) * 128 or (lane >= SPARE and group == 7):
                    position, spill = spill, spill + 1
                    assert group == 0
                else:
                    position, lane = lane, lane + 1
                axes = ((1, 0, 2), (2, 0, 1), (1, 2, 0))[face]
                select[axes[0], i, position] = 1.0
                select[axes[1], j, position] = 1.0
                select[axes[2], 17 + normal, position] = 1.0
                for slot in moments:
                    gather[slot, position] = step * sign * moments[slot][i, j]
            left = trig(prow, odd, circle)
            right = trig(pcol, odd, circle)
            left_unit = left / np.sum(left * left, axis=1, keepdims=True)
            right_unit = right / np.sum(right * right, axis=1, keepdims=True)
            base = group * 32 + face * 9
            for slot, (l, m, which) in enumerate(terms[group]):
                table, r = wave[face]
                values = r ** (ORDER - odd) * table[which][l, m]
                block = left_unit @ values @ right_unit.T
                weight = (1.0 if m == 0 else 2.0) / (4.0 * math.pi * radius * 1.1 ** (l + 1))
                block = block * weight * sign * span * span
                spread[slot, : block.shape[0], base : base + block.shape[1]] = block
            tail = trig(pcol, odd, angle)
            columns[base : base + tail.shape[0]] = tail
            head = trig(prow, odd, angle)
            rows[group, face, : head.shape[0]] = head
    assert spill < ENERGY_LANE
    root = 1.0 / np.sqrt(1.0 - np.outer(np.sin(angle) ** 2, np.sin(angle) ** 2))
    return sine_rows, eigen, basis, select, gather, spread, columns, rows, root, root**15

MESH = pl.DeviceIdType.MESH
SIDE = 16
HALF = 128
F32 = jnp.float32
BF16 = jnp.bfloat16
NN = (((1,), (0,)), ((), ()))
NT = (((1,), (1,)), ((), ()))


def split(value):
    high = value.astype(BF16)
    return high, (value - high.astype(F32)).astype(BF16)


def dot(a, b, dims=NN):
    return lax.dot_general(a, b, dims, preferred_element_type=F32)


def dot3(a, b, dims=NN):
    return dot(a[0], b[0], dims) + (dot(a[0], b[1], dims) + dot(a[1], b[0], dims))


def regroup(load, store, roll):
    lane = lax.broadcasted_iota(jnp.int32, (4 * SIDE, HALF), 1)
    rows = [
        jnp.concatenate([load(8 * a + i, h) for a in range(2) for h in range(2)], axis=0)
        for i in range(8)
    ]
    for step in (4, 2, 1):
        keep = (lane // (SIDE * step)) % 2 == 0
        for i in range(8):
            if i & step == 0:
                one, two = rows[i], rows[i + step]
                rows[i] = jnp.where(keep, one, roll(two, SIDE * step))
                rows[i + step] = jnp.where(keep, roll(one, HALF - SIDE * step), two)
    for i in range(8):
        for a in range(2):
            for h in range(2):
                part = 2 * a + h
                store(8 * h + i, a, rows[i][part * SIDE : (part + 1) * SIDE])


def local_entries(field, expand_x, expand_y, expand_z, energy):
    pieces = split(field)
    outcome = []
    for tile in range(4):
        lanes = slice(tile * 256, (tile + 1) * 256)
        mixed = dot3(pieces, (expand_x[0][:, lanes], expand_x[1][:, lanes]))
        total = mixed[:SIDE] * expand_z[0:1, lanes]
        for k in range(1, SIDE):
            total += mixed[k * SIDE : (k + 1) * SIDE] * expand_z[k : k + 1, lanes]
        summed = jnp.sum(total * expand_y[:, lanes], axis=0, keepdims=True)
        outcome += [summed[:, :HALF], summed[:, HALF:]]
    lane = lax.broadcasted_iota(jnp.int32, (1, HALF), 1)
    outcome[7] = jnp.where(lane == HALF - 1, energy, outcome[7])
    return outcome


def owner_map():
    row = lax.broadcasted_iota(jnp.int32, (LANES, 256), 0)
    lane = lax.broadcasted_iota(jnp.int32, (LANES, 256), 1)
    owner = jnp.where(row >= SPARE, 0, row // HALF)
    return jnp.where(owner == lane // 32, 1.0, 0.0).astype(BF16)


def surface_hats(entries, gather, spread, onehot, columns, heads, root, power, at_y, at_z, sines):
    product = jnp.concatenate(
        [gather[:, r * HALF : (r + 1) * HALF] * entries[r : r + 1, :] for r in range(8)], axis=1
    )
    high, rest = product.astype(BF16), None
    rest = product - high.astype(F32)
    middle = rest.astype(BF16)
    low = (rest - middle.astype(F32)).astype(BF16)
    moments = dot(high, onehot) + (dot(middle, onehot) + dot(low, onehot))
    shape = moments[0:1, :] * spread[0]
    for slot in range(1, 45):
        shape += moments[slot : slot + 1, :] * spread[slot]
    lane = lax.broadcasted_iota(jnp.int32, (SIDE, 256), 1)
    blocks = []
    for face in range(3):
        for normal in range(2):
            for odd in range(2):
                for head in range(2):
                    tail = (odd + normal + head) % 2
                    px, py, pz = (
                        (tail, head, normal),
                        (tail, normal, head),
                        (normal, head, tail),
                    )[face]
                    base = (px * 4 + py * 2 + pz) * 32 + face * 9
                    blocks.append(jnp.where((lane >= base) & (lane < base + 9), shape, 0.0))
    right = dot3(split(jnp.concatenate(blocks, axis=0)), columns)
    hats = []
    for face in range(3):
        left = at_z if face == 1 else at_y
        both = jnp.concatenate(left, axis=0)
        for normal in range(2):
            parts = []
            for odd in range(2):
                start = ((face * 2 + normal) * 2 + odd) * 32
                high, low = split(right[start : start + 32])
                stack = jnp.concatenate([high, low, high, low], axis=0)
                parts.append(dot(heads[odd * 256 : (odd + 1) * 256, :], stack))
            plane = split(power * (root * parts[0] + parts[1]))
            first = dot(both, plane[0])
            hats.append(first[:SIDE] + (first[SIDE:] + dot(left[0], plane[1])))
    full = dot3(split(jnp.concatenate(hats[:4], axis=0)), sines)
    last = dot3(split(jnp.concatenate(hats[4:], axis=0)), at_z, NT)
    return full, last


def source_block(k, full, last, edge_y, edge_z, edge_lane):
    ky = lax.broadcasted_iota(jnp.int32, (SIDE, 256), 0)
    wide = jnp.concatenate([edge_y, edge_y], axis=1)
    scale = edge_z[k : k + 1, :]
    scale = jnp.concatenate([scale, scale], axis=1)
    normal = k % 2
    value = full[normal * SIDE : (normal + 1) * SIDE] * scale
    side = jnp.where(
        ky % 2 == 0,
        full[2 * SIDE + k : 2 * SIDE + k + 1, :],
        full[3 * SIDE + k : 3 * SIDE + k + 1, :],
    )
    value += side * wide
    value += last[:SIDE, k : k + 1] * edge_lane[0] + last[SIDE:, k : k + 1] * edge_lane[1]
    return value


def start_all(phase, source, target, axis, me, send_sem, recv_sem, rows):
    def body(d, carry):
        copy_of(phase, source, target, axis, me, send_sem, recv_sem, rows, d).start()
        return carry

    lax.fori_loop(1, SIDE, body, 0)


def copy_of(phase, source, target, axis, me, send_sem, recv_sem, rows, d):
    peer = lax.rem(me + d, SIDE)
    if rows is None:
        src = source
    else:
        src = source.at[pl.ds(pl.multiple_of(peer * rows, rows), rows), :]
    count = source.shape[0] if rows is None else rows
    return pltpu.make_async_remote_copy(
        src_ref=src,
        dst_ref=target.at[pl.ds(pl.multiple_of(me * count, count), count), :],
        send_sem=send_sem.at[phase, d],
        recv_sem=recv_sem.at[phase, d],
        device_id={axis: peer},
        device_id_type=MESH,
    )


def finish_all(phase, source, target, axis, me, send_sem, recv_sem, rows, sent):
    def body(d, carry):
        copy = copy_of(phase, source, target, axis, me, send_sem, recv_sem, rows, d)
        if sent:
            copy.wait_send()
        else:
            copy.wait_recv()
        return carry

    lax.fori_loop(1, SIDE, body, 0)


def sum_slots(ref):
    total = ref[0:8, :]
    for slot in range(1, SIDE):
        total += ref[slot * 8 : (slot + 1) * 8, :]
    return total


CONSTANTS = 15


def kernel(*refs):
    charge_hbm = refs[0]
    held_hbm = refs[1 : 1 + CONSTANTS]
    out_ref, energy_ref = refs[1 + CONSTANTS : 3 + CONSTANTS]
    scratch = refs[3 + CONSTANTS :]
    charge = scratch[0]
    held = scratch[1 : 1 + CONSTANTS]
    sends = scratch[1 + CONSTANTS : 5 + CONSTANTS]
    lands = scratch[5 + CONSTANTS : 9 + CONSTANTS]
    (
        mats, spectrum, field_ref, inverse_ref, expand_high, expand_low, expand_y, expand_z,
        onehot, small_send, small_land, local_sem, send_sem, recv_sem,
    ) = scratch[9 + CONSTANTS :]
    (
        sine_high, sine_low, eigen_wide, edge_wide, lane_rows, basis_high, basis_low, select,
        gather, spread, column_high, column_low, heads, root, power,
    ) = held
    p = lax.axis_index("gx")
    q = lax.axis_index("gy")

    copies = [pltpu.make_async_copy(charge_hbm, charge, local_sem.at[0])]
    for i in range(CONSTANTS):
        copies.append(pltpu.make_async_copy(held_hbm[i], held[i], local_sem.at[i + 1]))
    for copy in copies:
        copy.start()

    barrier = pltpu.get_barrier_semaphore()

    def greet(d, carry):
        pl.semaphore_signal(
            barrier, inc=1, device_id={"gx": lax.rem(p + d, SIDE)}, device_id_type=MESH
        )
        pl.semaphore_signal(
            barrier, inc=1, device_id={"gy": lax.rem(q + d, SIDE)}, device_id_type=MESH
        )
        return carry

    lax.fori_loop(1, SIDE, greet, 0)

    def at(index):
        return pl.ds(pl.multiple_of(index * SIDE, SIDE), SIDE)

    def sines():
        return sine_high[...], sine_low[...]

    def launch(phase, value, axis, me):
        sends[phase][...] = dot3(sines(), split(value), NT)
        if phase == 0:
            pl.semaphore_wait(barrier, 2 * (SIDE - 1))
        start_all(phase, sends[phase], lands[phase], axis, me, send_sem, recv_sem, SIDE)
        lands[phase][at(me), :] = sends[phase][at(me), :]

    def collect(phase, axis, me, strided):
        finish_all(phase, sends[phase], lands[phase], axis, me, send_sem, recv_sem, SIDE, False)
        land = lands[phase]

        def load(a, h):
            return land[a * SIDE : (a + 1) * SIDE, h * HALF : (h + 1) * HALF]

        def store(g, h, piece):
            if strided:
                mats[h][pl.ds(g, SIDE, stride=SIDE), :] = piece
            else:
                mats[h][g * SIDE : (g + 1) * SIDE, :] = piece

        regroup(load, store, lambda v, amount: pltpu.roll(v, amount, 1))

    def mat():
        return jnp.concatenate([mats[0][...], mats[1][...]], axis=1)

    def small(phase, index, value, axis, me):
        small_send[index][...] = value
        start_all(phase, small_send[index], small_land[index], axis, me, send_sem, recv_sem, None)
        small_land[index][pl.ds(pl.multiple_of(me * 8, 8), 8), :] = value

    def small_total(phase, index, axis, me):
        finish_all(
            phase, small_send[index], small_land[index], axis, me, send_sem, recv_sem, None, False
        )
        return sum_slots(small_land[index])

    copies[0].wait()
    copies[1].wait()
    copies[2].wait()
    launch(0, charge[...], "gy", q)

    for copy in copies[3:]:
        copy.wait()
    for tile in range(4):
        lanes = slice(tile * 256, (tile + 1) * 256)
        expand_high[:, lanes] = dot(basis_high[...], select[0:32, lanes]).astype(BF16)
        expand_low[:, lanes] = dot(basis_low[...], select[0:32, lanes]).astype(BF16)
        expand_y[:, lanes] = dot(basis_high[at(p), :], select[32:64, lanes]) + dot(
            basis_low[at(p), :], select[32:64, lanes]
        )
        expand_z[:, lanes] = dot(basis_high[at(q), :], select[64:96, lanes]) + dot(
            basis_low[at(q), :], select[64:96, lanes]
        )
    eigen_y = eigen_wide[at(p), :]
    eigen_y = jnp.concatenate([eigen_y, eigen_y], axis=1) + lane_rows[0:1, :]
    eigen_z = eigen_wide[at(q), :]
    eigen_z = jnp.concatenate([eigen_z, eigen_z], axis=1)
    cube = ((N + 1) / 2.0) ** 3
    for k in range(SIDE):
        rows = slice(k * SIDE, (k + 1) * SIDE)
        inverse_ref[rows, :] = 1.0 / ((eigen_y + eigen_z[k : k + 1, :]) * cube)
    onehot[...] = owner_map()

    collect(0, "gy", q, True)
    launch(1, mat(), "gx", p)
    collect(1, "gx", p, False)

    value = dot3(split(mat()), sines())
    spectrum[...] = value
    field = value * inverse_ref[...]
    field_ref[...] = field
    energy = jnp.sum(jnp.sum(value * field, axis=1, keepdims=True), axis=0, keepdims=True)
    entries = local_entries(
        field, (expand_high, expand_low), expand_y, expand_z, energy
    )
    small(4, 0, jnp.concatenate(entries, axis=0), "gx", p)
    partial = small_total(4, 0, "gx", p)
    small(5, 1, partial, "gy", q)
    entries = small_total(5, 1, "gy", q)

    at_y = (sine_high[at(p), :], sine_low[at(p), :])
    at_z = (sine_high[at(q), :], sine_low[at(q), :])
    full, last = surface_hats(
        entries, gather, spread, onehot[...], (column_high[...], column_low[...]), heads,
        root[...], power[...], at_y, at_z, sines(),
    )
    edge_y = edge_wide[at(p), :]
    edge_z = edge_wide[at(q), :]
    edge_lane = (lane_rows[1:2, :], lane_rows[2:3, :])
    second = jnp.zeros((SIDE, 256), F32)
    for k in range(SIDE):
        rows = slice(k * SIDE, (k + 1) * SIDE)
        total = field_ref[rows, :] + inverse_ref[rows, :] * source_block(
            k, full, last, edge_y, edge_z, edge_lane
        )
        second += spectrum[rows, :] * total
        mats[0][rows, :] = total[:, :HALF]
        mats[1][rows, :] = total[:, HALF:]
    launch(2, mat(), "gx", p)
    second = jnp.sum(jnp.sum(second, axis=1, keepdims=True), axis=0, keepdims=True)
    small(6, 2, jnp.broadcast_to(second, (8, HALF)), "gx", p)
    collect(2, "gx", p, True)
    launch(3, mat(), "gy", q)
    small(7, 3, small_total(6, 2, "gx", p), "gy", q)
    collect(3, "gy", q, False)
    out_ref[...] = dot3(split(mat()), sines())
    second = small_total(7, 3, "gy", q)
    lane = lax.broadcasted_iota(jnp.int32, (8, HALF), 1)
    first = jnp.broadcast_to(entries[7:8, HALF - 1 :], (8, HALF))
    energy_ref[...] = jnp.where(lane == 0, first, second) * (1.0 / (N + 1)) ** 3

    axes = (("gy", q), ("gx", p), ("gx", p), ("gy", q))
    for phase in range(4):
        axis, me = axes[phase]
        finish_all(phase, sends[phase], lands[phase], axis, me, send_sem, recv_sem, SIDE, True)
    axes = (("gx", p), ("gy", q), ("gx", p), ("gy", q))
    for index in range(4):
        axis, me = axes[index]
        finish_all(
            4 + index, small_send[index], small_land[index], axis, me, send_sem, recv_sem, None, True
        )


def constants():
    sine_rows, eigen, basis, select, gather, spread, columns, rows, root, power = build_tables()

    def pair(table):
        table = table.astype(np.float32)
        high = table.astype(jnp.bfloat16)
        return high, (table - high.astype(np.float32)).astype(jnp.bfloat16)

    parity = np.arange(N) % 2
    lane_rows = np.zeros((8, N))
    lane_rows[0] = eigen
    lane_rows[1] = sine_rows[0] * (parity == 0)
    lane_rows[2] = sine_rows[0] * (parity == 1)
    heads = []
    for odd in range(2):
        tables = [trig(parity_of, odd, np.arctan(2.0 * (np.arange(N) - (N - 1) / 2.0) / (N + 1))) for parity_of in range(2)]
        wide = np.zeros((N, 32))
        for k, table in enumerate(tables):
            wide[:, 16 * k : 16 * k + table.shape[0]] = table.T
        high, low = pair(wide)
        heads.append(np.concatenate([high, high, low, low], axis=1))
    plain = np.float32
    return [
        *pair(sine_rows),
        np.repeat(eigen[:, None], HALF, 1).astype(plain),
        np.repeat(sine_rows[0][:, None], HALF, 1).astype(plain),
        lane_rows.astype(plain),
        *pair(basis),
        np.concatenate(list(select), axis=0).astype(jnp.bfloat16),
        gather.astype(plain),
        spread.astype(plain),
        *pair(columns),
        np.concatenate(heads, axis=0),
        root.astype(plain),
        power.astype(plain),
    ]


def solution(mesh):
    tables = constants()

    def shards(charge_density):
        cells_a, cells_b, length = charge_density.shape
        flat = charge_density.reshape(cells_a * cells_b, length)
        grid = pltpu.VMEM((256, 256), F32)
        hold = [pltpu.VMEM(table.shape, table.dtype) for table in tables]
        potential, energies = pl.pallas_call(
            kernel,
            out_shape=(
                jax.ShapeDtypeStruct((256, 256), F32),
                jax.ShapeDtypeStruct((8, HALF), F32),
            ),
            in_specs=[pl.BlockSpec(memory_space=pl.ANY)] * (1 + CONSTANTS),
            out_specs=(
                pl.BlockSpec(memory_space=pltpu.VMEM),
                pl.BlockSpec(memory_space=pltpu.VMEM),
            ),
            scratch_shapes=[
                grid,
                *hold,
                *[grid] * 8,
                [pltpu.VMEM((256, HALF), F32)] * 2,
                *[grid] * 3,
                pltpu.VMEM((256, LANES), BF16),
                pltpu.VMEM((256, LANES), BF16),
                pltpu.VMEM((SIDE, LANES), F32),
                pltpu.VMEM((SIDE, LANES), F32),
                pltpu.VMEM((LANES, 256), BF16),
                [pltpu.VMEM((8, HALF), F32)] * 4,
                [pltpu.VMEM((8 * SIDE, HALF), F32)] * 4,
                pltpu.SemaphoreType.DMA((1 + CONSTANTS,)),
                pltpu.SemaphoreType.DMA((8, SIDE)),
                pltpu.SemaphoreType.DMA((8, SIDE)),
            ],
            compiler_params=pltpu.CompilerParams(
                collective_id=0, has_side_effects=True, vmem_limit_bytes=48 * 1024 * 1024
            ),
        )(flat, *[jnp.asarray(table) for table in tables])
        return potential.reshape(cells_a, cells_b, length), energies[0, :2]

    return jax.shard_map(
        shards,
        mesh=mesh,
        in_specs=(P("gx", "gy", None),),
        out_specs=(P("gx", "gy", None), P()),
        check_vma=False,
    )
```

```python
import math

import jax
import jax.numpy as jnp
import numpy as np
from jax import lax
from jax.experimental import pallas as pl
from jax.experimental.pallas import tpu as pltpu
from jax.sharding import PartitionSpec as P

ORDER = 16
N = 256
SLOTS = 48
LANES = 1024
SPARE = 7 * 128 + 112
ENERGY_LANE = 1023


def harmonics(x, y, z):
    cosine = {(0, 0): np.ones_like(x)}
    sine = {(0, 0): np.zeros_like(x)}
    for l in range(1, ORDER + 1):
        scale = 1.0 if l == 1 else math.sqrt((2 * l - 1) / (2.0 * l))
        c, s = cosine[l - 1, l - 1], sine[l - 1, l - 1]
        cosine[l, l] = scale * (x * c - y * s)
        sine[l, l] = scale * (x * s + y * c)
        for m in range(l):
            near = (2 * l - 1) / math.sqrt(l * l - m * m)
            far = math.sqrt((l - 1) ** 2 - m * m) / math.sqrt(l * l - m * m)
            for table in (cosine, sine):
                older = table[l - 2, m] if l - 2 >= m else 0.0
                table[l, m] = near * z * table[l - 1, m] - far * older
    return cosine, sine


def face_point(face, t, s):
    one = np.ones_like(t)
    return ((s, t, one), (s, one, t), (one, t, s))[face]


def face_parity(face, px, py, pz):
    return ((py, px, pz), (pz, px, py), (py, pz, px))[face]


def trig(parity, odd, angle):
    if odd:
        orders = np.arange(1, 16, 2)
    else:
        orders = np.arange(0, 17, 2) if parity == 0 else np.arange(2, 17, 2)
    wave = np.cos if parity == 0 else np.sin
    return wave(orders[:, None] * angle[None, :])


def build_tables():
    span = N + 1.0
    step = 1.0 / span
    radius = math.sqrt(3.0) / 2.0
    index = np.arange(N) + 1
    sine_rows = np.sin(np.pi * (index[:, None] * index[None, :] % (2 * N + 2)) / span)
    eigen = 4.0 * span * span * np.sin(np.pi * index / (2 * span)) ** 2
    scaled = 2.0 * (np.arange(N) - (N - 1) / 2.0) * step
    angle = np.arctan(scaled)

    terms = [[] for _ in range(8)]
    for l in range(ORDER + 1):
        for m in range(l + 1):
            terms[(m % 2) * 4 + (l - m) % 2].append((l, m, 0))
            if m:
                terms[((m - 1) % 2) * 4 + 2 + (l - m) % 2].append((l, m, 1))

    nodes, quad = np.polynomial.legendre.leggauss(24)
    legendre = np.polynomial.legendre.legvander(nodes, ORDER).T
    basis = np.zeros((N, 32))
    basis[:, : ORDER + 1] = sine_rows @ np.polynomial.legendre.legvander(scaled, ORDER)
    even = (np.arange(N) % 2 == 0).astype(np.float64)
    basis[:, 17] = sine_rows[0] * even
    basis[:, 18] = sine_rows[0] * (1.0 - even)
    project = legendre * quad[None, :] * (np.arange(ORDER + 1) + 0.5)[:, None]
    turns = 64
    circle = 2.0 * np.pi * np.arange(turns) / turns
    ones_t, ones_s = np.meshgrid(nodes, nodes, indexing="ij")
    alpha, beta = np.meshgrid(circle, circle, indexing="ij")
    solid, wave = [], []
    for face in range(3):
        x, y, z = face_point(face, ones_t, ones_s)
        r = np.sqrt(x * x + y * y + z * z)
        table = harmonics(x / r, y / r, z / r)
        solid.append((table, r / math.sqrt(3.0)))
        ca, sa, cb, sb = np.cos(alpha), np.sin(alpha), np.cos(beta), np.sin(beta)
        parts = (sa * cb, ca * sb, ca * cb)
        order = ((1, 0, 2), (1, 2, 0), (2, 0, 1))[face]
        x, y, z = (parts[k] for k in order)
        r = np.sqrt(x * x + y * y + z * z)
        safe = np.where(r < 1e-12, 1.0, r)
        wave.append((harmonics(x / safe, y / safe, z / safe), np.where(r < 1e-12, 0.0, r)))

    select = np.zeros((3, 32, LANES))
    gather = np.zeros((SLOTS, LANES))
    spread = np.zeros((SLOTS, 16, 256))
    columns = np.zeros((256, N))
    rows = np.zeros((8, 3, 16, N))
    spill = SPARE
    for group in range(8):
        px, py, pz = group >> 2 & 1, group >> 1 & 1, group & 1
        odd = (px + py + pz) % 2
        lane = group * 128
        for face in range(3):
            prow, pcol, normal = face_parity(face, px, py, pz)
            sign = 2.0 if normal == 0 else -2.0
            entries = [
                (i, j)
                for i in range(prow, ORDER + 1, 2)
                for j in range(pcol, ORDER + 1, 2)
                if i + j + normal <= ORDER - odd
            ]
            moments = {}
            for slot, (l, m, which) in enumerate(terms[group]):
                table, ratio = solid[face]
                values = ratio**l * table[which][l, m]
                moments[slot] = project @ values @ project.T
            for i, j in entries:
                if lane >= (group + 1) * 128 or (lane >= SPARE and group == 7):
                    position, spill = spill, spill + 1
                    assert group == 0
                else:
                    position, lane = lane, lane + 1
                axes = ((1, 0, 2), (2, 0, 1), (1, 2, 0))[face]
                select[axes[0], i, position] = 1.0
                select[axes[1], j, position] = 1.0
                select[axes[2], 17 + normal, position] = 1.0
                for slot in moments:
                    gather[slot, position] = step * sign * moments[slot][i, j]
            left = trig(prow, odd, circle)
            right = trig(pcol, odd, circle)
            left_unit = left / np.sum(left * left, axis=1, keepdims=True)
            right_unit = right / np.sum(right * right, axis=1, keepdims=True)
            base = group * 32 + face * 9
            for slot, (l, m, which) in enumerate(terms[group]):
                table, r = wave[face]
                values = r ** (ORDER - odd) * table[which][l, m]
                block = left_unit @ values @ right_unit.T
                weight = (1.0 if m == 0 else 2.0) / (4.0 * math.pi * radius * 1.1 ** (l + 1))
                block = block * weight * sign * span * span
                spread[slot, : block.shape[0], base : base + block.shape[1]] = block
            tail = trig(pcol, odd, angle)
            columns[base : base + tail.shape[0]] = tail
            head = trig(prow, odd, angle)
            rows[group, face, : head.shape[0]] = head
    assert spill < ENERGY_LANE
    root = 1.0 / np.sqrt(1.0 - np.outer(np.sin(angle) ** 2, np.sin(angle) ** 2))
    return sine_rows, eigen, basis, select, gather, spread, columns, rows, root, root**15

MESH = pl.DeviceIdType.MESH
SIDE = 16
HALF = 128
F32 = jnp.float32
BF16 = jnp.bfloat16
NN = (((1,), (0,)), ((), ()))
NT = (((1,), (1,)), ((), ()))


def split(value):
    high = value.astype(BF16)
    return high, (value - high.astype(F32)).astype(BF16)


def dot(a, b, dims=NN):
    return lax.dot_general(a, b, dims, preferred_element_type=F32)


def dot3(a, b, dims=NN):
    return dot(a[0], b[0], dims) + (dot(a[0], b[1], dims) + dot(a[1], b[0], dims))


def regroup(load, store, roll):
    lane = lax.broadcasted_iota(jnp.int32, (4 * SIDE, HALF), 1)
    rows = [
        jnp.concatenate([load(8 * a + i, h) for a in range(2) for h in range(2)], axis=0)
        for i in range(8)
    ]
    for step in (4, 2, 1):
        keep = (lane // (SIDE * step)) % 2 == 0
        for i in range(8):
            if i & step == 0:
                one, two = rows[i], rows[i + step]
                rows[i] = jnp.where(keep, one, roll(two, SIDE * step))
                rows[i + step] = jnp.where(keep, roll(one, HALF - SIDE * step), two)
    for i in range(8):
        for a in range(2):
            for h in range(2):
                part = 2 * a + h
                store(8 * h + i, a, rows[i][part * SIDE : (part + 1) * SIDE])


def local_entries(field, expand_x, expand_y, expand_z, energy):
    pieces = split(field)
    outcome = []
    for tile in range(4):
        lanes = slice(tile * 256, (tile + 1) * 256)
        mixed = dot3(pieces, (expand_x[0][:, lanes], expand_x[1][:, lanes]))
        total = mixed[:SIDE] * expand_z[0:1, lanes]
        for k in range(1, SIDE):
            total += mixed[k * SIDE : (k + 1) * SIDE] * expand_z[k : k + 1, lanes]
        summed = jnp.sum(total * expand_y[:, lanes], axis=0, keepdims=True)
        outcome += [summed[:, :HALF], summed[:, HALF:]]
    lane = lax.broadcasted_iota(jnp.int32, (1, HALF), 1)
    outcome[7] = jnp.where(lane == HALF - 1, energy, outcome[7])
    return outcome


def owner_map():
    row = lax.broadcasted_iota(jnp.int32, (LANES, 256), 0)
    lane = lax.broadcasted_iota(jnp.int32, (LANES, 256), 1)
    owner = jnp.where(row >= SPARE, 0, row // HALF)
    return jnp.where(owner == lane // 32, 1.0, 0.0).astype(BF16)


def surface_hats(entries, gather, spread, onehot, columns, heads, root, power, at_y, at_z, sines):
    product = jnp.concatenate(
        [gather[:, r * HALF : (r + 1) * HALF] * entries[r : r + 1, :] for r in range(8)], axis=1
    )
    high, rest = product.astype(BF16), None
    rest = product - high.astype(F32)
    middle = rest.astype(BF16)
    low = (rest - middle.astype(F32)).astype(BF16)
    moments = dot(high, onehot) + (dot(middle, onehot) + dot(low, onehot))
    shape = moments[0:1, :] * spread[0]
    for slot in range(1, 45):
        shape += moments[slot : slot + 1, :] * spread[slot]
    lane = lax.broadcasted_iota(jnp.int32, (SIDE, 256), 1)
    blocks = []
    for face in range(3):
        for normal in range(2):
            for odd in range(2):
                for head in range(2):
                    tail = (odd + normal + head) % 2
                    px, py, pz = (
                        (tail, head, normal),
                        (tail, normal, head),
                        (normal, head, tail),
                    )[face]
                    base = (px * 4 + py * 2 + pz) * 32 + face * 9
                    blocks.append(jnp.where((lane >= base) & (lane < base + 9), shape, 0.0))
    right = dot3(split(jnp.concatenate(blocks, axis=0)), columns)
    hats = []
    for face in range(3):
        left = at_z if face == 1 else at_y
        both = jnp.concatenate(left, axis=0)
        for normal in range(2):
            parts = []
            for odd in range(2):
                start = ((face * 2 + normal) * 2 + odd) * 32
                high, low = split(right[start : start + 32])
                stack = jnp.concatenate([high, low, high, low], axis=0)
                parts.append(dot(heads[odd * 256 : (odd + 1) * 256, :], stack))
            plane = split(power * (root * parts[0] + parts[1]))
            first = dot(both, plane[0])
            hats.append(first[:SIDE] + (first[SIDE:] + dot(left[0], plane[1])))
    full = dot3(split(jnp.concatenate(hats[:4], axis=0)), sines)
    last = dot3(split(jnp.concatenate(hats[4:], axis=0)), at_z, NT)
    return full, last


def source_block(k, full, last, edge_y, edge_z, edge_lane):
    ky = lax.broadcasted_iota(jnp.int32, (SIDE, 256), 0)
    wide = jnp.concatenate([edge_y, edge_y], axis=1)
    scale = edge_z[k : k + 1, :]
    scale = jnp.concatenate([scale, scale], axis=1)
    normal = k % 2
    value = full[normal * SIDE : (normal + 1) * SIDE] * scale
    side = jnp.where(
        ky % 2 == 0,
        full[2 * SIDE + k : 2 * SIDE + k + 1, :],
        full[3 * SIDE + k : 3 * SIDE + k + 1, :],
    )
    value += side * wide
    value += last[:SIDE, k : k + 1] * edge_lane[0] + last[SIDE:, k : k + 1] * edge_lane[1]
    return value


def start_all(phase, source, target, axis, me, send_sem, recv_sem, rows):
    def body(d, carry):
        copy_of(phase, source, target, axis, me, send_sem, recv_sem, rows, d).start()
        return carry

    lax.fori_loop(1, SIDE, body, 0)


def copy_of(phase, source, target, axis, me, send_sem, recv_sem, rows, d):
    peer = lax.rem(me + d, SIDE)
    if rows is None:
        src = source
    else:
        src = source.at[pl.ds(pl.multiple_of(peer * rows, rows), rows), :]
    count = source.shape[0] if rows is None else rows
    return pltpu.make_async_remote_copy(
        src_ref=src,
        dst_ref=target.at[pl.ds(pl.multiple_of(me * count, count), count), :],
        send_sem=send_sem.at[phase, d],
        recv_sem=recv_sem.at[phase, d],
        device_id={axis: peer},
        device_id_type=MESH,
    )


def finish_all(phase, source, target, axis, me, send_sem, recv_sem, rows, sent):
    def body(d, carry):
        copy = copy_of(phase, source, target, axis, me, send_sem, recv_sem, rows, d)
        if sent:
            copy.wait_send()
        else:
            copy.wait_recv()
        return carry

    lax.fori_loop(1, SIDE, body, 0)


def sum_slots(ref):
    total = ref[0:8, :]
    for slot in range(1, SIDE):
        total += ref[slot * 8 : (slot + 1) * 8, :]
    return total


CONSTANTS = 15


def kernel(*refs):
    charge_hbm = refs[0]
    held_hbm = refs[1 : 1 + CONSTANTS]
    out_ref, energy_ref = refs[1 + CONSTANTS : 3 + CONSTANTS]
    scratch = refs[3 + CONSTANTS :]
    charge = scratch[0]
    held = scratch[1 : 1 + CONSTANTS]
    sends = scratch[1 + CONSTANTS : 5 + CONSTANTS]
    lands = scratch[5 + CONSTANTS : 9 + CONSTANTS]
    (
        mats, spectrum, field_ref, inverse_ref, expand_high, expand_low, expand_y, expand_z,
        onehot, small_send, small_land, local_sem, send_sem, recv_sem,
    ) = scratch[9 + CONSTANTS :]
    (
        sine_high, sine_low, eigen_wide, edge_wide, lane_rows, basis_high, basis_low, select,
        gather, spread, column_high, column_low, heads, root, power,
    ) = held
    p = lax.axis_index("gx")
    q = lax.axis_index("gy")

    copies = [pltpu.make_async_copy(charge_hbm, charge, local_sem.at[0])]
    for i in range(CONSTANTS):
        copies.append(pltpu.make_async_copy(held_hbm[i], held[i], local_sem.at[i + 1]))
    for copy in copies:
        copy.start()

    barrier = pltpu.get_barrier_semaphore()

    def greet(d, carry):
        pl.semaphore_signal(
            barrier, inc=1, device_id={"gx": lax.rem(p + d, SIDE)}, device_id_type=MESH
        )
        pl.semaphore_signal(
            barrier, inc=1, device_id={"gy": lax.rem(q + d, SIDE)}, device_id_type=MESH
        )
        return carry

    lax.fori_loop(1, SIDE, greet, 0)

    def at(index):
        return pl.ds(pl.multiple_of(index * SIDE, SIDE), SIDE)

    def sines():
        return sine_high[...], sine_low[...]

    def launch(phase, value, axis, me):
        sends[phase][...] = dot3(sines(), split(value), NT)
        if phase == 0:
            pl.semaphore_wait(barrier, 2 * (SIDE - 1))
        start_all(phase, sends[phase], lands[phase], axis, me, send_sem, recv_sem, SIDE)
        lands[phase][at(me), :] = sends[phase][at(me), :]

    def collect(phase, axis, me, strided):
        finish_all(phase, sends[phase], lands[phase], axis, me, send_sem, recv_sem, SIDE, False)
        land = lands[phase]

        def load(a, h):
            return land[a * SIDE : (a + 1) * SIDE, h * HALF : (h + 1) * HALF]

        def store(g, h, piece):
            if strided:
                mats[h][pl.ds(g, SIDE, stride=SIDE), :] = piece
            else:
                mats[h][g * SIDE : (g + 1) * SIDE, :] = piece

        regroup(load, store, lambda v, amount: pltpu.roll(v, amount, 1))

    def mat():
        return jnp.concatenate([mats[0][...], mats[1][...]], axis=1)

    def small(phase, index, value, axis, me):
        small_send[index][...] = value
        start_all(phase, small_send[index], small_land[index], axis, me, send_sem, recv_sem, None)
        small_land[index][pl.ds(pl.multiple_of(me * 8, 8), 8), :] = value

    def small_total(phase, index, axis, me):
        finish_all(
            phase, small_send[index], small_land[index], axis, me, send_sem, recv_sem, None, False
        )
        return sum_slots(small_land[index])

    copies[0].wait()
    copies[1].wait()
    copies[2].wait()
    launch(0, charge[...], "gy", q)

    for copy in copies[3:]:
        copy.wait()
    for tile in range(4):
        lanes = slice(tile * 256, (tile + 1) * 256)
        expand_high[:, lanes] = dot(basis_high[...], select[0:32, lanes]).astype(BF16)
        expand_low[:, lanes] = dot(basis_low[...], select[0:32, lanes]).astype(BF16)
        expand_y[:, lanes] = dot(basis_high[at(p), :], select[32:64, lanes]) + dot(
            basis_low[at(p), :], select[32:64, lanes]
        )
        expand_z[:, lanes] = dot(basis_high[at(q), :], select[64:96, lanes]) + dot(
            basis_low[at(q), :], select[64:96, lanes]
        )
    eigen_y = eigen_wide[at(p), :]
    eigen_y = jnp.concatenate([eigen_y, eigen_y], axis=1) + lane_rows[0:1, :]
    eigen_z = eigen_wide[at(q), :]
    eigen_z = jnp.concatenate([eigen_z, eigen_z], axis=1)
    cube = ((N + 1) / 2.0) ** 3
    for k in range(SIDE):
        rows = slice(k * SIDE, (k + 1) * SIDE)
        inverse_ref[rows, :] = 1.0 / ((eigen_y + eigen_z[k : k + 1, :]) * cube)
    onehot[...] = owner_map()

    collect(0, "gy", q, True)
    launch(1, mat(), "gx", p)
    collect(1, "gx", p, False)

    value = dot3(split(mat()), sines())
    spectrum[...] = value
    field = value * inverse_ref[...]
    field_ref[...] = field
    energy = jnp.sum(jnp.sum(value * field, axis=1, keepdims=True), axis=0, keepdims=True)
    entries = local_entries(
        field, (expand_high, expand_low), expand_y, expand_z, energy
    )
    small(4, 0, jnp.concatenate(entries, axis=0), "gx", p)
    partial = small_total(4, 0, "gx", p)
    small(5, 1, partial, "gy", q)
    entries = small_total(5, 1, "gy", q)

    at_y = (sine_high[at(p), :], sine_low[at(p), :])
    at_z = (sine_high[at(q), :], sine_low[at(q), :])
    full, last = surface_hats(
        entries, gather, spread, onehot[...], (column_high[...], column_low[...]), heads,
        root[...], power[...], at_y, at_z, sines(),
    )
    edge_y = edge_wide[at(p), :]
    edge_z = edge_wide[at(q), :]
    edge_lane = (lane_rows[1:2, :], lane_rows[2:3, :])
    second = jnp.zeros((SIDE, 256), F32)
    for k in range(SIDE):
        rows = slice(k * SIDE, (k + 1) * SIDE)
        total = field_ref[rows, :] + inverse_ref[rows, :] * source_block(
            k, full, last, edge_y, edge_z, edge_lane
        )
        second += spectrum[rows, :] * total
        mats[0][rows, :] = total[:, :HALF]
        mats[1][rows, :] = total[:, HALF:]
    launch(2, mat(), "gx", p)
    second = jnp.sum(jnp.sum(second, axis=1, keepdims=True), axis=0, keepdims=True)
    small(6, 2, jnp.broadcast_to(second, (8, HALF)), "gx", p)
    collect(2, "gx", p, True)
    launch(3, mat(), "gy", q)
    small(7, 3, small_total(6, 2, "gx", p), "gy", q)
    collect(3, "gy", q, False)
    out_ref[...] = dot3(split(mat()), sines())
    second = small_total(7, 3, "gy", q)
    lane = lax.broadcasted_iota(jnp.int32, (8, HALF), 1)
    first = jnp.broadcast_to(entries[7:8, HALF - 1 :], (8, HALF))
    energy_ref[...] = jnp.where(lane == 0, first, second) * (1.0 / (N + 1)) ** 3

    axes = (("gy", q), ("gx", p), ("gx", p), ("gy", q))
    for phase in range(4):
        axis, me = axes[phase]
        finish_all(phase, sends[phase], lands[phase], axis, me, send_sem, recv_sem, SIDE, True)
    axes = (("gx", p), ("gy", q), ("gx", p), ("gy", q))
    for index in range(4):
        axis, me = axes[index]
        finish_all(
            4 + index, small_send[index], small_land[index], axis, me, send_sem, recv_sem, None, True
        )


def constants():
    sine_rows, eigen, basis, select, gather, spread, columns, rows, root, power = build_tables()

    def pair(table):
        table = table.astype(np.float32)
        high = table.astype(jnp.bfloat16)
        return high, (table - high.astype(np.float32)).astype(jnp.bfloat16)

    parity = np.arange(N) % 2
    lane_rows = np.zeros((8, N))
    lane_rows[0] = eigen
    lane_rows[1] = sine_rows[0] * (parity == 0)
    lane_rows[2] = sine_rows[0] * (parity == 1)
    heads = []
    for odd in range(2):
        tables = [trig(parity_of, odd, np.arctan(2.0 * (np.arange(N) - (N - 1) / 2.0) / (N + 1))) for parity_of in range(2)]
        wide = np.zeros((N, 32))
        for k, table in enumerate(tables):
            wide[:, 16 * k : 16 * k + table.shape[0]] = table.T
        high, low = pair(wide)
        heads.append(np.concatenate([high, high, low, low], axis=1))
    plain = np.float32
    return [
        *pair(sine_rows),
        np.repeat(eigen[:, None], HALF, 1).astype(plain),
        np.repeat(sine_rows[0][:, None], HALF, 1).astype(plain),
        lane_rows.astype(plain),
        *pair(basis),
        np.concatenate(list(select), axis=0).astype(jnp.bfloat16),
        gather.astype(plain),
        spread.astype(plain),
        *pair(columns),
        np.concatenate(heads, axis=0),
        root.astype(plain),
        power.astype(plain),
    ]


def solution(mesh):
    tables = constants()

    def shards(charge_density):
        cells_a, cells_b, length = charge_density.shape
        flat = charge_density.reshape(cells_a * cells_b, length)
        grid = pltpu.VMEM((256, 256), F32)
        hold = [pltpu.VMEM(table.shape, table.dtype) for table in tables]
        potential, energies = pl.pallas_call(
            kernel,
            out_shape=(
                jax.ShapeDtypeStruct((256, 256), F32),
                jax.ShapeDtypeStruct((8, HALF), F32),
            ),
            in_specs=[pl.BlockSpec(memory_space=pl.ANY)] * (1 + CONSTANTS),
            out_specs=(
                pl.BlockSpec(memory_space=pltpu.VMEM),
                pl.BlockSpec(memory_space=pltpu.VMEM),
            ),
            scratch_shapes=[
                grid,
                *hold,
                *[grid] * 8,
                [pltpu.VMEM((256, HALF), F32)] * 2,
                *[grid] * 3,
                pltpu.VMEM((256, LANES), BF16),
                pltpu.VMEM((256, LANES), BF16),
                pltpu.VMEM((SIDE, LANES), F32),
                pltpu.VMEM((SIDE, LANES), F32),
                pltpu.VMEM((LANES, 256), BF16),
                [pltpu.VMEM((8, HALF), F32)] * 4,
                [pltpu.VMEM((8 * SIDE, HALF), F32)] * 4,
                pltpu.SemaphoreType.DMA((1 + CONSTANTS,)),
                pltpu.SemaphoreType.DMA((8, SIDE)),
                pltpu.SemaphoreType.DMA((8, SIDE)),
            ],
            compiler_params=pltpu.CompilerParams(
                collective_id=0, has_side_effects=True, vmem_limit_bytes=67043328
            ),
        )(flat, *[jnp.asarray(table) for table in tables])
        return potential.reshape(cells_a, cells_b, length), energies[0, :2]

    return jax.shard_map(
        shards,
        mesh=mesh,
        in_specs=(P("gx", "gy", None),),
        out_specs=(P("gx", "gy", None), P()),
        check_vma=False,
    )
```

```python
import math

import jax
import jax.numpy as jnp
import numpy as np
from jax import lax
from jax.experimental import pallas as pl
from jax.experimental.pallas import tpu as pltpu
from jax.sharding import PartitionSpec as P

ORDER = 16
N = 256
SLOTS = 48
LANES = 1024
SPARE = 7 * 128 + 112
ENERGY_LANE = 1023


def harmonics(x, y, z):
    cosine = {(0, 0): np.ones_like(x)}
    sine = {(0, 0): np.zeros_like(x)}
    for l in range(1, ORDER + 1):
        scale = 1.0 if l == 1 else math.sqrt((2 * l - 1) / (2.0 * l))
        c, s = cosine[l - 1, l - 1], sine[l - 1, l - 1]
        cosine[l, l] = scale * (x * c - y * s)
        sine[l, l] = scale * (x * s + y * c)
        for m in range(l):
            near = (2 * l - 1) / math.sqrt(l * l - m * m)
            far = math.sqrt((l - 1) ** 2 - m * m) / math.sqrt(l * l - m * m)
            for table in (cosine, sine):
                older = table[l - 2, m] if l - 2 >= m else 0.0
                table[l, m] = near * z * table[l - 1, m] - far * older
    return cosine, sine


def face_point(face, t, s):
    one = np.ones_like(t)
    return ((s, t, one), (s, one, t), (one, t, s))[face]


def face_parity(face, px, py, pz):
    return ((py, px, pz), (pz, px, py), (py, pz, px))[face]


def trig(parity, odd, angle):
    if odd:
        orders = np.arange(1, 16, 2)
    else:
        orders = np.arange(0, 17, 2) if parity == 0 else np.arange(2, 17, 2)
    wave = np.cos if parity == 0 else np.sin
    return wave(orders[:, None] * angle[None, :])


def build_tables():
    span = N + 1.0
    step = 1.0 / span
    radius = math.sqrt(3.0) / 2.0
    index = np.arange(N) + 1
    sine_rows = np.sin(np.pi * (index[:, None] * index[None, :] % (2 * N + 2)) / span)
    eigen = 4.0 * span * span * np.sin(np.pi * index / (2 * span)) ** 2
    scaled = 2.0 * (np.arange(N) - (N - 1) / 2.0) * step
    angle = np.arctan(scaled)

    terms = [[] for _ in range(8)]
    for l in range(ORDER + 1):
        for m in range(l + 1):
            terms[(m % 2) * 4 + (l - m) % 2].append((l, m, 0))
            if m:
                terms[((m - 1) % 2) * 4 + 2 + (l - m) % 2].append((l, m, 1))

    nodes, quad = np.polynomial.legendre.leggauss(24)
    legendre = np.polynomial.legendre.legvander(nodes, ORDER).T
    basis = np.zeros((N, 32))
    basis[:, : ORDER + 1] = sine_rows @ np.polynomial.legendre.legvander(scaled, ORDER)
    even = (np.arange(N) % 2 == 0).astype(np.float64)
    basis[:, 17] = sine_rows[0] * even
    basis[:, 18] = sine_rows[0] * (1.0 - even)
    project = legendre * quad[None, :] * (np.arange(ORDER + 1) + 0.5)[:, None]
    turns = 64
    circle = 2.0 * np.pi * np.arange(turns) / turns
    ones_t, ones_s = np.meshgrid(nodes, nodes, indexing="ij")
    alpha, beta = np.meshgrid(circle, circle, indexing="ij")
    solid, wave = [], []
    for face in range(3):
        x, y, z = face_point(face, ones_t, ones_s)
        r = np.sqrt(x * x + y * y + z * z)
        table = harmonics(x / r, y / r, z / r)
        solid.append((table, r / math.sqrt(3.0)))
        ca, sa, cb, sb = np.cos(alpha), np.sin(alpha), np.cos(beta), np.sin(beta)
        parts = (sa * cb, ca * sb, ca * cb)
        order = ((1, 0, 2), (1, 2, 0), (2, 0, 1))[face]
        x, y, z = (parts[k] for k in order)
        r = np.sqrt(x * x + y * y + z * z)
        safe = np.where(r < 1e-12, 1.0, r)
        wave.append((harmonics(x / safe, y / safe, z / safe), np.where(r < 1e-12, 0.0, r)))

    select = np.zeros((3, 32, LANES))
    gather = np.zeros((SLOTS, LANES))
    spread = np.zeros((SLOTS, 16, 256))
    columns = np.zeros((256, N))
    rows = np.zeros((8, 3, 16, N))
    spill = SPARE
    for group in range(8):
        px, py, pz = group >> 2 & 1, group >> 1 & 1, group & 1
        odd = (px + py + pz) % 2
        lane = group * 128
        for face in range(3):
            prow, pcol, normal = face_parity(face, px, py, pz)
            sign = 2.0 if normal == 0 else -2.0
            entries = [
                (i, j)
                for i in range(prow, ORDER + 1, 2)
                for j in range(pcol, ORDER + 1, 2)
                if i + j + normal <= ORDER - odd
            ]
            moments = {}
            for slot, (l, m, which) in enumerate(terms[group]):
                table, ratio = solid[face]
                values = ratio**l * table[which][l, m]
                moments[slot] = project @ values @ project.T
            for i, j in entries:
                if lane >= (group + 1) * 128 or (lane >= SPARE and group == 7):
                    position, spill = spill, spill + 1
                    assert group == 0
                else:
                    position, lane = lane, lane + 1
                axes = ((1, 0, 2), (2, 0, 1), (1, 2, 0))[face]
                select[axes[0], i, position] = 1.0
                select[axes[1], j, position] = 1.0
                select[axes[2], 17 + normal, position] = 1.0
                for slot in moments:
                    gather[slot, position] = step * sign * moments[slot][i, j]
            left = trig(prow, odd, circle)
            right = trig(pcol, odd, circle)
            left_unit = left / np.sum(left * left, axis=1, keepdims=True)
            right_unit = right / np.sum(right * right, axis=1, keepdims=True)
            base = group * 32 + face * 9
            for slot, (l, m, which) in enumerate(terms[group]):
                table, r = wave[face]
                values = r ** (ORDER - odd) * table[which][l, m]
                block = left_unit @ values @ right_unit.T
                weight = (1.0 if m == 0 else 2.0) / (4.0 * math.pi * radius * 1.1 ** (l + 1))
                block = block * weight * sign * span * span
                spread[slot, : block.shape[0], base : base + block.shape[1]] = block
            tail = trig(pcol, odd, angle)
            columns[base : base + tail.shape[0]] = tail
            head = trig(prow, odd, angle)
            rows[group, face, : head.shape[0]] = head
    assert spill < ENERGY_LANE
    root = 1.0 / np.sqrt(1.0 - np.outer(np.sin(angle) ** 2, np.sin(angle) ** 2))
    return sine_rows, eigen, basis, select, gather, spread, columns, rows, root, root**15

MESH = pl.DeviceIdType.MESH
SIDE = 16
WIDE = 24
HALF = 128
F32 = jnp.float32
BF16 = jnp.bfloat16
NN = (((1,), (0,)), ((), ()))
NT = (((1,), (1,)), ((), ()))


def split(value):
    high = value.astype(BF16)
    return high, (value - high.astype(F32)).astype(BF16)


def dot(a, b, dims=NN):
    return lax.dot_general(a, b, dims, preferred_element_type=F32)


def dot3(a, b, dims=NN):
    return dot(a[0], b[0], dims) + (dot(a[0], b[1], dims) + dot(a[1], b[0], dims))


def regroup(load, store, roll):
    lane = lax.broadcasted_iota(jnp.int32, (4 * SIDE, HALF), 1)
    rows = [
        jnp.concatenate([load(8 * a + i, h) for a in range(2) for h in range(2)], axis=0)
        for i in range(8)
    ]
    for step in (4, 2, 1):
        keep = (lane // (SIDE * step)) % 2 == 0
        for i in range(8):
            if i & step == 0:
                one, two = rows[i], rows[i + step]
                rows[i] = jnp.where(keep, one, roll(two, SIDE * step))
                rows[i + step] = jnp.where(keep, roll(one, HALF - SIDE * step), two)
    for i in range(8):
        for a in range(2):
            for h in range(2):
                part = 2 * a + h
                store(8 * h + i, a, rows[i][part * SIDE : (part + 1) * SIDE])


def green_rows(sines, basis_rows):
    return jnp.concatenate([sines[x : x + 1, :] * basis_rows for x in range(SIDE)], axis=0)


def weighted_rows(table, values):
    total = table[:WIDE] * values[0:1, :]
    for x in range(1, SIDE):
        total += table[x * WIDE : (x + 1) * WIDE] * values[x : x + 1, :]
    return total


def local_entries(folded, expand_y, expand_z, select_x):
    pieces = split(folded)
    outcome = []
    for tile in range(4):
        lanes = slice(tile * 256, (tile + 1) * 256)
        mixed = dot3(pieces, (expand_y[0][:, lanes], expand_y[1][:, lanes]))
        total = mixed[:WIDE] * expand_z[0:1, lanes]
        for k in range(1, SIDE):
            total += mixed[k * WIDE : (k + 1) * WIDE] * expand_z[k : k + 1, lanes]
        chosen = select_x[0:32, lanes].astype(F32)[:WIDE]
        summed = jnp.sum(total * chosen, axis=0, keepdims=True)
        outcome += [summed[:, :HALF], summed[:, HALF:]]
    return outcome


def owner_map():
    row = lax.broadcasted_iota(jnp.int32, (LANES, 256), 0)
    lane = lax.broadcasted_iota(jnp.int32, (LANES, 256), 1)
    owner = jnp.where(row >= SPARE, 0, row // HALF)
    return jnp.where(owner == lane // 32, 1.0, 0.0).astype(BF16)


def surface_hats(entries, gather, spread, onehot, columns, heads, root, power, at_y, at_z, sines):
    product = jnp.concatenate(
        [gather[:, r * HALF : (r + 1) * HALF] * entries[r : r + 1, :] for r in range(8)], axis=1
    )
    high, rest = product.astype(BF16), None
    rest = product - high.astype(F32)
    middle = rest.astype(BF16)
    low = (rest - middle.astype(F32)).astype(BF16)
    moments = dot(high, onehot) + (dot(middle, onehot) + dot(low, onehot))
    shape = moments[0:1, :] * spread[0]
    for slot in range(1, 45):
        shape += moments[slot : slot + 1, :] * spread[slot]
    lane = lax.broadcasted_iota(jnp.int32, (SIDE, 256), 1)
    blocks = []
    for face in range(3):
        for normal in range(2):
            for odd in range(2):
                for head in range(2):
                    tail = (odd + normal + head) % 2
                    px, py, pz = (
                        (tail, head, normal),
                        (tail, normal, head),
                        (normal, head, tail),
                    )[face]
                    base = (px * 4 + py * 2 + pz) * 32 + face * 9
                    blocks.append(jnp.where((lane >= base) & (lane < base + 9), shape, 0.0))
    right = dot3(split(jnp.concatenate(blocks, axis=0)), columns)
    hats = []
    for face in range(3):
        left = at_z if face == 1 else at_y
        both = jnp.concatenate(left, axis=0)
        for normal in range(2):
            parts = []
            for odd in range(2):
                start = ((face * 2 + normal) * 2 + odd) * 32
                high, low = split(right[start : start + 32])
                stack = jnp.concatenate([high, low, high, low], axis=0)
                parts.append(dot(heads[odd * 256 : (odd + 1) * 256, :], stack))
            plane = split(power * (root * parts[0] + parts[1]))
            first = dot(both, plane[0])
            hats.append(first[:SIDE] + (first[SIDE:] + dot(left[0], plane[1])))
    full = dot3(split(jnp.concatenate(hats[:4], axis=0)), sines)
    last = dot3(split(jnp.concatenate(hats[4:], axis=0)), at_z, NT)
    return full, last


def source_block(k, full, last, edge_y, edge_z, edge_lane):
    ky = lax.broadcasted_iota(jnp.int32, (SIDE, 256), 0)
    wide = jnp.concatenate([edge_y, edge_y], axis=1)
    scale = edge_z[k : k + 1, :]
    scale = jnp.concatenate([scale, scale], axis=1)
    normal = k % 2
    value = full[normal * SIDE : (normal + 1) * SIDE] * scale
    side = jnp.where(
        ky % 2 == 0,
        full[2 * SIDE + k : 2 * SIDE + k + 1, :],
        full[3 * SIDE + k : 3 * SIDE + k + 1, :],
    )
    value += side * wide
    value += last[:SIDE, k : k + 1] * edge_lane[0] + last[SIDE:, k : k + 1] * edge_lane[1]
    return value


def start_all(phase, source, target, axis, me, send_sem, recv_sem, rows):
    def body(d, carry):
        copy_of(phase, source, target, axis, me, send_sem, recv_sem, rows, d).start()
        return carry

    lax.fori_loop(1, SIDE, body, 0)


def copy_of(phase, source, target, axis, me, send_sem, recv_sem, rows, d):
    peer = lax.rem(me + d, SIDE)
    if rows is None:
        src = source
    else:
        src = source.at[pl.ds(pl.multiple_of(peer * rows, rows), rows), :]
    count = source.shape[0] if rows is None else rows
    return pltpu.make_async_remote_copy(
        src_ref=src,
        dst_ref=target.at[pl.ds(pl.multiple_of(me * count, count), count), :],
        send_sem=send_sem.at[phase, d],
        recv_sem=recv_sem.at[phase, d],
        device_id={axis: peer},
        device_id_type=MESH,
    )


def finish_all(phase, source, target, axis, me, send_sem, recv_sem, rows, sent):
    def body(d, carry):
        copy = copy_of(phase, source, target, axis, me, send_sem, recv_sem, rows, d)
        if sent:
            copy.wait_send()
        else:
            copy.wait_recv()
        return carry

    lax.fori_loop(1, SIDE, body, 0)


def sum_slots(ref):
    total = ref[0:8, :]
    for slot in range(1, SIDE):
        total += ref[slot * 8 : (slot + 1) * 8, :]
    return total


CONSTANTS = 16


def kernel(*refs):
    charge_hbm = refs[0]
    held_hbm = refs[1 : 1 + CONSTANTS]
    out_ref, energy_ref = refs[1 + CONSTANTS : 3 + CONSTANTS]
    scratch = refs[3 + CONSTANTS :]
    charge = scratch[0]
    held = scratch[1 : 1 + CONSTANTS]
    sends = scratch[1 + CONSTANTS : 5 + CONSTANTS]
    lands = scratch[5 + CONSTANTS : 9 + CONSTANTS]
    (
        mats, spectrum, field_ref, inverse_ref, expand_high, expand_low, expand_z, pair_sum, half_rows, green, folded,
        onehot, small_send, small_land, local_sem, send_sem, recv_sem,
    ) = scratch[9 + CONSTANTS :]
    (
        sine_high, sine_low, eigen_wide, edge_wide, lane_rows, basis_high, basis_low, select,
        gather, spread, column_high, column_low, heads, root, power, basis_rows,
    ) = held
    p = lax.axis_index("gx")
    q = lax.axis_index("gy")

    copies = [pltpu.make_async_copy(charge_hbm, charge, local_sem.at[0])]
    for i in range(CONSTANTS):
        copies.append(pltpu.make_async_copy(held_hbm[i], held[i], local_sem.at[i + 1]))
    for copy in copies:
        copy.start()

    barrier = pltpu.get_barrier_semaphore()

    def greet(d, carry):
        pl.semaphore_signal(
            barrier, inc=1, device_id={"gx": lax.rem(p + d, SIDE)}, device_id_type=MESH
        )
        pl.semaphore_signal(
            barrier, inc=1, device_id={"gy": lax.rem(q + d, SIDE)}, device_id_type=MESH
        )
        return carry

    lax.fori_loop(1, SIDE, greet, 0)

    def at(index):
        return pl.ds(pl.multiple_of(index * SIDE, SIDE), SIDE)

    def sines():
        return sine_high[...], sine_low[...]

    def launch(phase, value, axis, me):
        sends[phase][...] = dot3(sines(), split(value), NT)
        if phase == 0:
            pl.semaphore_wait(barrier, 2 * (SIDE - 1))
        start_all(phase, sends[phase], lands[phase], axis, me, send_sem, recv_sem, SIDE)
        lands[phase][at(me), :] = sends[phase][at(me), :]

    def collect(phase, axis, me, strided):
        finish_all(phase, sends[phase], lands[phase], axis, me, send_sem, recv_sem, SIDE, False)
        land = lands[phase]

        def load(a, h):
            return land[a * SIDE : (a + 1) * SIDE, h * HALF : (h + 1) * HALF]

        def store(g, h, piece):
            if strided:
                mats[h][pl.ds(g, SIDE, stride=SIDE), :] = piece
            else:
                mats[h][g * SIDE : (g + 1) * SIDE, :] = piece

        regroup(load, store, lambda v, amount: pltpu.roll(v, amount, 1))

    def mat():
        return jnp.concatenate([mats[0][...], mats[1][...]], axis=1)

    def small(phase, index, value, axis, me):
        small_send[index][...] = value
        start_all(phase, small_send[index], small_land[index], axis, me, send_sem, recv_sem, None)
        small_land[index][pl.ds(pl.multiple_of(me * 8, 8), 8), :] = value

    def small_total(phase, index, axis, me):
        finish_all(
            phase, small_send[index], small_land[index], axis, me, send_sem, recv_sem, None, False
        )
        return sum_slots(small_land[index])

    copies[0].wait()
    copies[1].wait()
    copies[2].wait()
    launch(0, charge[...], "gy", q)

    for copy in copies[3:]:
        copy.wait()
    for tile in range(4):
        lanes = slice(tile * 256, (tile + 1) * 256)
        expand_high[:, lanes] = dot(basis_high[...], select[32:64, lanes]).astype(BF16)
        expand_low[:, lanes] = dot(basis_low[...], select[32:64, lanes]).astype(BF16)
        expand_z[:, lanes] = dot(basis_high[at(q), :], select[64:96, lanes]) + dot(
            basis_low[at(q), :], select[64:96, lanes]
        )
    cube = ((N + 1) / 2.0) ** 3
    pair_sum[:, :HALF] = eigen_wide[...] + lane_rows[0:1, :HALF]
    pair_sum[:, HALF:] = eigen_wide[...] + lane_rows[0:1, HALF:]
    near = sine_high[at(p), :].astype(F32) + sine_low[at(p), :].astype(F32)
    lead_high, lead_low = split(green_rows(near, basis_rows[...]))

    def fill(k, carry):
        shift = eigen_wide[pl.ds(q * SIDE + k, 1), :]
        shift = jnp.concatenate([shift, shift], axis=1)
        weights = split(1.0 / ((pair_sum[...] + shift) * cube))
        green[k] = dot3((lead_high, lead_low), weights)
        return carry

    lax.fori_loop(0, SIDE, fill, 0)
    eigen_y = eigen_wide[at(p), :]
    eigen_y = jnp.concatenate([eigen_y, eigen_y], axis=1) + lane_rows[0:1, :]
    eigen_z = eigen_wide[at(q), :]
    eigen_z = jnp.concatenate([eigen_z, eigen_z], axis=1)
    for k in range(SIDE):
        rows = slice(k * SIDE, (k + 1) * SIDE)
        inverse_ref[rows, :] = 1.0 / ((eigen_y + eigen_z[k : k + 1, :]) * cube)
    onehot[...] = owner_map()

    collect(0, "gy", q, True)
    launch(1, mat(), "gx", p)
    half_rows[...] = dot3(split(mat()), sines())

    def fold(k, carry):
        folded[pl.ds(pl.multiple_of(k * WIDE, 8), WIDE), :] = weighted_rows(
            green[k], half_rows[at(k), :]
        )
        return carry

    lax.fori_loop(0, SIDE, fold, 0)
    entries = local_entries(folded[...], (expand_high, expand_low), expand_z, select)
    small(4, 0, jnp.concatenate(entries, axis=0), "gy", q)
    small(5, 1, small_total(4, 0, "gy", q), "gx", p)

    collect(1, "gx", p, False)
    value = dot3(split(mat()), sines())
    spectrum[...] = value
    field = value * inverse_ref[...]
    field_ref[...] = field
    energy = jnp.sum(jnp.sum(value * field, axis=1, keepdims=True), axis=0, keepdims=True)
    entries = small_total(5, 1, "gx", p)

    at_y = (sine_high[at(p), :], sine_low[at(p), :])
    at_z = (sine_high[at(q), :], sine_low[at(q), :])
    full, last = surface_hats(
        entries, gather, spread, onehot[...], (column_high[...], column_low[...]), heads,
        root[...], power[...], at_y, at_z, sines(),
    )
    edge_y = edge_wide[at(p), :]
    edge_z = edge_wide[at(q), :]
    edge_lane = (lane_rows[1:2, :], lane_rows[2:3, :])
    second = jnp.zeros((SIDE, 256), F32)
    for k in range(SIDE):
        rows = slice(k * SIDE, (k + 1) * SIDE)
        total = field_ref[rows, :] + inverse_ref[rows, :] * source_block(
            k, full, last, edge_y, edge_z, edge_lane
        )
        second += spectrum[rows, :] * total
        mats[0][rows, :] = total[:, :HALF]
        mats[1][rows, :] = total[:, HALF:]
    launch(2, mat(), "gx", p)
    second = jnp.sum(jnp.sum(second, axis=1, keepdims=True), axis=0, keepdims=True)
    lane = lax.broadcasted_iota(jnp.int32, (8, HALF), 1)
    small(6, 2, jnp.where(lane == 0, energy, second), "gx", p)
    collect(2, "gx", p, True)
    launch(3, mat(), "gy", q)
    small(7, 3, small_total(6, 2, "gx", p), "gy", q)
    collect(3, "gy", q, False)
    out_ref[...] = dot3(split(mat()), sines())
    energy_ref[...] = small_total(7, 3, "gy", q) * (1.0 / (N + 1)) ** 3

    axes = (("gy", q), ("gx", p), ("gx", p), ("gy", q))
    for phase in range(4):
        axis, me = axes[phase]
        finish_all(phase, sends[phase], lands[phase], axis, me, send_sem, recv_sem, SIDE, True)
    axes = (("gy", q), ("gx", p), ("gx", p), ("gy", q))
    for index in range(4):
        axis, me = axes[index]
        finish_all(
            4 + index, small_send[index], small_land[index], axis, me, send_sem, recv_sem, None, True
        )


def constants():
    sine_rows, eigen, basis, select, gather, spread, columns, rows, root, power = build_tables()

    def pair(table):
        table = table.astype(np.float32)
        high = table.astype(jnp.bfloat16)
        return high, (table - high.astype(np.float32)).astype(jnp.bfloat16)

    parity = np.arange(N) % 2
    lane_rows = np.zeros((8, N))
    lane_rows[0] = eigen
    lane_rows[1] = sine_rows[0] * (parity == 0)
    lane_rows[2] = sine_rows[0] * (parity == 1)
    heads = []
    for odd in range(2):
        tables = [trig(parity_of, odd, np.arctan(2.0 * (np.arange(N) - (N - 1) / 2.0) / (N + 1))) for parity_of in range(2)]
        wide = np.zeros((N, 32))
        for k, table in enumerate(tables):
            wide[:, 16 * k : 16 * k + table.shape[0]] = table.T
        high, low = pair(wide)
        heads.append(np.concatenate([high, high, low, low], axis=1))
    plain = np.float32
    return [
        *pair(sine_rows),
        np.repeat(eigen[:, None], HALF, 1).astype(plain),
        np.repeat(sine_rows[0][:, None], HALF, 1).astype(plain),
        lane_rows.astype(plain),
        *pair(basis),
        np.concatenate(list(select), axis=0).astype(jnp.bfloat16),
        gather.astype(plain),
        spread.astype(plain),
        *pair(columns),
        np.concatenate(heads, axis=0),
        root.astype(plain),
        power.astype(plain),
        np.ascontiguousarray(basis.T[:WIDE]).astype(plain),
    ]


def solution(mesh):
    tables = constants()

    def shards(charge_density):
        cells_a, cells_b, length = charge_density.shape
        flat = charge_density.reshape(cells_a * cells_b, length)
        grid = pltpu.VMEM((256, 256), F32)
        hold = [pltpu.VMEM(table.shape, table.dtype) for table in tables]
        potential, energies = pl.pallas_call(
            kernel,
            out_shape=(
                jax.ShapeDtypeStruct((256, 256), F32),
                jax.ShapeDtypeStruct((8, HALF), F32),
            ),
            in_specs=[pl.BlockSpec(memory_space=pl.ANY)] * (1 + CONSTANTS),
            out_specs=(
                pl.BlockSpec(memory_space=pltpu.VMEM),
                pl.BlockSpec(memory_space=pltpu.VMEM),
            ),
            scratch_shapes=[
                grid,
                *hold,
                *[grid] * 8,
                [pltpu.VMEM((256, HALF), F32)] * 2,
                *[grid] * 3,
                pltpu.VMEM((256, LANES), BF16),
                pltpu.VMEM((256, LANES), BF16),
                pltpu.VMEM((SIDE, LANES), F32),
                grid,
                grid,
                pltpu.VMEM((SIDE, SIDE * WIDE, 256), F32),
                pltpu.VMEM((SIDE * WIDE, 256), F32),
                pltpu.VMEM((LANES, 256), BF16),
                [pltpu.VMEM((8, HALF), F32)] * 4,
                [pltpu.VMEM((8 * SIDE, HALF), F32)] * 4,
                pltpu.SemaphoreType.DMA((1 + CONSTANTS,)),
                pltpu.SemaphoreType.DMA((8, SIDE)),
                pltpu.SemaphoreType.DMA((8, SIDE)),
            ],
            compiler_params=pltpu.CompilerParams(
                collective_id=0, has_side_effects=True, vmem_limit_bytes=67043328
            ),
        )(flat, *[jnp.asarray(table) for table in tables])
        return potential.reshape(cells_a, cells_b, length), energies[0, :2]

    return jax.shard_map(
        shards,
        mesh=mesh,
        in_specs=(P("gx", "gy", None),),
        out_specs=(P("gx", "gy", None), P()),
        check_vma=False,
    )
```

```python
import math

import jax
import jax.numpy as jnp
import numpy as np
from jax import lax
from jax.experimental import pallas as pl
from jax.experimental.pallas import tpu as pltpu
from jax.sharding import PartitionSpec as P

ORDER = 16
N = 256
SLOTS = 48
LANES = 1024
SPARE = 7 * 128 + 112
ENERGY_LANE = 1023


def harmonics(x, y, z):
    cosine = {(0, 0): np.ones_like(x)}
    sine = {(0, 0): np.zeros_like(x)}
    for l in range(1, ORDER + 1):
        scale = 1.0 if l == 1 else math.sqrt((2 * l - 1) / (2.0 * l))
        c, s = cosine[l - 1, l - 1], sine[l - 1, l - 1]
        cosine[l, l] = scale * (x * c - y * s)
        sine[l, l] = scale * (x * s + y * c)
        for m in range(l):
            near = (2 * l - 1) / math.sqrt(l * l - m * m)
            far = math.sqrt((l - 1) ** 2 - m * m) / math.sqrt(l * l - m * m)
            for table in (cosine, sine):
                older = table[l - 2, m] if l - 2 >= m else 0.0
                table[l, m] = near * z * table[l - 1, m] - far * older
    return cosine, sine


def face_point(face, t, s):
    one = np.ones_like(t)
    return ((s, t, one), (s, one, t), (one, t, s))[face]


def face_parity(face, px, py, pz):
    return ((py, px, pz), (pz, px, py), (py, pz, px))[face]


def trig(parity, odd, angle):
    if odd:
        orders = np.arange(1, 16, 2)
    else:
        orders = np.arange(0, 17, 2) if parity == 0 else np.arange(2, 17, 2)
    wave = np.cos if parity == 0 else np.sin
    return wave(orders[:, None] * angle[None, :])


def build_tables():
    span = N + 1.0
    step = 1.0 / span
    radius = math.sqrt(3.0) / 2.0
    index = np.arange(N) + 1
    sine_rows = np.sin(np.pi * (index[:, None] * index[None, :] % (2 * N + 2)) / span)
    eigen = 4.0 * span * span * np.sin(np.pi * index / (2 * span)) ** 2
    scaled = 2.0 * (np.arange(N) - (N - 1) / 2.0) * step
    angle = np.arctan(scaled)

    terms = [[] for _ in range(8)]
    for l in range(ORDER + 1):
        for m in range(l + 1):
            terms[(m % 2) * 4 + (l - m) % 2].append((l, m, 0))
            if m:
                terms[((m - 1) % 2) * 4 + 2 + (l - m) % 2].append((l, m, 1))

    nodes, quad = np.polynomial.legendre.leggauss(24)
    legendre = np.polynomial.legendre.legvander(nodes, ORDER).T
    basis = np.zeros((N, 32))
    basis[:, : ORDER + 1] = sine_rows @ np.polynomial.legendre.legvander(scaled, ORDER)
    even = (np.arange(N) % 2 == 0).astype(np.float64)
    basis[:, 17] = sine_rows[0] * even
    basis[:, 18] = sine_rows[0] * (1.0 - even)
    project = legendre * quad[None, :] * (np.arange(ORDER + 1) + 0.5)[:, None]
    turns = 64
    circle = 2.0 * np.pi * np.arange(turns) / turns
    ones_t, ones_s = np.meshgrid(nodes, nodes, indexing="ij")
    alpha, beta = np.meshgrid(circle, circle, indexing="ij")
    solid, wave = [], []
    for face in range(3):
        x, y, z = face_point(face, ones_t, ones_s)
        r = np.sqrt(x * x + y * y + z * z)
        table = harmonics(x / r, y / r, z / r)
        solid.append((table, r / math.sqrt(3.0)))
        ca, sa, cb, sb = np.cos(alpha), np.sin(alpha), np.cos(beta), np.sin(beta)
        parts = (sa * cb, ca * sb, ca * cb)
        order = ((1, 0, 2), (1, 2, 0), (2, 0, 1))[face]
        x, y, z = (parts[k] for k in order)
        r = np.sqrt(x * x + y * y + z * z)
        safe = np.where(r < 1e-12, 1.0, r)
        wave.append((harmonics(x / safe, y / safe, z / safe), np.where(r < 1e-12, 0.0, r)))

    select = np.zeros((3, 32, LANES))
    gather = np.zeros((SLOTS, LANES))
    spread = np.zeros((SLOTS, 16, 256))
    columns = np.zeros((256, N))
    rows = np.zeros((8, 3, 16, N))
    spill = SPARE
    for group in range(8):
        px, py, pz = group >> 2 & 1, group >> 1 & 1, group & 1
        odd = (px + py + pz) % 2
        lane = group * 128
        for face in range(3):
            prow, pcol, normal = face_parity(face, px, py, pz)
            sign = 2.0 if normal == 0 else -2.0
            entries = [
                (i, j)
                for i in range(prow, ORDER + 1, 2)
                for j in range(pcol, ORDER + 1, 2)
                if i + j + normal <= ORDER - odd
            ]
            moments = {}
            for slot, (l, m, which) in enumerate(terms[group]):
                table, ratio = solid[face]
                values = ratio**l * table[which][l, m]
                moments[slot] = project @ values @ project.T
            for i, j in entries:
                if lane >= (group + 1) * 128 or (lane >= SPARE and group == 7):
                    position, spill = spill, spill + 1
                    assert group == 0
                else:
                    position, lane = lane, lane + 1
                axes = ((1, 0, 2), (2, 0, 1), (1, 2, 0))[face]
                select[axes[0], i, position] = 1.0
                select[axes[1], j, position] = 1.0
                select[axes[2], 17 + normal, position] = 1.0
                for slot in moments:
                    gather[slot, position] = step * sign * moments[slot][i, j]
            left = trig(prow, odd, circle)
            right = trig(pcol, odd, circle)
            left_unit = left / np.sum(left * left, axis=1, keepdims=True)
            right_unit = right / np.sum(right * right, axis=1, keepdims=True)
            base = group * 32 + face * 9
            for slot, (l, m, which) in enumerate(terms[group]):
                table, r = wave[face]
                values = r ** (ORDER - odd) * table[which][l, m]
                block = left_unit @ values @ right_unit.T
                weight = (1.0 if m == 0 else 2.0) / (4.0 * math.pi * radius * 1.1 ** (l + 1))
                block = block * weight * sign * span * span
                spread[slot, : block.shape[0], base : base + block.shape[1]] = block
            tail = trig(pcol, odd, angle)
            columns[base : base + tail.shape[0]] = tail
            head = trig(prow, odd, angle)
            rows[group, face, : head.shape[0]] = head
    assert spill < ENERGY_LANE
    root = 1.0 / np.sqrt(1.0 - np.outer(np.sin(angle) ** 2, np.sin(angle) ** 2))
    return sine_rows, eigen, basis, select, gather, spread, columns, rows, root, root**15

MESH = pl.DeviceIdType.MESH
SIDE = 16
WIDE = 24
HALF = 128
F32 = jnp.float32
BF16 = jnp.bfloat16
NN = (((1,), (0,)), ((), ()))
NT = (((1,), (1,)), ((), ()))


def split(value):
    high = value.astype(BF16)
    return high, (value - high.astype(F32)).astype(BF16)


def dot(a, b, dims=NN):
    return lax.dot_general(a, b, dims, preferred_element_type=F32)


def dot3(a, b, dims=NN):
    return dot(a[0], b[0], dims) + (dot(a[0], b[1], dims) + dot(a[1], b[0], dims))


def regroup(load, store, roll):
    lane = lax.broadcasted_iota(jnp.int32, (4 * SIDE, HALF), 1)
    rows = [
        jnp.concatenate([load(8 * a + i, h) for a in range(2) for h in range(2)], axis=0)
        for i in range(8)
    ]
    for step in (4, 2, 1):
        keep = (lane // (SIDE * step)) % 2 == 0
        for i in range(8):
            if i & step == 0:
                one, two = rows[i], rows[i + step]
                rows[i] = jnp.where(keep, one, roll(two, SIDE * step))
                rows[i + step] = jnp.where(keep, roll(one, HALF - SIDE * step), two)
    for i in range(8):
        for a in range(2):
            for h in range(2):
                part = 2 * a + h
                store(8 * h + i, a, rows[i][part * SIDE : (part + 1) * SIDE])


def green_rows(sines, basis_rows):
    rows = [sines[x : x + 1, :] * basis_rows for x in range(SIDE)]
    return jnp.concatenate(rows + [sines * basis_rows[17:18], sines * basis_rows[18:19]], axis=0)


def weighted_rows(table, values):
    total = table[:WIDE] * values[0:1, :]
    for x in range(1, SIDE):
        total += table[x * WIDE : (x + 1) * WIDE] * values[x : x + 1, :]
    return total


def local_entries(folded, expand_y, expand_z, select_x):
    pieces = split(folded)
    outcome = []
    for tile in range(4):
        lanes = slice(tile * 256, (tile + 1) * 256)
        mixed = dot3(pieces, (expand_y[0][:, lanes], expand_y[1][:, lanes]))
        total = mixed[:WIDE] * expand_z[0:1, lanes]
        for k in range(1, SIDE):
            total += mixed[k * WIDE : (k + 1) * WIDE] * expand_z[k : k + 1, lanes]
        chosen = select_x[0:32, lanes].astype(F32)[:WIDE]
        summed = jnp.sum(total * chosen, axis=0, keepdims=True)
        outcome += [summed[:, :HALF], summed[:, HALF:]]
    return outcome


def owner_map():
    row = lax.broadcasted_iota(jnp.int32, (LANES, 256), 0)
    lane = lax.broadcasted_iota(jnp.int32, (LANES, 256), 1)
    owner = jnp.where(row >= SPARE, 0, row // HALF)
    return jnp.where(owner == lane // 32, 1.0, 0.0).astype(BF16)


def surface_planes(entries, gather, spread, onehot, columns, heads, root, power):
    product = jnp.concatenate(
        [gather[:, r * HALF : (r + 1) * HALF] * entries[r : r + 1, :] for r in range(8)], axis=1
    )
    high, rest = product.astype(BF16), None
    rest = product - high.astype(F32)
    middle = rest.astype(BF16)
    low = (rest - middle.astype(F32)).astype(BF16)
    moments = dot(high, onehot) + (dot(middle, onehot) + dot(low, onehot))
    shape = moments[0:1, :] * spread[0]
    for slot in range(1, 45):
        shape += moments[slot : slot + 1, :] * spread[slot]
    lane = lax.broadcasted_iota(jnp.int32, (SIDE, 256), 1)
    blocks = []
    for face in range(3):
        for normal in range(2):
            for odd in range(2):
                for head in range(2):
                    tail = (odd + normal + head) % 2
                    px, py, pz = (
                        (tail, head, normal),
                        (tail, normal, head),
                        (normal, head, tail),
                    )[face]
                    base = (px * 4 + py * 2 + pz) * 32 + face * 9
                    blocks.append(jnp.where((lane >= base) & (lane < base + 9), shape, 0.0))
    right = dot3(split(jnp.concatenate(blocks, axis=0)), columns)
    planes = []
    for face in range(3):
        for normal in range(2):
            parts = []
            for odd in range(2):
                start = ((face * 2 + normal) * 2 + odd) * 32
                high, low = split(right[start : start + 32])
                stack = jnp.concatenate([high, low, high, low], axis=0)
                parts.append(dot(heads[odd * 256 : (odd + 1) * 256, :], stack))
            planes.append(split(power * (root * parts[0] + parts[1])))
    return planes


def few_rows(rows, matrix, dims=NN):
    both = dot(jnp.concatenate(rows, axis=0), matrix[0], dims)
    return both[:SIDE] + (both[SIDE:] + dot(rows[0], matrix[1], dims))


def side_hats(planes, at_y, at_z, sines):
    hat_y = dot3(
        split(jnp.concatenate([few_rows(at_z, planes[2 + n]) for n in range(2)], axis=0)), sines
    )
    half = [few_rows(at_z, planes[4 + n], NT) for n in range(2)]
    hat_x = dot3(split(jnp.concatenate(half, axis=0)), sines)
    return hat_y, hat_x, [dot3(at_y, split(half[n]), NT) for n in range(2)]


def corrected(k, shape, scale, hat_y, hat_x, edge, inverse, edge_green, at_x):
    even = lax.broadcasted_iota(jnp.int32, (256, 256), 0) % 2 == 0
    mixed = shape * scale + jnp.where(even, hat_y[0], hat_y[1]) * edge
    value = few_rows(at_x, split(mixed * inverse), NT)
    return value + hat_x[0] * edge_green[:SIDE] + hat_x[1] * edge_green[SIDE:]


def source_block(k, hat_z, hat_y, last, edge_y, edge_z, edge_lane):
    ky = lax.broadcasted_iota(jnp.int32, (SIDE, 256), 0)
    value = hat_z[k % 2] * edge_z[k : k + 1, :]
    side = jnp.where(ky % 2 == 0, hat_y[k : k + 1, :], hat_y[SIDE + k : SIDE + k + 1, :])
    value += side * edge_y
    value += last[0][:, k : k + 1] * edge_lane[0] + last[1][:, k : k + 1] * edge_lane[1]
    return value


def start_all(phase, source, target, axis, me, send_sem, recv_sem, rows):
    def body(d, carry):
        copy_of(phase, source, target, axis, me, send_sem, recv_sem, rows, d).start()
        return carry

    lax.fori_loop(1, SIDE, body, 0)


def copy_of(phase, source, target, axis, me, send_sem, recv_sem, rows, d):
    peer = lax.rem(me + d, SIDE)
    if rows is None:
        src = source
    else:
        src = source.at[pl.ds(pl.multiple_of(peer * rows, rows), rows), :]
    count = source.shape[0] if rows is None else rows
    return pltpu.make_async_remote_copy(
        src_ref=src,
        dst_ref=target.at[pl.ds(pl.multiple_of(me * count, count), count), :],
        send_sem=send_sem.at[phase, d],
        recv_sem=recv_sem.at[phase, d],
        device_id={axis: peer},
        device_id_type=MESH,
    )


def finish_all(phase, source, target, axis, me, send_sem, recv_sem, rows, sent):
    def body(d, carry):
        copy = copy_of(phase, source, target, axis, me, send_sem, recv_sem, rows, d)
        if sent:
            copy.wait_send()
        else:
            copy.wait_recv()
        return carry

    lax.fori_loop(1, SIDE, body, 0)


def sum_slots(ref):
    total = ref[0:8, :]
    for slot in range(1, SIDE):
        total += ref[slot * 8 : (slot + 1) * 8, :]
    return total


CONSTANTS = 16


def kernel(*refs):
    charge_hbm = refs[0]
    held_hbm = refs[1 : 1 + CONSTANTS]
    out_ref, energy_ref = refs[1 + CONSTANTS : 3 + CONSTANTS]
    scratch = refs[3 + CONSTANTS :]
    charge = scratch[0]
    held = scratch[1 : 1 + CONSTANTS]
    sends = scratch[1 + CONSTANTS : 5 + CONSTANTS]
    lands = scratch[5 + CONSTANTS : 9 + CONSTANTS]
    (
        mats, field_ref, inverse, shape_z, expand_high, expand_low, expand_z, pair_sum, half_rows, green, folded, hats, extra,
        onehot, small_send, small_land, local_sem, send_sem, recv_sem,
    ) = scratch[9 + CONSTANTS :]
    (
        sine_high, sine_low, eigen_wide, edge_wide, lane_rows, basis_high, basis_low, select,
        gather, spread, column_high, column_low, heads, root, power, basis_rows,
    ) = held
    p = lax.axis_index("gx")
    q = lax.axis_index("gy")

    copies = [pltpu.make_async_copy(charge_hbm, charge, local_sem.at[0])]
    for i in range(CONSTANTS):
        copies.append(pltpu.make_async_copy(held_hbm[i], held[i], local_sem.at[i + 1]))
    for copy in copies:
        copy.start()

    barrier = pltpu.get_barrier_semaphore()

    def greet(d, carry):
        pl.semaphore_signal(
            barrier, inc=1, device_id={"gx": lax.rem(p + d, SIDE)}, device_id_type=MESH
        )
        pl.semaphore_signal(
            barrier, inc=1, device_id={"gy": lax.rem(q + d, SIDE)}, device_id_type=MESH
        )
        return carry

    lax.fori_loop(1, SIDE, greet, 0)

    def at(index):
        return pl.ds(pl.multiple_of(index * SIDE, SIDE), SIDE)

    def sines():
        return sine_high[...], sine_low[...]

    def launch(phase, value, axis, me):
        sends[phase][...] = dot3(sines(), split(value), NT)
        if phase == 0:
            pl.semaphore_wait(barrier, 2 * (SIDE - 1))
        start_all(phase, sends[phase], lands[phase], axis, me, send_sem, recv_sem, SIDE)
        lands[phase][at(me), :] = sends[phase][at(me), :]

    def collect(phase, axis, me, strided, added=None):
        finish_all(phase, sends[phase], lands[phase], axis, me, send_sem, recv_sem, SIDE, False)
        land = lands[phase]

        def load(a, h):
            return land[a * SIDE : (a + 1) * SIDE, h * HALF : (h + 1) * HALF]

        def store(g, h, piece):
            if added is not None:
                piece += added[g * SIDE : (g + 1) * SIDE, h * HALF : (h + 1) * HALF]
            if strided:
                mats[h][pl.ds(g, SIDE, stride=SIDE), :] = piece
            else:
                mats[h][g * SIDE : (g + 1) * SIDE, :] = piece

        regroup(load, store, lambda v, amount: pltpu.roll(v, amount, 1))

    def mat():
        return jnp.concatenate([mats[0][...], mats[1][...]], axis=1)

    def small(phase, index, value, axis, me):
        small_send[index][...] = value
        start_all(phase, small_send[index], small_land[index], axis, me, send_sem, recv_sem, None)
        small_land[index][pl.ds(pl.multiple_of(me * 8, 8), 8), :] = value

    def small_total(phase, index, axis, me):
        finish_all(
            phase, small_send[index], small_land[index], axis, me, send_sem, recv_sem, None, False
        )
        return sum_slots(small_land[index])

    copies[0].wait()
    copies[1].wait()
    copies[2].wait()
    launch(0, charge[...], "gy", q)

    for copy in copies[3:]:
        copy.wait()
    for tile in range(4):
        lanes = slice(tile * 256, (tile + 1) * 256)
        expand_high[:, lanes] = dot(basis_high[...], select[32:64, lanes]).astype(BF16)
        expand_low[:, lanes] = dot(basis_low[...], select[32:64, lanes]).astype(BF16)
        expand_z[:, lanes] = dot(basis_high[at(q), :], select[64:96, lanes]) + dot(
            basis_low[at(q), :], select[64:96, lanes]
        )
    cube = ((N + 1) / 2.0) ** 3
    pair_sum[:, :HALF] = eigen_wide[...] + lane_rows[0:1, :HALF]
    pair_sum[:, HALF:] = eigen_wide[...] + lane_rows[0:1, HALF:]
    near = sine_high[at(p), :].astype(F32) + sine_low[at(p), :].astype(F32)
    lead_high, lead_low = split(green_rows(near, basis_rows[...]))

    def fill(k, carry):
        shift = eigen_wide[pl.ds(q * SIDE + k, 1), :]
        shift = jnp.concatenate([shift, shift], axis=1)
        whole = 1.0 / ((pair_sum[...] + shift) * cube)
        inverse[k] = whole
        green[k] = dot3((lead_high, lead_low), split(whole))
        return carry

    lax.fori_loop(0, SIDE, fill, 0)
    onehot[...] = owner_map()

    collect(0, "gy", q, True)
    launch(1, mat(), "gx", p)
    half_rows[...] = dot3(split(mat()), sines())

    def fold(k, carry):
        folded[pl.ds(pl.multiple_of(k * WIDE, 8), WIDE), :] = weighted_rows(
            green[k], half_rows[at(k), :]
        )
        return carry

    lax.fori_loop(0, SIDE, fold, 0)
    entries = local_entries(folded[...], (expand_high, expand_low), expand_z, select)
    small(4, 0, jnp.concatenate(entries, axis=0), "gy", q)
    small(5, 1, small_total(4, 0, "gy", q), "gx", p)

    collect(1, "gx", p, False)
    value = dot3(split(mat()), sines())
    field = value * jnp.concatenate([inverse[k, at(p), :] for k in range(SIDE)], axis=0)
    field_ref[...] = field
    launch(2, field, "gx", p)
    energy = jnp.sum(jnp.sum(value * field, axis=1, keepdims=True), axis=0, keepdims=True)
    entries = small_total(5, 1, "gx", p)

    at_x = at_y = (sine_high[at(p), :], sine_low[at(p), :])
    at_z = (sine_high[at(q), :], sine_low[at(q), :])
    planes = surface_planes(
        entries, gather, spread, onehot[...], (column_high[...], column_low[...]), heads,
        root[...], power[...],
    )
    for n in range(2):
        shape_z[n] = dot3(split(dot3(sines(), planes[n])), sines())
    hat_y, hat_x, last = side_hats(planes, at_y, at_z, sines())
    hats[0] = hat_y
    hats[1] = hat_x

    edge_y = edge_wide[at(p), :]
    edge_y = jnp.concatenate([edge_y, edge_y], axis=1)
    edge_z = edge_wide[at(q), :]
    edge_z = jnp.concatenate([edge_z, edge_z], axis=1)
    edge_lane = (lane_rows[1:2, :], lane_rows[2:3, :])
    near_z = [shape_z[n, at(p), :] for n in range(2)]
    cross = jnp.zeros((SIDE, 256), F32)
    for k in range(SIDE):
        cross += field_ref[k * SIDE : (k + 1) * SIDE, :] * source_block(
            k, near_z, hat_y, last, edge_y, edge_z, edge_lane
        )
    second = energy + jnp.sum(jnp.sum(cross, axis=1, keepdims=True), axis=0, keepdims=True)
    lane = lax.broadcasted_iota(jnp.int32, (8, HALF), 1)
    small(6, 2, jnp.where(lane == 0, energy, second), "gx", p)

    edge = jnp.concatenate([edge_wide[...], edge_wide[...]], axis=1)

    def correct(k, carry):
        scale = edge_wide[pl.ds(q * SIDE + k, 1), :]
        extra[at(k), :] = corrected(
            k,
            shape_z[lax.rem(k, 2)],
            jnp.concatenate([scale, scale], axis=1),
            (hats[0, pl.ds(k, 1), :], hats[0, pl.ds(SIDE + k, 1), :]),
            (hats[1, pl.ds(k, 1), :], hats[1, pl.ds(SIDE + k, 1), :]),
            edge,
            inverse[k],
            green[k, SIDE * WIDE :, :],
            at_x,
        )
        return carry

    lax.fori_loop(0, SIDE, correct, 0)
    collect(2, "gx", p, True, extra)
    launch(3, mat(), "gy", q)
    small(7, 3, small_total(6, 2, "gx", p), "gy", q)
    collect(3, "gy", q, False)
    out_ref[...] = dot3(split(mat()), sines())
    energy_ref[...] = small_total(7, 3, "gy", q) * (1.0 / (N + 1)) ** 3

    axes = (("gy", q), ("gx", p), ("gx", p), ("gy", q))
    for phase in range(4):
        axis, me = axes[phase]
        finish_all(phase, sends[phase], lands[phase], axis, me, send_sem, recv_sem, SIDE, True)
    axes = (("gy", q), ("gx", p), ("gx", p), ("gy", q))
    for index in range(4):
        axis, me = axes[index]
        finish_all(
            4 + index, small_send[index], small_land[index], axis, me, send_sem, recv_sem, None, True
        )


def constants():
    sine_rows, eigen, basis, select, gather, spread, columns, rows, root, power = build_tables()

    def pair(table):
        table = table.astype(np.float32)
        high = table.astype(jnp.bfloat16)
        return high, (table - high.astype(np.float32)).astype(jnp.bfloat16)

    parity = np.arange(N) % 2
    lane_rows = np.zeros((8, N))
    lane_rows[0] = eigen
    lane_rows[1] = sine_rows[0] * (parity == 0)
    lane_rows[2] = sine_rows[0] * (parity == 1)
    heads = []
    for odd in range(2):
        tables = [trig(parity_of, odd, np.arctan(2.0 * (np.arange(N) - (N - 1) / 2.0) / (N + 1))) for parity_of in range(2)]
        wide = np.zeros((N, 32))
        for k, table in enumerate(tables):
            wide[:, 16 * k : 16 * k + table.shape[0]] = table.T
        high, low = pair(wide)
        heads.append(np.concatenate([high, high, low, low], axis=1))
    plain = np.float32
    return [
        *pair(sine_rows),
        np.repeat(eigen[:, None], HALF, 1).astype(plain),
        np.repeat(sine_rows[0][:, None], HALF, 1).astype(plain),
        lane_rows.astype(plain),
        *pair(basis),
        np.concatenate(list(select), axis=0).astype(jnp.bfloat16),
        gather.astype(plain),
        spread.astype(plain),
        *pair(columns),
        np.concatenate(heads, axis=0),
        root.astype(plain),
        power.astype(plain),
        np.ascontiguousarray(basis.T[:WIDE]).astype(plain),
    ]


def solution(mesh):
    tables = constants()

    def shards(charge_density):
        cells_a, cells_b, length = charge_density.shape
        flat = charge_density.reshape(cells_a * cells_b, length)
        grid = pltpu.VMEM((256, 256), F32)
        hold = [pltpu.VMEM(table.shape, table.dtype) for table in tables]
        potential, energies = pl.pallas_call(
            kernel,
            out_shape=(
                jax.ShapeDtypeStruct((256, 256), F32),
                jax.ShapeDtypeStruct((8, HALF), F32),
            ),
            in_specs=[pl.BlockSpec(memory_space=pl.ANY)] * (1 + CONSTANTS),
            out_specs=(
                pl.BlockSpec(memory_space=pltpu.VMEM),
                pl.BlockSpec(memory_space=pltpu.VMEM),
            ),
            scratch_shapes=[
                grid,
                *hold,
                *[grid] * 8,
                [pltpu.VMEM((256, HALF), F32)] * 2,
                grid,
                pltpu.VMEM((SIDE, 256, 256), F32),
                pltpu.VMEM((2, 256, 256), F32),
                pltpu.VMEM((256, LANES), BF16),
                pltpu.VMEM((256, LANES), BF16),
                pltpu.VMEM((SIDE, LANES), F32),
                grid,
                grid,
                pltpu.VMEM((SIDE, SIDE * WIDE + 2 * SIDE, 256), F32),
                pltpu.VMEM((SIDE * WIDE, 256), F32),
                pltpu.VMEM((2, 2 * SIDE, 256), F32),
                grid,
                pltpu.VMEM((LANES, 256), BF16),
                [pltpu.VMEM((8, HALF), F32)] * 4,
                [pltpu.VMEM((8 * SIDE, HALF), F32)] * 4,
                pltpu.SemaphoreType.DMA((1 + CONSTANTS,)),
                pltpu.SemaphoreType.DMA((8, SIDE)),
                pltpu.SemaphoreType.DMA((8, SIDE)),
            ],
            compiler_params=pltpu.CompilerParams(
                collective_id=0, has_side_effects=True, vmem_limit_bytes=67043328
            ),
        )(flat, *[jnp.asarray(table) for table in tables])
        return potential.reshape(cells_a, cells_b, length), energies[0, :2]

    return jax.shard_map(
        shards,
        mesh=mesh,
        in_specs=(P("gx", "gy", None),),
        out_specs=(P("gx", "gy", None), P()),
        check_vma=False,
    )
```

```python
import math

import jax
import jax.numpy as jnp
import numpy as np
from jax import lax
from jax.experimental import pallas as pl
from jax.experimental.pallas import tpu as pltpu
from jax.sharding import PartitionSpec as P

ORDER = 16
N = 256
SLOTS = 48
LANES = 1024
SPARE = 7 * 128 + 112
ENERGY_LANE = 1023


def harmonics(x, y, z):
    cosine = {(0, 0): np.ones_like(x)}
    sine = {(0, 0): np.zeros_like(x)}
    for l in range(1, ORDER + 1):
        scale = 1.0 if l == 1 else math.sqrt((2 * l - 1) / (2.0 * l))
        c, s = cosine[l - 1, l - 1], sine[l - 1, l - 1]
        cosine[l, l] = scale * (x * c - y * s)
        sine[l, l] = scale * (x * s + y * c)
        for m in range(l):
            near = (2 * l - 1) / math.sqrt(l * l - m * m)
            far = math.sqrt((l - 1) ** 2 - m * m) / math.sqrt(l * l - m * m)
            for table in (cosine, sine):
                older = table[l - 2, m] if l - 2 >= m else 0.0
                table[l, m] = near * z * table[l - 1, m] - far * older
    return cosine, sine


def face_point(face, t, s):
    one = np.ones_like(t)
    return ((s, t, one), (s, one, t), (one, t, s))[face]


def face_parity(face, px, py, pz):
    return ((py, px, pz), (pz, px, py), (py, pz, px))[face]


def trig(parity, odd, angle):
    if odd:
        orders = np.arange(1, 16, 2)
    else:
        orders = np.arange(0, 17, 2) if parity == 0 else np.arange(2, 17, 2)
    wave = np.cos if parity == 0 else np.sin
    return wave(orders[:, None] * angle[None, :])


def build_tables():
    span = N + 1.0
    step = 1.0 / span
    radius = math.sqrt(3.0) / 2.0
    index = np.arange(N) + 1
    sine_rows = np.sin(np.pi * (index[:, None] * index[None, :] % (2 * N + 2)) / span)
    eigen = 4.0 * span * span * np.sin(np.pi * index / (2 * span)) ** 2
    scaled = 2.0 * (np.arange(N) - (N - 1) / 2.0) * step
    angle = np.arctan(scaled)

    terms = [[] for _ in range(8)]
    for l in range(ORDER + 1):
        for m in range(l + 1):
            terms[(m % 2) * 4 + (l - m) % 2].append((l, m, 0))
            if m:
                terms[((m - 1) % 2) * 4 + 2 + (l - m) % 2].append((l, m, 1))

    nodes, quad = np.polynomial.legendre.leggauss(24)
    legendre = np.polynomial.legendre.legvander(nodes, ORDER).T
    basis = np.zeros((N, 32))
    basis[:, : ORDER + 1] = sine_rows @ np.polynomial.legendre.legvander(scaled, ORDER)
    even = (np.arange(N) % 2 == 0).astype(np.float64)
    basis[:, 17] = sine_rows[0] * even
    basis[:, 18] = sine_rows[0] * (1.0 - even)
    project = legendre * quad[None, :] * (np.arange(ORDER + 1) + 0.5)[:, None]
    turns = 64
    circle = 2.0 * np.pi * np.arange(turns) / turns
    ones_t, ones_s = np.meshgrid(nodes, nodes, indexing="ij")
    alpha, beta = np.meshgrid(circle, circle, indexing="ij")
    solid, wave = [], []
    for face in range(3):
        x, y, z = face_point(face, ones_t, ones_s)
        r = np.sqrt(x * x + y * y + z * z)
        table = harmonics(x / r, y / r, z / r)
        solid.append((table, r / math.sqrt(3.0)))
        ca, sa, cb, sb = np.cos(alpha), np.sin(alpha), np.cos(beta), np.sin(beta)
        parts = (sa * cb, ca * sb, ca * cb)
        order = ((1, 0, 2), (1, 2, 0), (2, 0, 1))[face]
        x, y, z = (parts[k] for k in order)
        r = np.sqrt(x * x + y * y + z * z)
        safe = np.where(r < 1e-12, 1.0, r)
        wave.append((harmonics(x / safe, y / safe, z / safe), np.where(r < 1e-12, 0.0, r)))

    select = np.zeros((3, 32, LANES))
    gather = np.zeros((SLOTS, LANES))
    spread = np.zeros((SLOTS, 16, 256))
    columns = np.zeros((256, N))
    rows = np.zeros((8, 3, 16, N))
    spill = SPARE
    for group in range(8):
        px, py, pz = group >> 2 & 1, group >> 1 & 1, group & 1
        odd = (px + py + pz) % 2
        lane = group * 128
        for face in range(3):
            prow, pcol, normal = face_parity(face, px, py, pz)
            sign = 2.0 if normal == 0 else -2.0
            entries = [
                (i, j)
                for i in range(prow, ORDER + 1, 2)
                for j in range(pcol, ORDER + 1, 2)
                if i + j + normal <= ORDER - odd
            ]
            moments = {}
            for slot, (l, m, which) in enumerate(terms[group]):
                table, ratio = solid[face]
                values = ratio**l * table[which][l, m]
                moments[slot] = project @ values @ project.T
            for i, j in entries:
                if lane >= (group + 1) * 128 or (lane >= SPARE and group == 7):
                    position, spill = spill, spill + 1
                    assert group == 0
                else:
                    position, lane = lane, lane + 1
                axes = ((1, 0, 2), (2, 0, 1), (1, 2, 0))[face]
                select[axes[0], i, position] = 1.0
                select[axes[1], j, position] = 1.0
                select[axes[2], 17 + normal, position] = 1.0
                for slot in moments:
                    gather[slot, position] = step * sign * moments[slot][i, j]
            left = trig(prow, odd, circle)
            right = trig(pcol, odd, circle)
            left_unit = left / np.sum(left * left, axis=1, keepdims=True)
            right_unit = right / np.sum(right * right, axis=1, keepdims=True)
            base = group * 32 + face * 9
            for slot, (l, m, which) in enumerate(terms[group]):
                table, r = wave[face]
                values = r ** (ORDER - odd) * table[which][l, m]
                block = left_unit @ values @ right_unit.T
                weight = (1.0 if m == 0 else 2.0) / (4.0 * math.pi * radius * 1.1 ** (l + 1))
                block = block * weight * sign * span * span
                spread[slot, : block.shape[0], base : base + block.shape[1]] = block
            tail = trig(pcol, odd, angle)
            columns[base : base + tail.shape[0]] = tail
            head = trig(prow, odd, angle)
            rows[group, face, : head.shape[0]] = head
    assert spill < ENERGY_LANE
    root = 1.0 / np.sqrt(1.0 - np.outer(np.sin(angle) ** 2, np.sin(angle) ** 2))
    return sine_rows, eigen, basis, select, gather, spread, columns, rows, root, root**15

MESH = pl.DeviceIdType.MESH
SIDE = 16
WIDE = 24
EARLY = 2
VMEM_LIMIT = 67043328 - 1024 * 1024
HALF = 128
F32 = jnp.float32
BF16 = jnp.bfloat16
NN = (((1,), (0,)), ((), ()))
NT = (((1,), (1,)), ((), ()))


def split(value):
    high = value.astype(BF16)
    return high, (value - high.astype(F32)).astype(BF16)


def dot(a, b, dims=NN):
    return lax.dot_general(a, b, dims, preferred_element_type=F32)


def dot3(a, b, dims=NN):
    return dot(a[0], b[0], dims) + (dot(a[0], b[1], dims) + dot(a[1], b[0], dims))


def regroup(load, store, roll):
    lane = lax.broadcasted_iota(jnp.int32, (4 * SIDE, HALF), 1)
    rows = [
        jnp.concatenate([load(8 * a + i, h) for a in range(2) for h in range(2)], axis=0)
        for i in range(8)
    ]
    for step in (4, 2, 1):
        keep = (lane // (SIDE * step)) % 2 == 0
        for i in range(8):
            if i & step == 0:
                one, two = rows[i], rows[i + step]
                rows[i] = jnp.where(keep, one, roll(two, SIDE * step))
                rows[i + step] = jnp.where(keep, roll(one, HALF - SIDE * step), two)
    for i in range(8):
        for a in range(2):
            for h in range(2):
                part = 2 * a + h
                store(8 * h + i, a, rows[i][part * SIDE : (part + 1) * SIDE])


def green_rows(sines, basis_rows):
    rows = [sines[x : x + 1, :] * basis_rows for x in range(SIDE)]
    return jnp.concatenate(rows + [sines * basis_rows[17:18], sines * basis_rows[18:19]], axis=0)


def weighted_rows(table, values):
    total = table[:WIDE] * values[0:1, :]
    for x in range(1, SIDE):
        total += table[x * WIDE : (x + 1) * WIDE] * values[x : x + 1, :]
    return total


def local_entries(folded, expand_y, expand_z, select):
    pieces = split(folded)
    outcome = []
    for tile in range(4):
        lanes = slice(tile * 256, (tile + 1) * 256)
        mixed = dot3(pieces, (expand_y[0][:, lanes], expand_y[1][:, lanes]))
        total = mixed[:WIDE] * expand_z[0:1, lanes]
        for k in range(1, SIDE):
            total += mixed[k * WIDE : (k + 1) * WIDE] * expand_z[k : k + 1, lanes]
        chosen = select[tile][0:32, :].astype(F32)[:WIDE]
        summed = jnp.sum(total * chosen, axis=0, keepdims=True)
        outcome += [summed[:, :HALF], summed[:, HALF:]]
    return outcome


def owner_map():
    row = lax.broadcasted_iota(jnp.int32, (LANES, 256), 0)
    lane = lax.broadcasted_iota(jnp.int32, (LANES, 256), 1)
    owner = jnp.where(row >= SPARE, 0, row // HALF)
    return jnp.where(owner == lane // 32, 1.0, 0.0).astype(BF16)


def surface_planes(entries, gather, spread, onehot, columns, heads, root, power):
    product = jnp.concatenate(
        [gather[r][...] * entries[r : r + 1, :] for r in range(8)], axis=1
    )
    high, rest = product.astype(BF16), None
    rest = product - high.astype(F32)
    middle = rest.astype(BF16)
    low = (rest - middle.astype(F32)).astype(BF16)
    moments = dot(high, onehot) + (dot(middle, onehot) + dot(low, onehot))
    shape = moments[0:1, :] * spread[0][0:8, :]
    for slot in range(1, 45):
        shape += moments[slot : slot + 1, :] * spread[0][slot * 8 : slot * 8 + 8, :]
    ninth = jnp.sum(moments * spread[1][...], axis=0, keepdims=True)
    below = lax.broadcasted_iota(jnp.int32, (8, 256), 0) == 0
    shape = jnp.concatenate([shape, jnp.where(below, ninth, 0.0)], axis=0)
    lane = lax.broadcasted_iota(jnp.int32, (SIDE, 256), 1)
    blocks = []
    for face in range(3):
        for normal in range(2):
            for odd in range(2):
                for head in range(2):
                    tail = (odd + normal + head) % 2
                    px, py, pz = (
                        (tail, head, normal),
                        (tail, normal, head),
                        (normal, head, tail),
                    )[face]
                    base = (px * 4 + py * 2 + pz) * 32 + face * 9
                    blocks.append(jnp.where((lane >= base) & (lane < base + 9), shape, 0.0))
    right = dot3(split(jnp.concatenate(blocks, axis=0)), columns)
    planes = []
    for face in range(3):
        for normal in range(2):
            parts = []
            for odd in range(2):
                start = ((face * 2 + normal) * 2 + odd) * 32
                high, low = split(right[start : start + 32])
                stack = jnp.concatenate([high, low, high, low], axis=0)
                parts.append(dot(heads[odd][...], stack))
            planes.append(split(power * (root * parts[0] + parts[1])))
    return planes


def few_rows(rows, matrix, dims=NN):
    both = dot(jnp.concatenate(rows, axis=0), matrix[0], dims)
    return both[:SIDE] + (both[SIDE:] + dot(rows[0], matrix[1], dims))


def side_hats(planes, at_y, at_z, sines):
    half_y = split(jnp.concatenate([few_rows(at_z, planes[2 + n]) for n in range(2)], axis=0))
    hat_y, turned = dot3(half_y, sines), dot3(sines, half_y, NT)
    half = [few_rows(at_z, planes[4 + n], NT) for n in range(2)]
    hat_x = dot3(split(jnp.concatenate(half, axis=0)), sines)
    near_x = [dot3(at_y, split(half[n]), NT) for n in range(2)]
    half_z = split(jnp.concatenate([few_rows(at_y, planes[n]) for n in range(2)], axis=0))
    return hat_y, turned, hat_x, near_x, dot3(half_z, sines)


def corrected(shape, scale, column, edge_lane, hat_x, inverse, edge_green, at_x):
    even = lax.broadcasted_iota(jnp.int32, (1, 256), 1) % 2 == 0
    mixed = shape * scale + jnp.where(even, column[0], column[1]) * edge_lane
    value = few_rows(at_x, split(mixed * inverse))
    return value + hat_x[0] * edge_green[:SIDE] + hat_x[1] * edge_green[SIDE:]


def source_block(k, hat_z, hat_y, last, edge_y, edge_z, edge_lane):
    ky = lax.broadcasted_iota(jnp.int32, (SIDE, 256), 0)
    value = hat_z[(k % 2) * SIDE : (k % 2 + 1) * SIDE] * edge_z[k : k + 1, :]
    side = jnp.where(ky % 2 == 0, hat_y[k : k + 1, :], hat_y[SIDE + k : SIDE + k + 1, :])
    value += side * edge_y
    value += last[0][:, k : k + 1] * edge_lane[0] + last[1][:, k : k + 1] * edge_lane[1]
    return value


def offset(axis, i):
    if axis == "gy":
        return 8 + (1 - 2 * (i % 2)) * ((i + 1) // 2)
    j = i // 2
    return 4 + (1 - 2 * (j % 2)) * ((j + 1) // 2) + 8 * (i % 2) + 8 * (i // 14)


def start_all(phase, source, target, axis, me, send_sem, recv_sem, rows):
    def body(i, carry):
        d = offset(axis, i)
        copy_of(phase, source, target, axis, me, send_sem, recv_sem, rows, d).start()
        return carry

    lax.fori_loop(0, SIDE - 1, body, 0)


def copy_of(phase, source, target, axis, me, send_sem, recv_sem, rows, d):
    peer = lax.rem(me + d, SIDE)
    if rows is None:
        src = source
    else:
        src = source.at[pl.ds(pl.multiple_of(peer * rows, rows), rows), :]
    count = source.shape[0] if rows is None else rows
    return pltpu.make_async_remote_copy(
        src_ref=src,
        dst_ref=target.at[pl.ds(pl.multiple_of(me * count, count), count), :],
        send_sem=send_sem.at[phase, d],
        recv_sem=recv_sem.at[phase, d],
        device_id={axis: peer},
        device_id_type=MESH,
    )


def finish_all(phase, source, target, axis, me, send_sem, recv_sem, rows, sent):
    def body(d, carry):
        copy = copy_of(phase, source, target, axis, me, send_sem, recv_sem, rows, d)
        if sent:
            copy.wait_send()
        else:
            copy.wait_recv()
        return carry

    lax.fori_loop(1, SIDE, body, 0)


def sum_slots(ref):
    total = ref[0:8, :]
    for slot in range(1, SIDE):
        total += ref[slot * 8 : (slot + 1) * 8, :]
    return total


def unpack(plain, narrow, cut):
    return dict(
        eigen_wide=cut(plain, 0, 256, 0, 128),
        edge_wide=cut(plain, 0, 256, 128, 256),
        lane_rows=cut(plain, 256, 264, 0, 256),
        basis_rows=cut(plain, 264, 288, 0, 256),
        gather=[
            cut(plain, 288 + SLOTS * (r // 2), 288 + SLOTS * (r // 2 + 1), r % 2 * 128, r % 2 * 128 + 128)
            for r in range(8)
        ],
        spread=(cut(plain, 480, 864, 0, 256), cut(plain, 864, 912, 0, 256)),
        root=cut(plain, 912, 1168, 0, 256),
        sine_high=cut(narrow, 0, 256, 0, 256),
        sine_low=cut(narrow, 256, 512, 0, 256),
        basis_high=cut(narrow, 512, 768, 0, 128),
        basis_low=cut(narrow, 512, 768, 128, 256),
        select=[cut(narrow, 768 + 96 * t, 864 + 96 * t, 0, 256) for t in range(4)],
        column_high=cut(narrow, 1152, 1408, 0, 256),
        column_low=cut(narrow, 1408, 1664, 0, 256),
        heads=[cut(narrow, 1664, 1920, 128 * odd, 128 * odd + 128) for odd in range(2)],
    )


def kernel(charge_hbm, plain_hbm, narrow_hbm, out_ref, energy_ref, *scratch):
    charge, plain, narrow = scratch[:3]
    sends = scratch[3:7]
    lands = scratch[7:11]
    (
        mats, field_ref, inverse, shape_z, expand_high, expand_low, expand_z, pair_sum, half_rows,
        green, folded, hats, extra, turned_y, power, own, onehot, small_send, small_land, local_sem,
        send_sem, recv_sem,
    ) = scratch[11:]
    table = unpack(plain, narrow, lambda ref, a, b, c, d: ref.at[a:b, c:d])
    eigen_wide, edge_wide, lane_rows = table["eigen_wide"], table["edge_wide"], table["lane_rows"]
    sine_high, sine_low, select = table["sine_high"], table["sine_low"], table["select"]
    p = lax.axis_index("gx")
    q = lax.axis_index("gy")

    pieces = (
        (charge_hbm, charge),
        (narrow_hbm.at[0:512, :], narrow.at[0:512, :]),
        (narrow_hbm.at[512:1920, :], narrow.at[512:1920, :]),
        (plain_hbm, plain),
    )
    copies = [
        pltpu.make_async_copy(source, target, local_sem.at[i])
        for i, (source, target) in enumerate(pieces)
    ]
    for copy in copies:
        copy.start()

    barrier = pltpu.get_barrier_semaphore()

    def greet(d, carry):
        pl.semaphore_signal(
            barrier, inc=1, device_id={"gx": lax.rem(p + d, SIDE)}, device_id_type=MESH
        )
        pl.semaphore_signal(
            barrier, inc=1, device_id={"gy": lax.rem(q + d, SIDE)}, device_id_type=MESH
        )
        return carry

    lax.fori_loop(1, SIDE, greet, 0)

    def at(index):
        return pl.ds(pl.multiple_of(index * SIDE, SIDE), SIDE)

    def sines():
        return sine_high[...], sine_low[...]

    def launch(phase, value, axis, me, ready=None):
        sends[phase][...] = dot3(sines(), split(value), NT)
        if ready is not None:
            ready()
        start_all(phase, sends[phase], lands[phase], axis, me, send_sem, recv_sem, SIDE)
        lands[phase][at(me), :] = sends[phase][at(me), :]

    def collect(phase, axis, me, strided, added=None):
        finish_all(phase, sends[phase], lands[phase], axis, me, send_sem, recv_sem, SIDE, False)
        land = lands[phase]

        def load(a, h):
            return land[a * SIDE : (a + 1) * SIDE, h * HALF : (h + 1) * HALF]

        def store(g, h, piece):
            if added is not None:
                piece += added[g * SIDE : (g + 1) * SIDE, h * HALF : (h + 1) * HALF]
            if strided:
                mats[h][pl.ds(g, SIDE, stride=SIDE), :] = piece
            else:
                mats[h][g * SIDE : (g + 1) * SIDE, :] = piece

        regroup(load, store, lambda v, amount: pltpu.roll(v, amount, 1))

    def mat():
        return jnp.concatenate([mats[0][...], mats[1][...]], axis=1)

    def small(phase, index, value, axis, me):
        small_send[index][...] = value
        start_all(phase, small_send[index], small_land[index], axis, me, send_sem, recv_sem, None)
        small_land[index][pl.ds(pl.multiple_of(me * 8, 8), 8), :] = value

    def small_total(phase, index, axis, me):
        finish_all(
            phase, small_send[index], small_land[index], axis, me, send_sem, recv_sem, None, False
        )
        return sum_slots(small_land[index])

    cube = ((N + 1) / 2.0) ** 3

    def lead_rows():
        near = sine_high[at(p), :].astype(F32) + sine_low[at(p), :].astype(F32)
        return split(green_rows(near, table["basis_rows"][...]))

    def fill(k, lead):
        whole = 1.0 / ((pair_sum[...] + own[pl.ds(k, 1), :]) * cube)
        inverse[k] = whole
        green[k] = dot3(lead, split(whole))
        return lead

    def prepare():
        copies[2].wait()
        copies[3].wait()
        for tile in range(4):
            lanes = slice(tile * 256, (tile + 1) * 256)
            chosen = select[tile]
            basis = (table["basis_high"][...][:, :32], table["basis_low"][...][:, :32])
            expand_high[:, lanes] = dot(basis[0], chosen[32:64, :]).astype(BF16)
            expand_low[:, lanes] = dot(basis[1], chosen[32:64, :]).astype(BF16)
            near = (table["basis_high"][at(q), :][:, :32], table["basis_low"][at(q), :][:, :32])
            expand_z[:, lanes] = dot(near[0], chosen[64:96, :]) + dot(near[1], chosen[64:96, :])
        for half in range(2):
            lanes = slice(half * HALF, (half + 1) * HALF)
            own[0:SIDE, lanes] = eigen_wide[at(q), :]
            own[SIDE : 2 * SIDE, lanes] = edge_wide[at(q), :]
        pair_sum[:, :HALF] = eigen_wide[...] + lane_rows[0:1, :HALF]
        pair_sum[:, HALF:] = eigen_wide[...] + lane_rows[0:1, HALF:]
        lax.fori_loop(0, EARLY, fill, lead_rows())
        pl.semaphore_wait(barrier, 2 * (SIDE - 1))

    def drain_big(phase, axis, me):
        finish_all(phase, sends[phase], lands[phase], axis, me, send_sem, recv_sem, SIDE, True)

    def drain_small(phase, index, axis, me):
        finish_all(
            phase, small_send[index], small_land[index], axis, me, send_sem, recv_sem, None, True
        )

    copies[0].wait()
    copies[1].wait()
    launch(0, charge[...], "gy", q, prepare)
    lax.fori_loop(EARLY, SIDE, fill, lead_rows())

    collect(0, "gy", q, True)
    launch(1, mat(), "gx", p)
    half_rows[...] = dot3(split(mat()), sines())

    def fold(k, carry):
        folded[pl.ds(pl.multiple_of(k * WIDE, 8), WIDE), :] = weighted_rows(
            green[k], half_rows[at(k), :]
        )
        return carry

    lax.fori_loop(0, SIDE, fold, 0)
    entries = local_entries(folded[...], (expand_high, expand_low), expand_z, select)
    small(4, 0, jnp.concatenate(entries, axis=0), "gy", q)
    onehot[...] = owner_map()
    root = table["root"][...]
    square = root * root
    fourth = square * square
    power[...] = fourth * fourth * (fourth * (square * root))
    drain_big(0, "gy", q)
    small(5, 1, small_total(4, 0, "gy", q), "gx", p)

    collect(1, "gx", p, False)
    value = dot3(split(mat()), sines())
    field = value * jnp.concatenate([inverse[k, at(p), :] for k in range(SIDE)], axis=0)
    field_ref[...] = field
    launch(2, field, "gx", p)
    energy = jnp.sum(jnp.sum(value * field, axis=1, keepdims=True), axis=0, keepdims=True)
    entries = small_total(5, 1, "gx", p)

    at_x = at_y = (sine_high[at(p), :], sine_low[at(p), :])
    at_z = (sine_high[at(q), :], sine_low[at(q), :])
    planes = surface_planes(
        entries, table["gather"], table["spread"], onehot[...],
        (table["column_high"][...], table["column_low"][...]), table["heads"],
        table["root"][...], power[...],
    )
    hat_y, turned, hat_x, near_x, near_z = side_hats(planes, at_y, at_z, sines())
    edge_y = edge_wide[at(p), :]
    edge_y = jnp.concatenate([edge_y, edge_y], axis=1)
    edge_z = own[SIDE : 2 * SIDE, :]
    edge_lane = (lane_rows[1:2, :], lane_rows[2:3, :])
    cross = jnp.zeros((SIDE, 256), F32)
    for k in range(SIDE):
        cross += field_ref[k * SIDE : (k + 1) * SIDE, :] * source_block(
            k, near_z, hat_y, near_x, edge_y, edge_z, edge_lane
        )
    second = energy + jnp.sum(jnp.sum(cross, axis=1, keepdims=True), axis=0, keepdims=True)
    lane = lax.broadcasted_iota(jnp.int32, (8, HALF), 1)
    small(6, 2, jnp.where(lane == 0, energy, second), "gx", p)

    for n in range(2):
        shape_z[n] = dot3(sines(), split(dot3(sines(), planes[n])), NT)
    hats[...] = hat_x
    turned_y[:, : 2 * SIDE] = turned

    def correct(k, carry):
        rolled = pltpu.roll(turned_y[...], HALF - k, 1)
        extra[at(k), :] = corrected(
            shape_z[lax.rem(k, 2)],
            own[pl.ds(SIDE + k, 1), :],
            (rolled[:, 0:1], rolled[:, SIDE : SIDE + 1]),
            lane_rows[3:4, :],
            (hats[pl.ds(k, 1), :], hats[pl.ds(SIDE + k, 1), :]),
            inverse[k],
            green[k, SIDE * WIDE :, :],
            at_x,
        )
        return carry

    lax.fori_loop(0, SIDE, correct, 0)
    collect(2, "gx", p, True, extra)
    launch(3, mat(), "gy", q)
    drain_big(1, "gx", p)
    drain_big(2, "gx", p)
    drain_small(4, 0, "gy", q)
    drain_small(5, 1, "gx", p)
    small(7, 3, small_total(6, 2, "gx", p), "gy", q)
    drain_small(6, 2, "gx", p)
    collect(3, "gy", q, False)
    out_ref[...] = dot3(split(mat()), sines())
    drain_big(3, "gy", q)
    energy_ref[...] = small_total(7, 3, "gy", q) * (1.0 / (N + 1)) ** 3
    drain_small(7, 3, "gy", q)


def constants():
    sine_rows, eigen, basis, select, gather, spread, columns, rows, root, power = build_tables()

    def pair(table):
        table = table.astype(np.float32)
        high = table.astype(jnp.bfloat16)
        return high, (table - high.astype(np.float32)).astype(jnp.bfloat16)

    parity = np.arange(N) % 2
    lane_rows = np.zeros((8, N))
    lane_rows[0] = eigen
    lane_rows[1] = sine_rows[0] * (parity == 0)
    lane_rows[2] = sine_rows[0] * (parity == 1)
    lane_rows[3] = sine_rows[0]
    heads = []
    for odd in range(2):
        tables = [trig(parity_of, odd, np.arctan(2.0 * (np.arange(N) - (N - 1) / 2.0) / (N + 1))) for parity_of in range(2)]
        wide = np.zeros((N, 32))
        for k, table in enumerate(tables):
            wide[:, 16 * k : 16 * k + table.shape[0]] = table.T
        high, low = pair(wide)
        heads.append(np.concatenate([high, high, low, low], axis=1))
    plain = np.concatenate(
        [
            np.concatenate([np.repeat(v[:, None], HALF, 1) for v in (eigen, sine_rows[0])], axis=1),
            lane_rows,
            basis.T[:WIDE],
            *[gather[:, 256 * t : 256 * (t + 1)] for t in range(4)],
            spread[:, :8].reshape(8 * SLOTS, 256),
            spread[:, 8],
            root,
        ],
        axis=0,
    ).astype(np.float32)
    wide = np.zeros((N, HALF - 32))
    high, low = pair(basis)
    narrow = np.concatenate(
        [
            *pair(sine_rows),
            np.concatenate([high, wide.astype(high.dtype), low, wide.astype(high.dtype)], axis=1),
            *[
                np.concatenate(list(select), axis=0)[:, 256 * t : 256 * (t + 1)].astype(jnp.bfloat16)
                for t in range(4)
            ],
            *pair(columns),
            np.concatenate(heads, axis=1),
        ],
        axis=0,
    )
    return plain, narrow


def solution(mesh):
    tables = constants()

    def shards(charge_density):
        cells_a, cells_b, length = charge_density.shape
        flat = charge_density.reshape(cells_a * cells_b, length)
        grid = pltpu.VMEM((256, 256), F32)
        potential, energies = pl.pallas_call(
            kernel,
            out_shape=(
                pltpu.VMEM((256, 256), F32),
                pltpu.VMEM((8, HALF), F32),
            ),
            in_specs=[pl.BlockSpec(memory_space=pl.ANY)] * 3,
            out_specs=(
                pl.BlockSpec(memory_space=pltpu.VMEM),
                pl.BlockSpec(memory_space=pltpu.VMEM),
            ),
            scratch_shapes=[
                grid,
                *[pltpu.VMEM(table.shape, table.dtype) for table in tables],
                *[grid] * 8,
                [pltpu.VMEM((256, HALF), F32)] * 2,
                grid,
                pltpu.VMEM((SIDE, 256, 256), F32),
                pltpu.VMEM((2, 256, 256), F32),
                pltpu.VMEM((256, LANES), BF16),
                pltpu.VMEM((256, LANES), BF16),
                pltpu.VMEM((SIDE, LANES), F32),
                grid,
                grid,
                pltpu.VMEM((SIDE, SIDE * WIDE + 2 * SIDE, 256), F32),
                pltpu.VMEM((SIDE * WIDE, 256), F32),
                pltpu.VMEM((2 * SIDE, 256), F32),
                grid,
                pltpu.VMEM((256, HALF), F32),
                grid,
                pltpu.VMEM((2 * SIDE, 256), F32),
                pltpu.VMEM((LANES, 256), BF16),
                [pltpu.VMEM((8, HALF), F32)] * 4,
                [pltpu.VMEM((8 * SIDE, HALF), F32)] * 4,
                pltpu.SemaphoreType.DMA((4,)),
                pltpu.SemaphoreType.DMA((8, SIDE)),
                pltpu.SemaphoreType.DMA((8, SIDE)),
            ],
            compiler_params=pltpu.CompilerParams(
                collective_id=0, has_side_effects=True, vmem_limit_bytes=VMEM_LIMIT
            ),
        )(flat, *[jnp.asarray(table) for table in tables])
        return potential.reshape(cells_a, cells_b, length), energies[0, :2]

    return jax.shard_map(
        shards,
        mesh=mesh,
        in_specs=(P("gx", "gy", None),),
        out_specs=(P("gx", "gy", None), P()),
        check_vma=False,
    )
```

```python
import math

import jax
import jax.numpy as jnp
import numpy as np
from jax import lax
from jax.experimental import pallas as pl
from jax.experimental.pallas import tpu as pltpu
from jax.sharding import PartitionSpec as P

ORDER = 16
N = 256
SLOTS = 48
LANES = 1024
SPARE = 7 * 128 + 112
ENERGY_LANE = 1023


def harmonics(x, y, z):
    cosine = {(0, 0): np.ones_like(x)}
    sine = {(0, 0): np.zeros_like(x)}
    for l in range(1, ORDER + 1):
        scale = 1.0 if l == 1 else math.sqrt((2 * l - 1) / (2.0 * l))
        c, s = cosine[l - 1, l - 1], sine[l - 1, l - 1]
        cosine[l, l] = scale * (x * c - y * s)
        sine[l, l] = scale * (x * s + y * c)
        for m in range(l):
            near = (2 * l - 1) / math.sqrt(l * l - m * m)
            far = math.sqrt((l - 1) ** 2 - m * m) / math.sqrt(l * l - m * m)
            for table in (cosine, sine):
                older = table[l - 2, m] if l - 2 >= m else 0.0
                table[l, m] = near * z * table[l - 1, m] - far * older
    return cosine, sine


def face_point(face, t, s):
    one = np.ones_like(t)
    return ((s, t, one), (s, one, t), (one, t, s))[face]


def face_parity(face, px, py, pz):
    return ((py, px, pz), (pz, px, py), (py, pz, px))[face]


def trig(parity, odd, angle):
    if odd:
        orders = np.arange(1, 16, 2)
    else:
        orders = np.arange(0, 17, 2) if parity == 0 else np.arange(2, 17, 2)
    wave = np.cos if parity == 0 else np.sin
    return wave(orders[:, None] * angle[None, :])


def build_tables():
    span = N + 1.0
    step = 1.0 / span
    radius = math.sqrt(3.0) / 2.0
    index = np.arange(N) + 1
    sine_rows = np.sin(np.pi * (index[:, None] * index[None, :] % (2 * N + 2)) / span)
    eigen = 4.0 * span * span * np.sin(np.pi * index / (2 * span)) ** 2
    scaled = 2.0 * (np.arange(N) - (N - 1) / 2.0) * step
    angle = np.arctan(scaled)

    terms = [[] for _ in range(8)]
    for l in range(ORDER + 1):
        for m in range(l + 1):
            terms[(m % 2) * 4 + (l - m) % 2].append((l, m, 0))
            if m:
                terms[((m - 1) % 2) * 4 + 2 + (l - m) % 2].append((l, m, 1))

    nodes, quad = np.polynomial.legendre.leggauss(24)
    legendre = np.polynomial.legendre.legvander(nodes, ORDER).T
    basis = np.zeros((N, 32))
    basis[:, : ORDER + 1] = sine_rows @ np.polynomial.legendre.legvander(scaled, ORDER)
    even = (np.arange(N) % 2 == 0).astype(np.float64)
    basis[:, 17] = sine_rows[0] * even
    basis[:, 18] = sine_rows[0] * (1.0 - even)
    project = legendre * quad[None, :] * (np.arange(ORDER + 1) + 0.5)[:, None]
    turns = 64
    circle = 2.0 * np.pi * np.arange(turns) / turns
    ones_t, ones_s = np.meshgrid(nodes, nodes, indexing="ij")
    alpha, beta = np.meshgrid(circle, circle, indexing="ij")
    solid, wave = [], []
    for face in range(3):
        x, y, z = face_point(face, ones_t, ones_s)
        r = np.sqrt(x * x + y * y + z * z)
        table = harmonics(x / r, y / r, z / r)
        solid.append((table, r / math.sqrt(3.0)))
        ca, sa, cb, sb = np.cos(alpha), np.sin(alpha), np.cos(beta), np.sin(beta)
        parts = (sa * cb, ca * sb, ca * cb)
        order = ((1, 0, 2), (1, 2, 0), (2, 0, 1))[face]
        x, y, z = (parts[k] for k in order)
        r = np.sqrt(x * x + y * y + z * z)
        safe = np.where(r < 1e-12, 1.0, r)
        wave.append((harmonics(x / safe, y / safe, z / safe), np.where(r < 1e-12, 0.0, r)))

    select = np.zeros((3, 32, LANES))
    gather = np.zeros((SLOTS, LANES))
    spread = np.zeros((SLOTS, 16, 256))
    columns = np.zeros((256, N))
    rows = np.zeros((8, 3, 16, N))
    spill = SPARE
    for group in range(8):
        px, py, pz = group >> 2 & 1, group >> 1 & 1, group & 1
        odd = (px + py + pz) % 2
        lane = group * 128
        for face in range(3):
            prow, pcol, normal = face_parity(face, px, py, pz)
            sign = 2.0 if normal == 0 else -2.0
            entries = [
                (i, j)
                for i in range(prow, ORDER + 1, 2)
                for j in range(pcol, ORDER + 1, 2)
                if i + j + normal <= ORDER - odd
            ]
            moments = {}
            for slot, (l, m, which) in enumerate(terms[group]):
                table, ratio = solid[face]
                values = ratio**l * table[which][l, m]
                moments[slot] = project @ values @ project.T
            for i, j in entries:
                if lane >= (group + 1) * 128 or (lane >= SPARE and group == 7):
                    position, spill = spill, spill + 1
                    assert group == 0
                else:
                    position, lane = lane, lane + 1
                axes = ((1, 0, 2), (2, 0, 1), (1, 2, 0))[face]
                select[axes[0], i, position] = 1.0
                select[axes[1], j, position] = 1.0
                select[axes[2], 17 + normal, position] = 1.0
                for slot in moments:
                    gather[slot, position] = step * sign * moments[slot][i, j]
            left = trig(prow, odd, circle)
            right = trig(pcol, odd, circle)
            left_unit = left / np.sum(left * left, axis=1, keepdims=True)
            right_unit = right / np.sum(right * right, axis=1, keepdims=True)
            base = group * 32 + face * 9
            for slot, (l, m, which) in enumerate(terms[group]):
                table, r = wave[face]
                values = r ** (ORDER - odd) * table[which][l, m]
                block = left_unit @ values @ right_unit.T
                weight = (1.0 if m == 0 else 2.0) / (4.0 * math.pi * radius * 1.1 ** (l + 1))
                block = block * weight * sign * span * span
                spread[slot, : block.shape[0], base : base + block.shape[1]] = block
            tail = trig(pcol, odd, angle)
            columns[base : base + tail.shape[0]] = tail
            head = trig(prow, odd, angle)
            rows[group, face, : head.shape[0]] = head
    assert spill < ENERGY_LANE
    root = 1.0 / np.sqrt(1.0 - np.outer(np.sin(angle) ** 2, np.sin(angle) ** 2))
    return sine_rows, eigen, basis, select, gather, spread, columns, rows, root, root**15

MESH = pl.DeviceIdType.MESH
SIDE = 16
WIDE = 24
EARLY = 0
UNROLL = 2
VMEM_LIMIT = 67043328 - 1024 * 1024
HALF = 128
F32 = jnp.float32
BF16 = jnp.bfloat16
NN = (((1,), (0,)), ((), ()))
NT = (((1,), (1,)), ((), ()))


def split(value):
    high = value.astype(BF16)
    return high, (value - high.astype(F32)).astype(BF16)


def dot(a, b, dims=NN):
    return lax.dot_general(a, b, dims, preferred_element_type=F32)


def dot3(a, b, dims=NN):
    return dot(a[0], b[0], dims) + (dot(a[0], b[1], dims) + dot(a[1], b[0], dims))


def regroup(load, store, roll):
    lane = lax.broadcasted_iota(jnp.int32, (4 * SIDE, HALF), 1)
    rows = [
        jnp.concatenate([load(8 * a + i, h) for a in range(2) for h in range(2)], axis=0)
        for i in range(8)
    ]
    for step in (4, 2, 1):
        keep = (lane // (SIDE * step)) % 2 == 0
        for i in range(8):
            if i & step == 0:
                one, two = rows[i], rows[i + step]
                rows[i] = jnp.where(keep, one, roll(two, SIDE * step))
                rows[i + step] = jnp.where(keep, roll(one, HALF - SIDE * step), two)
    for i in range(8):
        for a in range(2):
            for h in range(2):
                part = 2 * a + h
                store(8 * h + i, a, rows[i][part * SIDE : (part + 1) * SIDE])


def green_rows(sines, basis_rows):
    rows = [sines[x : x + 1, :] * basis_rows for x in range(SIDE)]
    return jnp.concatenate(rows + [sines * basis_rows[17:18], sines * basis_rows[18:19]], axis=0)


def weighted_rows(table, values):
    total = table[:WIDE] * values[0:1, :]
    for x in range(1, SIDE):
        total += table[x * WIDE : (x + 1) * WIDE] * values[x : x + 1, :]
    return total


def local_entries(folded, expand_y, expand_z, select):
    pieces = split(folded)
    outcome = []
    for tile in range(4):
        lanes = slice(tile * 256, (tile + 1) * 256)
        mixed = dot3(pieces, (expand_y[0][:, lanes], expand_y[1][:, lanes]))
        total = mixed[:WIDE] * expand_z[0:1, lanes]
        for k in range(1, SIDE):
            total += mixed[k * WIDE : (k + 1) * WIDE] * expand_z[k : k + 1, lanes]
        chosen = select[tile][0:32, :].astype(F32)[:WIDE]
        summed = jnp.sum(total * chosen, axis=0, keepdims=True)
        outcome += [summed[:, :HALF], summed[:, HALF:]]
    return outcome


def owner_map():
    row = lax.broadcasted_iota(jnp.int32, (LANES, 256), 0)
    lane = lax.broadcasted_iota(jnp.int32, (LANES, 256), 1)
    owner = jnp.where(row >= SPARE, 0, row // HALF)
    return jnp.where(owner == lane // 32, 1.0, 0.0).astype(BF16)


def surface_planes(entries, gather, spread, onehot, columns, heads, root, power):
    product = jnp.concatenate(
        [gather[r][...] * entries[r : r + 1, :] for r in range(8)], axis=1
    )
    high, rest = product.astype(BF16), None
    rest = product - high.astype(F32)
    middle = rest.astype(BF16)
    low = (rest - middle.astype(F32)).astype(BF16)
    moments = dot(high, onehot) + (dot(middle, onehot) + dot(low, onehot))
    shape = moments[0:1, :] * spread[0][0:8, :]
    for slot in range(1, 45):
        shape += moments[slot : slot + 1, :] * spread[0][slot * 8 : slot * 8 + 8, :]
    ninth = jnp.sum(moments * spread[1][...], axis=0, keepdims=True)
    below = lax.broadcasted_iota(jnp.int32, (8, 256), 0) == 0
    shape = jnp.concatenate([shape, jnp.where(below, ninth, 0.0)], axis=0)
    lane = lax.broadcasted_iota(jnp.int32, (SIDE, 256), 1)
    blocks = []
    for face in range(3):
        for normal in range(2):
            for odd in range(2):
                for head in range(2):
                    tail = (odd + normal + head) % 2
                    px, py, pz = (
                        (tail, head, normal),
                        (tail, normal, head),
                        (normal, head, tail),
                    )[face]
                    base = (px * 4 + py * 2 + pz) * 32 + face * 9
                    blocks.append(jnp.where((lane >= base) & (lane < base + 9), shape, 0.0))
    right = dot3(split(jnp.concatenate(blocks, axis=0)), columns)
    planes = []
    for face in range(3):
        for normal in range(2):
            parts = []
            for odd in range(2):
                start = ((face * 2 + normal) * 2 + odd) * 32
                high, low = split(right[start : start + 32])
                stack = jnp.concatenate([high, low, high, low], axis=0)
                parts.append(dot(heads[odd][...], stack))
            planes.append(split(power * (root * parts[0] + parts[1])))
    return planes


def few_rows(rows, matrix, dims=NN):
    both = dot(jnp.concatenate(rows, axis=0), matrix[0], dims)
    return both[:SIDE] + (both[SIDE:] + dot(rows[0], matrix[1], dims))


def side_hats(planes, at_y, at_z, sines):
    half_y = split(jnp.concatenate([few_rows(at_z, planes[2 + n]) for n in range(2)], axis=0))
    hat_y = dot3(half_y, sines)
    half = [few_rows(at_z, planes[4 + n], NT) for n in range(2)]
    hat_x = dot3(split(jnp.concatenate(half, axis=0)), sines)
    near_x = [dot3(at_y, split(half[n]), NT) for n in range(2)]
    half_z = split(jnp.concatenate([few_rows(at_y, planes[n]) for n in range(2)], axis=0))
    return hat_y, hat_x, near_x, dot3(half_z, sines)


def corrected(shape, scale, hat_y, edge, hat_x, inverse, edge_green, at_x):
    even = lax.broadcasted_iota(jnp.int32, (256, 256), 0) % 2 == 0
    mixed = shape * scale + jnp.where(even, hat_y[0], hat_y[1]) * edge
    value = few_rows(at_x, split(mixed * inverse), NT)
    return value + hat_x[0] * edge_green[:SIDE] + hat_x[1] * edge_green[SIDE:]


def source_block(k, hat_z, hat_y, last, edge_y, edge_z, edge_lane):
    ky = lax.broadcasted_iota(jnp.int32, (SIDE, 256), 0)
    value = hat_z[(k % 2) * SIDE : (k % 2 + 1) * SIDE] * edge_z[k : k + 1, :]
    side = jnp.where(ky % 2 == 0, hat_y[k : k + 1, :], hat_y[SIDE + k : SIDE + k + 1, :])
    value += side * edge_y
    value += last[0][:, k : k + 1] * edge_lane[0] + last[1][:, k : k + 1] * edge_lane[1]
    return value


FAR = {
    "gx": (4, 12, 3, 11, 5, 13, 2, 10, 6, 14, 1, 9, 7, 15, 8),
    "gy": (8, 7, 9, 6, 10, 5, 11, 4, 12, 3, 13, 2, 14, 1, 15),
}


def start_all(phase, source, target, axis, me, send_sem, recv_sem, rows):
    for d in FAR[axis]:
        peer = lax.rem(me + d, SIDE)
        count = source.shape[0] if rows is None else rows
        src = source if rows is None else source.at[pl.ds(pl.multiple_of(peer * rows, rows), rows), :]
        pltpu.make_async_remote_copy(
            src_ref=src,
            dst_ref=target.at[pl.ds(pl.multiple_of(me * count, count), count), :],
            send_sem=send_sem.at[phase],
            recv_sem=recv_sem.at[phase],
            device_id={axis: peer},
            device_id_type=MESH,
        ).start()


def whole_of(phase, target, axis, me, send_sem, recv_sem):
    rows = target.shape[0] // SIDE * (SIDE - 1)
    return pltpu.make_async_remote_copy(
        src_ref=target.at[0:rows, :],
        dst_ref=target.at[0:rows, :],
        send_sem=send_sem.at[phase],
        recv_sem=recv_sem.at[phase],
        device_id={axis: lax.rem(me + 1, SIDE)},
        device_id_type=MESH,
    )


def sum_slots(ref):
    total = ref[0:8, :]
    for slot in range(1, SIDE):
        total += ref[slot * 8 : (slot + 1) * 8, :]
    return total


def unpack(plain, narrow, cut):
    return dict(
        eigen_wide=cut(plain, 0, 256, 0, 128),
        edge_wide=cut(plain, 0, 256, 128, 256),
        lane_rows=cut(plain, 256, 264, 0, 256),
        basis_rows=cut(plain, 264, 288, 0, 256),
        gather=[
            cut(plain, 288 + SLOTS * (r // 2), 288 + SLOTS * (r // 2 + 1), r % 2 * 128, r % 2 * 128 + 128)
            for r in range(8)
        ],
        spread=(cut(plain, 480, 864, 0, 256), cut(plain, 864, 912, 0, 256)),
        root=cut(plain, 912, 1168, 0, 256),
        sine_high=cut(narrow, 0, 256, 0, 256),
        sine_low=cut(narrow, 256, 512, 0, 256),
        basis_high=cut(narrow, 512, 768, 0, 128),
        basis_low=cut(narrow, 512, 768, 128, 256),
        select=[cut(narrow, 768 + 96 * t, 864 + 96 * t, 0, 256) for t in range(4)],
        column_high=cut(narrow, 1152, 1408, 0, 256),
        column_low=cut(narrow, 1408, 1664, 0, 256),
        heads=[cut(narrow, 1664, 1920, 128 * odd, 128 * odd + 128) for odd in range(2)],
    )


def kernel(charge_hbm, plain_hbm, narrow_hbm, out_ref, energy_ref, *scratch):
    charge, plain, narrow = scratch[:3]
    sends = scratch[3:7]
    lands = scratch[7:11]
    (
        mats, field_ref, inverse, shape_z, expand_high, expand_low, expand_z, pair_sum, half_rows,
        green, folded, hats, extra, power, own, onehot, small_send, small_land, local_sem,
        send_sem, recv_sem,
    ) = scratch[11:]
    table = unpack(plain, narrow, lambda ref, a, b, c, d: ref.at[a:b, c:d])
    eigen_wide, edge_wide, lane_rows = table["eigen_wide"], table["edge_wide"], table["lane_rows"]
    sine_high, sine_low, select = table["sine_high"], table["sine_low"], table["select"]
    p = lax.axis_index("gx")
    q = lax.axis_index("gy")

    pieces = (
        (charge_hbm, charge),
        (narrow_hbm.at[0:512, :], narrow.at[0:512, :]),
        (narrow_hbm.at[512:1920, :], narrow.at[512:1920, :]),
        (plain_hbm, plain),
    )
    copies = [
        pltpu.make_async_copy(source, target, local_sem.at[i])
        for i, (source, target) in enumerate(pieces)
    ]
    for copy in copies:
        copy.start()

    barrier = pltpu.get_barrier_semaphore()

    def greet(d, carry):
        pl.semaphore_signal(
            barrier, inc=1, device_id={"gx": lax.rem(p + d, SIDE)}, device_id_type=MESH
        )
        pl.semaphore_signal(
            barrier, inc=1, device_id={"gy": lax.rem(q + d, SIDE)}, device_id_type=MESH
        )
        return carry

    lax.fori_loop(1, SIDE, greet, 0)

    def at(index):
        return pl.ds(pl.multiple_of(index * SIDE, SIDE), SIDE)

    def sines():
        return sine_high[...], sine_low[...]

    def launch(phase, value, axis, me, ready=None):
        sends[phase][...] = dot3(sines(), split(value), NT)
        if ready is not None:
            ready()
        start_all(phase, sends[phase], lands[phase], axis, me, send_sem, recv_sem, SIDE)
        lands[phase][at(me), :] = sends[phase][at(me), :]

    def collect(phase, axis, me, strided, added=None):
        whole_of(phase, lands[phase], axis, me, send_sem, recv_sem).wait_recv()
        land = lands[phase]

        def load(a, h):
            return land[a * SIDE : (a + 1) * SIDE, h * HALF : (h + 1) * HALF]

        def store(g, h, piece):
            if added is not None:
                piece += added[g * SIDE : (g + 1) * SIDE, h * HALF : (h + 1) * HALF]
            if strided:
                mats[h][pl.ds(g, SIDE, stride=SIDE), :] = piece
            else:
                mats[h][g * SIDE : (g + 1) * SIDE, :] = piece

        regroup(load, store, lambda v, amount: pltpu.roll(v, amount, 1))

    def mat():
        return jnp.concatenate([mats[0][...], mats[1][...]], axis=1)

    def small(phase, index, value, axis, me):
        small_send[index][...] = value
        start_all(phase, small_send[index], small_land[index], axis, me, send_sem, recv_sem, None)
        small_land[index][pl.ds(pl.multiple_of(me * 8, 8), 8), :] = value

    def small_total(phase, index, axis, me):
        whole_of(phase, small_land[index], axis, me, send_sem, recv_sem).wait_recv()
        return sum_slots(small_land[index])

    cube = ((N + 1) / 2.0) ** 3

    def lead_rows():
        near = sine_high[at(p), :].astype(F32) + sine_low[at(p), :].astype(F32)
        return split(green_rows(near, table["basis_rows"][...]))

    def fill(k, lead):
        whole = 1.0 / ((pair_sum[...] + own[pl.ds(k, 1), :]) * cube)
        inverse[k] = whole
        green[k] = dot3(lead, split(whole))
        return lead

    def prepare():
        copies[2].wait()
        copies[3].wait()
        for tile in range(4):
            lanes = slice(tile * 256, (tile + 1) * 256)
            chosen = select[tile]
            basis = (table["basis_high"][...][:, :32], table["basis_low"][...][:, :32])
            expand_high[:, lanes] = dot(basis[0], chosen[32:64, :]).astype(BF16)
            expand_low[:, lanes] = dot(basis[1], chosen[32:64, :]).astype(BF16)
            near = (table["basis_high"][at(q), :][:, :32], table["basis_low"][at(q), :][:, :32])
            expand_z[:, lanes] = dot(near[0], chosen[64:96, :]) + dot(near[1], chosen[64:96, :])
        for half in range(2):
            lanes = slice(half * HALF, (half + 1) * HALF)
            own[0:SIDE, lanes] = eigen_wide[at(q), :]
            own[SIDE : 2 * SIDE, lanes] = edge_wide[at(q), :]
        pair_sum[:, :HALF] = eigen_wide[...] + lane_rows[0:1, :HALF]
        pair_sum[:, HALF:] = eigen_wide[...] + lane_rows[0:1, HALF:]
        lax.fori_loop(0, EARLY, fill, lead_rows())
        pl.semaphore_wait(barrier, 2 * (SIDE - 1))

    def drain_big(phase, axis, me):
        whole_of(phase, lands[phase], axis, me, send_sem, recv_sem).wait_send()

    def drain_small(phase, index, axis, me):
        whole_of(phase, small_land[index], axis, me, send_sem, recv_sem).wait_send()

    copies[0].wait()
    copies[1].wait()
    launch(0, charge[...], "gy", q, prepare)
    lax.fori_loop(EARLY, SIDE, fill, lead_rows())

    collect(0, "gy", q, True)
    launch(1, mat(), "gx", p)
    half_rows[...] = dot3(split(mat()), sines())

    def fold(k, carry):
        folded[pl.ds(pl.multiple_of(k * WIDE, 8), WIDE), :] = weighted_rows(
            green[k], half_rows[at(k), :]
        )
        return carry

    lax.fori_loop(0, SIDE, fold, 0)
    entries = local_entries(folded[...], (expand_high, expand_low), expand_z, select)
    small(4, 0, jnp.concatenate(entries, axis=0), "gy", q)
    onehot[...] = owner_map()
    root = table["root"][...]
    square = root * root
    fourth = square * square
    power[...] = fourth * fourth * (fourth * (square * root))
    drain_big(0, "gy", q)
    small(5, 1, small_total(4, 0, "gy", q), "gx", p)

    collect(1, "gx", p, False)
    value = dot3(split(mat()), sines())
    field = value * jnp.concatenate([inverse[k, at(p), :] for k in range(SIDE)], axis=0)
    field_ref[...] = field
    launch(2, field, "gx", p)
    energy = jnp.sum(jnp.sum(value * field, axis=1, keepdims=True), axis=0, keepdims=True)
    entries = small_total(5, 1, "gx", p)

    at_x = at_y = (sine_high[at(p), :], sine_low[at(p), :])
    at_z = (sine_high[at(q), :], sine_low[at(q), :])
    planes = surface_planes(
        entries, table["gather"], table["spread"], onehot[...],
        (table["column_high"][...], table["column_low"][...]), table["heads"],
        table["root"][...], power[...],
    )
    hat_y, hat_x, near_x, near_z = side_hats(planes, at_y, at_z, sines())
    edge_y = edge_wide[at(p), :]
    edge_y = jnp.concatenate([edge_y, edge_y], axis=1)
    edge_z = own[SIDE : 2 * SIDE, :]
    edge_lane = (lane_rows[1:2, :], lane_rows[2:3, :])
    cross = jnp.zeros((SIDE, 256), F32)
    for k in range(SIDE):
        cross += field_ref[k * SIDE : (k + 1) * SIDE, :] * source_block(
            k, near_z, hat_y, near_x, edge_y, edge_z, edge_lane
        )
    second = energy + jnp.sum(jnp.sum(cross, axis=1, keepdims=True), axis=0, keepdims=True)
    lane = lax.broadcasted_iota(jnp.int32, (8, HALF), 1)
    small(6, 2, jnp.where(lane == 0, energy, second), "gx", p)

    for n in range(2):
        shape_z[n] = dot3(split(dot3(sines(), planes[n])), sines())
    hats[0] = hat_y
    hats[1] = hat_x
    edge = jnp.concatenate([edge_wide[...], edge_wide[...]], axis=1)

    def correct(k, carry):
        extra[at(k), :] = corrected(
            shape_z[lax.rem(k, 2)],
            own[pl.ds(SIDE + k, 1), :],
            (hats[0, pl.ds(k, 1), :], hats[0, pl.ds(SIDE + k, 1), :]),
            edge,
            (hats[1, pl.ds(k, 1), :], hats[1, pl.ds(SIDE + k, 1), :]),
            inverse[k],
            green[k, SIDE * WIDE :, :],
            at_x,
        )
        return carry

    lax.fori_loop(0, SIDE, correct, 0, unroll=UNROLL)
    collect(2, "gx", p, True, extra)
    launch(3, mat(), "gy", q)
    drain_big(1, "gx", p)
    drain_big(2, "gx", p)
    drain_small(4, 0, "gy", q)
    drain_small(5, 1, "gx", p)
    small(7, 3, small_total(6, 2, "gx", p), "gy", q)
    drain_small(6, 2, "gx", p)
    collect(3, "gy", q, False)
    out_ref[...] = dot3(split(mat()), sines())
    drain_big(3, "gy", q)
    energy_ref[...] = small_total(7, 3, "gy", q) * (1.0 / (N + 1)) ** 3
    drain_small(7, 3, "gy", q)


def constants():
    sine_rows, eigen, basis, select, gather, spread, columns, rows, root, power = build_tables()

    def pair(table):
        table = table.astype(np.float32)
        high = table.astype(jnp.bfloat16)
        return high, (table - high.astype(np.float32)).astype(jnp.bfloat16)

    parity = np.arange(N) % 2
    lane_rows = np.zeros((8, N))
    lane_rows[0] = eigen
    lane_rows[1] = sine_rows[0] * (parity == 0)
    lane_rows[2] = sine_rows[0] * (parity == 1)
    lane_rows[3] = sine_rows[0]
    heads = []
    for odd in range(2):
        tables = [trig(parity_of, odd, np.arctan(2.0 * (np.arange(N) - (N - 1) / 2.0) / (N + 1))) for parity_of in range(2)]
        wide = np.zeros((N, 32))
        for k, table in enumerate(tables):
            wide[:, 16 * k : 16 * k + table.shape[0]] = table.T
        high, low = pair(wide)
        heads.append(np.concatenate([high, high, low, low], axis=1))
    plain = np.concatenate(
        [
            np.concatenate([np.repeat(v[:, None], HALF, 1) for v in (eigen, sine_rows[0])], axis=1),
            lane_rows,
            basis.T[:WIDE],
            *[gather[:, 256 * t : 256 * (t + 1)] for t in range(4)],
            spread[:, :8].reshape(8 * SLOTS, 256),
            spread[:, 8],
            root,
        ],
        axis=0,
    ).astype(np.float32)
    wide = np.zeros((N, HALF - 32))
    high, low = pair(basis)
    narrow = np.concatenate(
        [
            *pair(sine_rows),
            np.concatenate([high, wide.astype(high.dtype), low, wide.astype(high.dtype)], axis=1),
            *[
                np.concatenate(list(select), axis=0)[:, 256 * t : 256 * (t + 1)].astype(jnp.bfloat16)
                for t in range(4)
            ],
            *pair(columns),
            np.concatenate(heads, axis=1),
        ],
        axis=0,
    )
    return plain, narrow


def solution(mesh):
    tables = constants()

    def shards(charge_density):
        cells_a, cells_b, length = charge_density.shape
        flat = charge_density.reshape(cells_a * cells_b, length)
        grid = pltpu.VMEM((256, 256), F32)
        potential, energies = pl.pallas_call(
            kernel,
            out_shape=(
                pltpu.VMEM((256, 256), F32),
                pltpu.VMEM((8, HALF), F32),
            ),
            in_specs=[pl.BlockSpec(memory_space=pl.ANY)] * 3,
            out_specs=(
                pl.BlockSpec(memory_space=pltpu.VMEM),
                pl.BlockSpec(memory_space=pltpu.VMEM),
            ),
            scratch_shapes=[
                grid,
                *[pltpu.VMEM(table.shape, table.dtype) for table in tables],
                *[grid] * 8,
                [pltpu.VMEM((256, HALF), F32)] * 2,
                grid,
                pltpu.VMEM((SIDE, 256, 256), F32),
                pltpu.VMEM((2, 256, 256), F32),
                pltpu.VMEM((256, LANES), BF16),
                pltpu.VMEM((256, LANES), BF16),
                pltpu.VMEM((SIDE, LANES), F32),
                grid,
                grid,
                pltpu.VMEM((SIDE, SIDE * WIDE + 2 * SIDE, 256), F32),
                pltpu.VMEM((SIDE * WIDE, 256), F32),
                pltpu.VMEM((2, 2 * SIDE, 256), F32),
                grid,
                grid,
                pltpu.VMEM((2 * SIDE, 256), F32),
                pltpu.VMEM((LANES, 256), BF16),
                [pltpu.VMEM((8, HALF), F32)] * 4,
                [pltpu.VMEM((8 * SIDE, HALF), F32)] * 4,
                pltpu.SemaphoreType.DMA((4,)),
                pltpu.SemaphoreType.DMA((8,)),
                pltpu.SemaphoreType.DMA((8,)),
            ],
            compiler_params=pltpu.CompilerParams(
                collective_id=0, has_side_effects=True, vmem_limit_bytes=VMEM_LIMIT
            ),
        )(flat, *[jnp.asarray(table) for table in tables])
        return potential.reshape(cells_a, cells_b, length), energies[0, :2]

    return jax.shard_map(
        shards,
        mesh=mesh,
        in_specs=(P("gx", "gy", None),),
        out_specs=(P("gx", "gy", None), P()),
        check_vma=False,
    )
```

```python
import math

import jax
import jax.numpy as jnp
import numpy as np
from jax import lax
from jax.experimental import pallas as pl
from jax.experimental.pallas import tpu as pltpu
from jax.sharding import PartitionSpec as P

ORDER = 16
N = 256
SLOTS = 48
LANES = 1024
SPARE = 7 * 128 + 112
ENERGY_LANE = 1023


def harmonics(x, y, z):
    cosine = {(0, 0): np.ones_like(x)}
    sine = {(0, 0): np.zeros_like(x)}
    for l in range(1, ORDER + 1):
        scale = 1.0 if l == 1 else math.sqrt((2 * l - 1) / (2.0 * l))
        c, s = cosine[l - 1, l - 1], sine[l - 1, l - 1]
        cosine[l, l] = scale * (x * c - y * s)
        sine[l, l] = scale * (x * s + y * c)
        for m in range(l):
            near = (2 * l - 1) / math.sqrt(l * l - m * m)
            far = math.sqrt((l - 1) ** 2 - m * m) / math.sqrt(l * l - m * m)
            for table in (cosine, sine):
                older = table[l - 2, m] if l - 2 >= m else 0.0
                table[l, m] = near * z * table[l - 1, m] - far * older
    return cosine, sine


def face_point(face, t, s):
    one = np.ones_like(t)
    return ((s, t, one), (s, one, t), (one, t, s))[face]


def face_parity(face, px, py, pz):
    return ((py, px, pz), (pz, px, py), (py, pz, px))[face]


def trig(parity, odd, angle):
    if odd:
        orders = np.arange(1, 16, 2)
    else:
        orders = np.arange(0, 17, 2) if parity == 0 else np.arange(2, 17, 2)
    wave = np.cos if parity == 0 else np.sin
    return wave(orders[:, None] * angle[None, :])


def build_tables():
    span = N + 1.0
    step = 1.0 / span
    radius = math.sqrt(3.0) / 2.0
    index = np.arange(N) + 1
    sine_rows = np.sin(np.pi * (index[:, None] * index[None, :] % (2 * N + 2)) / span)
    eigen = 4.0 * span * span * np.sin(np.pi * index / (2 * span)) ** 2
    scaled = 2.0 * (np.arange(N) - (N - 1) / 2.0) * step
    angle = np.arctan(scaled)

    terms = [[] for _ in range(8)]
    for l in range(ORDER + 1):
        for m in range(l + 1):
            terms[(m % 2) * 4 + (l - m) % 2].append((l, m, 0))
            if m:
                terms[((m - 1) % 2) * 4 + 2 + (l - m) % 2].append((l, m, 1))

    nodes, quad = np.polynomial.legendre.leggauss(24)
    legendre = np.polynomial.legendre.legvander(nodes, ORDER).T
    basis = np.zeros((N, 32))
    basis[:, : ORDER + 1] = sine_rows @ np.polynomial.legendre.legvander(scaled, ORDER)
    even = (np.arange(N) % 2 == 0).astype(np.float64)
    basis[:, 17] = sine_rows[0] * even
    basis[:, 18] = sine_rows[0] * (1.0 - even)
    project = legendre * quad[None, :] * (np.arange(ORDER + 1) + 0.5)[:, None]
    turns = 64
    circle = 2.0 * np.pi * np.arange(turns) / turns
    ones_t, ones_s = np.meshgrid(nodes, nodes, indexing="ij")
    alpha, beta = np.meshgrid(circle, circle, indexing="ij")
    solid, wave = [], []
    for face in range(3):
        x, y, z = face_point(face, ones_t, ones_s)
        r = np.sqrt(x * x + y * y + z * z)
        table = harmonics(x / r, y / r, z / r)
        solid.append((table, r / math.sqrt(3.0)))
        ca, sa, cb, sb = np.cos(alpha), np.sin(alpha), np.cos(beta), np.sin(beta)
        parts = (sa * cb, ca * sb, ca * cb)
        order = ((1, 0, 2), (1, 2, 0), (2, 0, 1))[face]
        x, y, z = (parts[k] for k in order)
        r = np.sqrt(x * x + y * y + z * z)
        safe = np.where(r < 1e-12, 1.0, r)
        wave.append((harmonics(x / safe, y / safe, z / safe), np.where(r < 1e-12, 0.0, r)))

    select = np.zeros((3, 32, LANES))
    gather = np.zeros((SLOTS, LANES))
    spread = np.zeros((SLOTS, 16, 256))
    columns = np.zeros((256, N))
    rows = np.zeros((8, 3, 16, N))
    spill = SPARE
    for group in range(8):
        px, py, pz = group >> 2 & 1, group >> 1 & 1, group & 1
        odd = (px + py + pz) % 2
        lane = group * 128
        for face in range(3):
            prow, pcol, normal = face_parity(face, px, py, pz)
            sign = 2.0 if normal == 0 else -2.0
            entries = [
                (i, j)
                for i in range(prow, ORDER + 1, 2)
                for j in range(pcol, ORDER + 1, 2)
                if i + j + normal <= ORDER - odd
            ]
            moments = {}
            for slot, (l, m, which) in enumerate(terms[group]):
                table, ratio = solid[face]
                values = ratio**l * table[which][l, m]
                moments[slot] = project @ values @ project.T
            for i, j in entries:
                if lane >= (group + 1) * 128 or (lane >= SPARE and group == 7):
                    position, spill = spill, spill + 1
                    assert group == 0
                else:
                    position, lane = lane, lane + 1
                axes = ((1, 0, 2), (2, 0, 1), (1, 2, 0))[face]
                select[axes[0], i, position] = 1.0
                select[axes[1], j, position] = 1.0
                select[axes[2], 17 + normal, position] = 1.0
                for slot in moments:
                    gather[slot, position] = step * sign * moments[slot][i, j]
            left = trig(prow, odd, circle)
            right = trig(pcol, odd, circle)
            left_unit = left / np.sum(left * left, axis=1, keepdims=True)
            right_unit = right / np.sum(right * right, axis=1, keepdims=True)
            base = group * 32 + face * 9
            for slot, (l, m, which) in enumerate(terms[group]):
                table, r = wave[face]
                values = r ** (ORDER - odd) * table[which][l, m]
                block = left_unit @ values @ right_unit.T
                weight = (1.0 if m == 0 else 2.0) / (4.0 * math.pi * radius * 1.1 ** (l + 1))
                block = block * weight * sign * span * span
                spread[slot, : block.shape[0], base : base + block.shape[1]] = block
            tail = trig(pcol, odd, angle)
            columns[base : base + tail.shape[0]] = tail
            head = trig(prow, odd, angle)
            rows[group, face, : head.shape[0]] = head
    assert spill < ENERGY_LANE
    root = 1.0 / np.sqrt(1.0 - np.outer(np.sin(angle) ** 2, np.sin(angle) ** 2))
    return sine_rows, eigen, basis, select, gather, spread, columns, rows, root, root**15

MESH = pl.DeviceIdType.MESH
SIDE = 16
WIDE = 24
EARLY = 0
UNROLL = 2
VMEM_LIMIT = 67043328 - 1024 * 1024
HALF = 128
F32 = jnp.float32
BF16 = jnp.bfloat16
NN = (((1,), (0,)), ((), ()))
NT = (((1,), (1,)), ((), ()))


def split(value):
    high = value.astype(BF16)
    return high, (value - high.astype(F32)).astype(BF16)


def dot(a, b, dims=NN):
    return lax.dot_general(a, b, dims, preferred_element_type=F32)


def dot3(a, b, dims=NN):
    return dot(a[0], b[0], dims) + (dot(a[0], b[1], dims) + dot(a[1], b[0], dims))


def regroup(load, store, roll):
    lane = lax.broadcasted_iota(jnp.int32, (4 * SIDE, HALF), 1)
    rows = [
        jnp.concatenate([load(8 * a + i, h) for a in range(2) for h in range(2)], axis=0)
        for i in range(8)
    ]
    for step in (4, 2, 1):
        keep = (lane // (SIDE * step)) % 2 == 0
        for i in range(8):
            if i & step == 0:
                one, two = rows[i], rows[i + step]
                rows[i] = jnp.where(keep, one, roll(two, SIDE * step))
                rows[i + step] = jnp.where(keep, roll(one, HALF - SIDE * step), two)
    for i in range(8):
        for a in range(2):
            for h in range(2):
                part = 2 * a + h
                store(8 * h + i, a, rows[i][part * SIDE : (part + 1) * SIDE])


def green_rows(sines, basis_rows):
    rows = [sines[x : x + 1, :] * basis_rows[:SIDE] for x in range(SIDE)]
    rows += [sines * basis_rows[f : f + 1] for f in range(SIDE, SIDE + 3)]
    return jnp.concatenate(rows, axis=0)


def weighted_rows(table, values):
    total = table[:SIDE] * values[0:1, :]
    for x in range(1, SIDE):
        total += table[x * SIDE : (x + 1) * SIDE] * values[x : x + 1, :]
    rows = [total]
    for f in range(SIDE, SIDE + 3):
        rows.append(jnp.sum(table[f * SIDE : (f + 1) * SIDE] * values, axis=0, keepdims=True))
    rows.append(jnp.zeros((WIDE - SIDE - 3, 256), F32))
    return jnp.concatenate(rows, axis=0)


def local_entries(folded, expand_y, expand_z, select):
    pieces = split(folded)
    outcome = []
    for tile in range(4):
        lanes = slice(tile * 256, (tile + 1) * 256)
        mixed = dot3(pieces, (expand_y[0][:, lanes], expand_y[1][:, lanes]))
        total = mixed[:WIDE] * expand_z[0:1, lanes]
        for k in range(1, SIDE):
            total += mixed[k * WIDE : (k + 1) * WIDE] * expand_z[k : k + 1, lanes]
        chosen = select[tile][0:32, :].astype(F32)[:WIDE]
        summed = jnp.sum(total * chosen, axis=0, keepdims=True)
        outcome += [summed[:, :HALF], summed[:, HALF:]]
    return outcome


def owner_map():
    row = lax.broadcasted_iota(jnp.int32, (LANES, 256), 0)
    lane = lax.broadcasted_iota(jnp.int32, (LANES, 256), 1)
    owner = jnp.where(row >= SPARE, 0, row // HALF)
    return jnp.where(owner == lane // 32, 1.0, 0.0).astype(BF16)


def surface_planes(entries, gather, spread, onehot, columns, heads, root, power):
    product = jnp.concatenate(
        [gather[r][...] * entries[r : r + 1, :] for r in range(8)], axis=1
    )
    high, rest = product.astype(BF16), None
    rest = product - high.astype(F32)
    middle = rest.astype(BF16)
    low = (rest - middle.astype(F32)).astype(BF16)
    moments = dot(jnp.concatenate([high, middle, low], axis=0), onehot)
    moments = moments[:SLOTS] + (moments[SLOTS : 2 * SLOTS] + moments[2 * SLOTS :])
    shape = moments[0:1, :] * spread[0][0:8, :]
    for slot in range(1, 45):
        shape += moments[slot : slot + 1, :] * spread[0][slot * 8 : slot * 8 + 8, :]
    ninth = jnp.sum(moments * spread[1][...], axis=0, keepdims=True)
    below = lax.broadcasted_iota(jnp.int32, (8, 256), 0) == 0
    shape = jnp.concatenate([shape, jnp.where(below, ninth, 0.0)], axis=0)
    lane = lax.broadcasted_iota(jnp.int32, (SIDE, 256), 1)
    blocks = []
    for face in range(3):
        for normal in range(2):
            for odd in range(2):
                for head in range(2):
                    tail = (odd + normal + head) % 2
                    px, py, pz = (
                        (tail, head, normal),
                        (tail, normal, head),
                        (normal, head, tail),
                    )[face]
                    base = (px * 4 + py * 2 + pz) * 32 + face * 9
                    blocks.append(jnp.where((lane >= base) & (lane < base + 9), shape, 0.0))
    right = dot3(split(jnp.concatenate(blocks, axis=0)), columns)
    planes = []
    for face in range(3):
        for normal in range(2):
            parts = []
            for odd in range(2):
                start = ((face * 2 + normal) * 2 + odd) * 32
                high, low = split(right[start : start + 32])
                stack = jnp.concatenate([high, low, high, low], axis=0)
                parts.append(dot(heads[odd][...], stack))
            planes.append(split(power * (root * parts[0] + parts[1])))
    return planes


def few_rows(rows, matrix, dims=NN):
    both = dot(jnp.concatenate(rows, axis=0), matrix[0], dims)
    return both[:SIDE] + (both[SIDE:] + dot(rows[0], matrix[1], dims))


def side_hats(planes, at_y, at_z, sines):
    half_y = split(jnp.concatenate([few_rows(at_z, planes[2 + n]) for n in range(2)], axis=0))
    hat_y = dot3(half_y, sines)
    half = [few_rows(at_z, planes[4 + n], NT) for n in range(2)]
    hat_x = dot3(split(jnp.concatenate(half, axis=0)), sines)
    near_x = [dot3(at_y, split(half[n]), NT) for n in range(2)]
    half_z = split(jnp.concatenate([few_rows(at_y, planes[n]) for n in range(2)], axis=0))
    return hat_y, hat_x, near_x, dot3(half_z, sines)


def corrected(shape, scale, hat_y, edge, hat_x, inverse, edge_green, at_x):
    even = lax.broadcasted_iota(jnp.int32, (256, 256), 0) % 2 == 0
    mixed = shape * scale + jnp.where(even, hat_y[0], hat_y[1]) * edge
    value = few_rows(at_x, split(mixed * inverse), NT)
    return value + hat_x[0] * edge_green[:SIDE] + hat_x[1] * edge_green[SIDE:]


def source_block(k, hat_z, hat_y, last, edge_y, edge_z, edge_lane):
    ky = lax.broadcasted_iota(jnp.int32, (SIDE, 256), 0)
    value = hat_z[(k % 2) * SIDE : (k % 2 + 1) * SIDE] * edge_z[k : k + 1, :]
    side = jnp.where(ky % 2 == 0, hat_y[k : k + 1, :], hat_y[SIDE + k : SIDE + k + 1, :])
    value += side * edge_y
    value += last[0][:, k : k + 1] * edge_lane[0] + last[1][:, k : k + 1] * edge_lane[1]
    return value


FAR = {
    "gx": (4, 12, 3, 11, 5, 13, 2, 10, 6, 14, 1, 9, 7, 15, 8),
    "gy": (8, 7, 9, 6, 10, 5, 11, 4, 12, 3, 13, 2, 14, 1, 15),
}


def start_all(phase, source, target, axis, me, send_sem, recv_sem, rows):
    for d in FAR[axis]:
        peer = lax.rem(me + d, SIDE)
        count = source.shape[0] if rows is None else rows
        src = source if rows is None else source.at[pl.ds(pl.multiple_of(peer * rows, rows), rows), :]
        pltpu.make_async_remote_copy(
            src_ref=src,
            dst_ref=target.at[pl.ds(pl.multiple_of(me * count, count), count), :],
            send_sem=send_sem.at[phase],
            recv_sem=recv_sem.at[phase],
            device_id={axis: peer},
            device_id_type=MESH,
        ).start()


def whole_of(phase, target, axis, me, send_sem, recv_sem):
    rows = target.shape[0] // SIDE * (SIDE - 1)
    return pltpu.make_async_remote_copy(
        src_ref=target.at[0:rows, :],
        dst_ref=target.at[0:rows, :],
        send_sem=send_sem.at[phase],
        recv_sem=recv_sem.at[phase],
        device_id={axis: lax.rem(me + 1, SIDE)},
        device_id_type=MESH,
    )


def sum_slots(ref):
    total = ref[0:8, :]
    for slot in range(1, SIDE):
        total += ref[slot * 8 : (slot + 1) * 8, :]
    return total


def unpack(plain, narrow, cut):
    return dict(
        eigen_wide=cut(plain, 0, 256, 0, 128),
        edge_wide=cut(plain, 0, 256, 128, 256),
        lane_rows=cut(plain, 256, 264, 0, 256),
        basis_rows=cut(plain, 264, 288, 0, 256),
        gather=[
            cut(plain, 288 + SLOTS * (r // 2), 288 + SLOTS * (r // 2 + 1), r % 2 * 128, r % 2 * 128 + 128)
            for r in range(8)
        ],
        spread=(cut(plain, 480, 864, 0, 256), cut(plain, 864, 912, 0, 256)),
        root=cut(plain, 912, 1168, 0, 256),
        sine_high=cut(narrow, 0, 256, 0, 256),
        sine_low=cut(narrow, 256, 512, 0, 256),
        basis_high=cut(narrow, 512, 768, 0, 128),
        basis_low=cut(narrow, 512, 768, 128, 256),
        select=[cut(narrow, 768 + 96 * t, 864 + 96 * t, 0, 256) for t in range(4)],
        column_high=cut(narrow, 1152, 1408, 0, 256),
        column_low=cut(narrow, 1408, 1664, 0, 256),
        heads=[cut(narrow, 1664, 1920, 128 * odd, 128 * odd + 128) for odd in range(2)],
    )


def kernel(charge_hbm, plain_hbm, narrow_hbm, out_ref, energy_ref, *scratch):
    charge, plain, narrow = scratch[:3]
    sends = scratch[3:7]
    lands = scratch[7:11]
    (
        mats, field_ref, inverse, shape_z, expand_high, expand_low, expand_z, pair_sum, half_rows,
        green, folded, hats, extra, power, own, onehot, small_send, small_land, local_sem,
        send_sem, recv_sem,
    ) = scratch[11:]
    table = unpack(plain, narrow, lambda ref, a, b, c, d: ref.at[a:b, c:d])
    eigen_wide, edge_wide, lane_rows = table["eigen_wide"], table["edge_wide"], table["lane_rows"]
    sine_high, sine_low, select = table["sine_high"], table["sine_low"], table["select"]
    p = lax.axis_index("gx")
    q = lax.axis_index("gy")

    pieces = (
        (charge_hbm, charge),
        (narrow_hbm.at[0:512, :], narrow.at[0:512, :]),
        (narrow_hbm.at[512:1920, :], narrow.at[512:1920, :]),
        (plain_hbm, plain),
    )
    copies = [
        pltpu.make_async_copy(source, target, local_sem.at[i])
        for i, (source, target) in enumerate(pieces)
    ]
    for copy in copies:
        copy.start()

    barrier = pltpu.get_barrier_semaphore()

    for axis, me in (("gx", p), ("gy", q)):
        for d in FAR[axis]:
            pl.semaphore_signal(
                barrier, inc=1, device_id={axis: lax.rem(me + d, SIDE)}, device_id_type=MESH
            )

    def at(index):
        return pl.ds(pl.multiple_of(index * SIDE, SIDE), SIDE)

    def sines():
        return sine_high[...], sine_low[...]

    def launch(phase, value, axis, me, ready=None):
        sends[phase][...] = dot3(sines(), split(value), NT)
        if ready is not None:
            ready()
        start_all(phase, sends[phase], lands[phase], axis, me, send_sem, recv_sem, SIDE)
        lands[phase][at(me), :] = sends[phase][at(me), :]

    def collect(phase, axis, me, strided, added=None):
        whole_of(phase, lands[phase], axis, me, send_sem, recv_sem).wait_recv()
        land = lands[phase]

        def load(a, h):
            return land[a * SIDE : (a + 1) * SIDE, h * HALF : (h + 1) * HALF]

        def store(g, h, piece):
            if added is not None:
                piece += added[g * SIDE : (g + 1) * SIDE, h * HALF : (h + 1) * HALF]
            if strided:
                mats[h][pl.ds(g, SIDE, stride=SIDE), :] = piece
            else:
                mats[h][g * SIDE : (g + 1) * SIDE, :] = piece

        regroup(load, store, lambda v, amount: pltpu.roll(v, amount, 1))

    def mat():
        return jnp.concatenate([mats[0][...], mats[1][...]], axis=1)

    def small(phase, index, value, axis, me):
        small_send[index][...] = value
        start_all(phase, small_send[index], small_land[index], axis, me, send_sem, recv_sem, None)
        small_land[index][pl.ds(pl.multiple_of(me * 8, 8), 8), :] = value

    def small_total(phase, index, axis, me):
        whole_of(phase, small_land[index], axis, me, send_sem, recv_sem).wait_recv()
        return sum_slots(small_land[index])

    cube = ((N + 1) / 2.0) ** 3

    def lead_rows():
        near = sine_high[at(p), :].astype(F32) + sine_low[at(p), :].astype(F32)
        return split(green_rows(near, table["basis_rows"][...]))

    def fill(k, lead):
        whole = 1.0 / ((pair_sum[...] + own[pl.ds(k, 1), :]) * cube)
        inverse[k] = whole
        green[k] = dot3(lead, split(whole))
        return lead

    def prepare():
        copies[2].wait()
        copies[3].wait()
        for tile in range(4):
            lanes = slice(tile * 256, (tile + 1) * 256)
            chosen = select[tile]
            basis = (table["basis_high"][...][:, :32], table["basis_low"][...][:, :32])
            expand_high[:, lanes] = dot(basis[0], chosen[32:64, :]).astype(BF16)
            expand_low[:, lanes] = dot(basis[1], chosen[32:64, :]).astype(BF16)
            near = (table["basis_high"][at(q), :][:, :32], table["basis_low"][at(q), :][:, :32])
            expand_z[:, lanes] = dot(near[0], chosen[64:96, :]) + dot(near[1], chosen[64:96, :])
        for half in range(2):
            lanes = slice(half * HALF, (half + 1) * HALF)
            own[0:SIDE, lanes] = eigen_wide[at(q), :]
            own[SIDE : 2 * SIDE, lanes] = edge_wide[at(q), :]
        pair_sum[:, :HALF] = eigen_wide[...] + lane_rows[0:1, :HALF]
        pair_sum[:, HALF:] = eigen_wide[...] + lane_rows[0:1, HALF:]
        lax.fori_loop(0, EARLY, fill, lead_rows())
        pl.semaphore_wait(barrier, 2 * (SIDE - 1))

    def drain_big(phase, axis, me):
        whole_of(phase, lands[phase], axis, me, send_sem, recv_sem).wait_send()

    def drain_small(phase, index, axis, me):
        whole_of(phase, small_land[index], axis, me, send_sem, recv_sem).wait_send()

    copies[0].wait()
    copies[1].wait()
    launch(0, charge[...], "gy", q, prepare)
    lax.fori_loop(EARLY, SIDE, fill, lead_rows())

    collect(0, "gy", q, True)
    launch(1, mat(), "gx", p)
    half_rows[...] = dot3(split(mat()), sines())

    def fold(k, carry):
        folded[pl.ds(pl.multiple_of(k * WIDE, 8), WIDE), :] = weighted_rows(
            green[k], half_rows[at(k), :]
        )
        return carry

    lax.fori_loop(0, SIDE, fold, 0)
    entries = local_entries(folded[...], (expand_high, expand_low), expand_z, select)
    small(4, 0, jnp.concatenate(entries, axis=0), "gy", q)
    onehot[...] = owner_map()
    root = table["root"][...]
    square = root * root
    fourth = square * square
    power[...] = fourth * fourth * (fourth * (square * root))
    drain_big(0, "gy", q)
    small(5, 1, small_total(4, 0, "gy", q), "gx", p)

    collect(1, "gx", p, False)
    value = dot3(split(mat()), sines())
    field = value * jnp.concatenate([inverse[k, at(p), :] for k in range(SIDE)], axis=0)
    field_ref[...] = field
    launch(2, field, "gx", p)
    energy = jnp.sum(jnp.sum(value * field, axis=1, keepdims=True), axis=0, keepdims=True)
    entries = small_total(5, 1, "gx", p)

    at_x = at_y = (sine_high[at(p), :], sine_low[at(p), :])
    at_z = (sine_high[at(q), :], sine_low[at(q), :])
    planes = surface_planes(
        entries, table["gather"], table["spread"], onehot[...],
        (table["column_high"][...], table["column_low"][...]), table["heads"],
        table["root"][...], power[...],
    )
    hat_y, hat_x, near_x, near_z = side_hats(planes, at_y, at_z, sines())
    edge_y = edge_wide[at(p), :]
    edge_y = jnp.concatenate([edge_y, edge_y], axis=1)
    edge_z = own[SIDE : 2 * SIDE, :]
    edge_lane = (lane_rows[1:2, :], lane_rows[2:3, :])
    cross = jnp.zeros((SIDE, 256), F32)
    for k in range(SIDE):
        cross += field_ref[k * SIDE : (k + 1) * SIDE, :] * source_block(
            k, near_z, hat_y, near_x, edge_y, edge_z, edge_lane
        )
    second = energy + jnp.sum(jnp.sum(cross, axis=1, keepdims=True), axis=0, keepdims=True)
    lane = lax.broadcasted_iota(jnp.int32, (8, HALF), 1)
    small(6, 2, jnp.where(lane == 0, energy, second), "gx", p)

    for n in range(2):
        shape_z[n] = dot3(split(dot3(sines(), planes[n])), sines())
    hats[0] = hat_y
    hats[1] = hat_x
    edge = jnp.concatenate([edge_wide[...], edge_wide[...]], axis=1)

    def correct(k, carry):
        extra[at(k), :] = corrected(
            shape_z[lax.rem(k, 2)],
            own[pl.ds(SIDE + k, 1), :],
            (hats[0, pl.ds(k, 1), :], hats[0, pl.ds(SIDE + k, 1), :]),
            edge,
            (hats[1, pl.ds(k, 1), :], hats[1, pl.ds(SIDE + k, 1), :]),
            inverse[k],
            green[k, 17 * SIDE :, :],
            at_x,
        )
        return carry

    lax.fori_loop(0, SIDE, correct, 0, unroll=UNROLL)
    collect(2, "gx", p, True, extra)
    launch(3, mat(), "gy", q)
    drain_big(1, "gx", p)
    drain_big(2, "gx", p)
    drain_small(4, 0, "gy", q)
    drain_small(5, 1, "gx", p)
    small(7, 3, small_total(6, 2, "gx", p), "gy", q)
    drain_small(6, 2, "gx", p)
    collect(3, "gy", q, False)
    out_ref[...] = dot3(split(mat()), sines())
    drain_big(3, "gy", q)
    energy_ref[...] = small_total(7, 3, "gy", q) * (1.0 / (N + 1)) ** 3
    drain_small(7, 3, "gy", q)


def constants():
    sine_rows, eigen, basis, select, gather, spread, columns, rows, root, power = build_tables()

    def pair(table):
        table = table.astype(np.float32)
        high = table.astype(jnp.bfloat16)
        return high, (table - high.astype(np.float32)).astype(jnp.bfloat16)

    parity = np.arange(N) % 2
    lane_rows = np.zeros((8, N))
    lane_rows[0] = eigen
    lane_rows[1] = sine_rows[0] * (parity == 0)
    lane_rows[2] = sine_rows[0] * (parity == 1)
    lane_rows[3] = sine_rows[0]
    heads = []
    for odd in range(2):
        tables = [trig(parity_of, odd, np.arctan(2.0 * (np.arange(N) - (N - 1) / 2.0) / (N + 1))) for parity_of in range(2)]
        wide = np.zeros((N, 32))
        for k, table in enumerate(tables):
            wide[:, 16 * k : 16 * k + table.shape[0]] = table.T
        high, low = pair(wide)
        heads.append(np.concatenate([high, high, low, low], axis=1))
    plain = np.concatenate(
        [
            np.concatenate([np.repeat(v[:, None], HALF, 1) for v in (eigen, sine_rows[0])], axis=1),
            lane_rows,
            basis.T[:WIDE],
            *[gather[:, 256 * t : 256 * (t + 1)] for t in range(4)],
            spread[:, :8].reshape(8 * SLOTS, 256),
            spread[:, 8],
            root,
        ],
        axis=0,
    ).astype(np.float32)
    wide = np.zeros((N, HALF - 32))
    high, low = pair(basis)
    narrow = np.concatenate(
        [
            *pair(sine_rows),
            np.concatenate([high, wide.astype(high.dtype), low, wide.astype(high.dtype)], axis=1),
            *[
                np.concatenate(list(select), axis=0)[:, 256 * t : 256 * (t + 1)].astype(jnp.bfloat16)
                for t in range(4)
            ],
            *pair(columns),
            np.concatenate(heads, axis=1),
        ],
        axis=0,
    )
    return plain, narrow


def solution(mesh):
    tables = constants()

    def shards(charge_density):
        cells_a, cells_b, length = charge_density.shape
        flat = charge_density.reshape(cells_a * cells_b, length)
        grid = pltpu.VMEM((256, 256), F32)
        potential, energies = pl.pallas_call(
            kernel,
            out_shape=(
                pltpu.VMEM((256, 256), F32),
                pltpu.VMEM((8, HALF), F32),
            ),
            in_specs=[pl.BlockSpec(memory_space=pl.ANY)] * 3,
            out_specs=(
                pl.BlockSpec(memory_space=pltpu.VMEM),
                pl.BlockSpec(memory_space=pltpu.VMEM),
            ),
            scratch_shapes=[
                grid,
                *[pltpu.VMEM(table.shape, table.dtype) for table in tables],
                *[grid] * 8,
                [pltpu.VMEM((256, HALF), F32)] * 2,
                grid,
                pltpu.VMEM((SIDE, 256, 256), F32),
                pltpu.VMEM((2, 256, 256), F32),
                pltpu.VMEM((256, LANES), BF16),
                pltpu.VMEM((256, LANES), BF16),
                pltpu.VMEM((SIDE, LANES), F32),
                grid,
                grid,
                pltpu.VMEM((SIDE, 19 * SIDE, 256), F32),
                pltpu.VMEM((SIDE * WIDE, 256), F32),
                pltpu.VMEM((2, 2 * SIDE, 256), F32),
                grid,
                grid,
                pltpu.VMEM((2 * SIDE, 256), F32),
                pltpu.VMEM((LANES, 256), BF16),
                [pltpu.VMEM((8, HALF), F32)] * 4,
                [pltpu.VMEM((8 * SIDE, HALF), F32)] * 4,
                pltpu.SemaphoreType.DMA((4,)),
                pltpu.SemaphoreType.DMA((8,)),
                pltpu.SemaphoreType.DMA((8,)),
            ],
            compiler_params=pltpu.CompilerParams(
                collective_id=0, has_side_effects=True, vmem_limit_bytes=VMEM_LIMIT
            ),
        )(flat, *[jnp.asarray(table) for table in tables])
        return potential.reshape(cells_a, cells_b, length), energies[0, :2]

    return jax.shard_map(
        shards,
        mesh=mesh,
        in_specs=(P("gx", "gy", None),),
        out_specs=(P("gx", "gy", None), P()),
        check_vma=False,
    )
```

```python
import math

import jax
import jax.numpy as jnp
import numpy as np
from jax import lax
from jax.experimental import pallas as pl
from jax.experimental.pallas import tpu as pltpu
from jax.sharding import PartitionSpec as P

ORDER = 16
N = 256
SLOTS = 48
LANES = 1024
SPARE = 128 + 112


def harmonics(x, y, z):
    cosine = {(0, 0): np.ones_like(x)}
    sine = {(0, 0): np.zeros_like(x)}
    for l in range(1, ORDER + 1):
        scale = 1.0 if l == 1 else math.sqrt((2 * l - 1) / (2.0 * l))
        c, s = cosine[l - 1, l - 1], sine[l - 1, l - 1]
        cosine[l, l] = scale * (x * c - y * s)
        sine[l, l] = scale * (x * s + y * c)
        for m in range(l):
            near = (2 * l - 1) / math.sqrt(l * l - m * m)
            far = math.sqrt((l - 1) ** 2 - m * m) / math.sqrt(l * l - m * m)
            for table in (cosine, sine):
                older = table[l - 2, m] if l - 2 >= m else 0.0
                table[l, m] = near * z * table[l - 1, m] - far * older
    return cosine, sine


def face_point(face, t, s):
    one = np.ones_like(t)
    return ((s, t, one), (s, one, t), (one, t, s))[face]


def face_parity(face, px, py, pz):
    return ((py, px, pz), (pz, px, py), (py, pz, px))[face]


def trig(parity, odd, angle):
    if odd:
        orders = np.arange(1, 16, 2)
    else:
        orders = np.arange(0, 17, 2) if parity == 0 else np.arange(2, 17, 2)
    wave = np.cos if parity == 0 else np.sin
    return wave(orders[:, None] * angle[None, :])


def build_tables():
    span = N + 1.0
    step = 1.0 / span
    radius = math.sqrt(3.0) / 2.0
    index = np.arange(N) + 1
    sine_rows = np.sin(np.pi * (index[:, None] * index[None, :] % (2 * N + 2)) / span)
    eigen = 4.0 * span * span * np.sin(np.pi * index / (2 * span)) ** 2
    scaled = 2.0 * (np.arange(N) - (N - 1) / 2.0) * step
    angle = np.arctan(scaled)

    terms = [[] for _ in range(8)]
    for l in range(ORDER + 1):
        for m in range(l + 1):
            terms[(m % 2) * 4 + (l - m) % 2].append((l, m, 0))
            if m:
                terms[((m - 1) % 2) * 4 + 2 + (l - m) % 2].append((l, m, 1))

    nodes, quad = np.polynomial.legendre.leggauss(24)
    legendre = np.polynomial.legendre.legvander(nodes, ORDER).T
    basis = np.zeros((N, 32))
    basis[:, : ORDER + 1] = sine_rows @ np.polynomial.legendre.legvander(scaled, ORDER)
    even = (np.arange(N) % 2 == 0).astype(np.float64)
    basis[:, 17] = sine_rows[0] * even
    basis[:, 18] = sine_rows[0] * (1.0 - even)
    project = legendre * quad[None, :] * (np.arange(ORDER + 1) + 0.5)[:, None]
    turns = 64
    circle = 2.0 * np.pi * np.arange(turns) / turns
    ones_t, ones_s = np.meshgrid(nodes, nodes, indexing="ij")
    alpha, beta = np.meshgrid(circle, circle, indexing="ij")
    solid, wave = [], []
    for face in range(3):
        x, y, z = face_point(face, ones_t, ones_s)
        r = np.sqrt(x * x + y * y + z * z)
        table = harmonics(x / r, y / r, z / r)
        solid.append((table, r / math.sqrt(3.0)))
        ca, sa, cb, sb = np.cos(alpha), np.sin(alpha), np.cos(beta), np.sin(beta)
        parts = (sa * cb, ca * sb, ca * cb)
        order = ((1, 0, 2), (1, 2, 0), (2, 0, 1))[face]
        x, y, z = (parts[k] for k in order)
        r = np.sqrt(x * x + y * y + z * z)
        safe = np.where(r < 1e-12, 1.0, r)
        wave.append((harmonics(x / safe, y / safe, z / safe), np.where(r < 1e-12, 0.0, r)))

    select = np.zeros((3, 32, LANES))
    gather = np.zeros((SLOTS, LANES))
    spread = np.zeros((SLOTS, 16, 256))
    columns = np.zeros((256, N))
    rows = np.zeros((8, 3, 16, N))
    spill = SPARE
    for group in range(8):
        px, py, pz = group >> 2 & 1, group >> 1 & 1, group & 1
        odd = (px + py + pz) % 2
        lane = group * 128
        for face in range(3):
            prow, pcol, normal = face_parity(face, px, py, pz)
            sign = 2.0 if normal == 0 else -2.0
            entries = [
                (i, j)
                for i in range(prow, ORDER + 1, 2)
                for j in range(pcol, ORDER + 1, 2)
                if i + j + normal <= ORDER - odd
            ]
            moments = {}
            for slot, (l, m, which) in enumerate(terms[group]):
                table, ratio = solid[face]
                values = ratio**l * table[which][l, m]
                moments[slot] = project @ values @ project.T
            for i, j in entries:
                if lane >= (group + 1) * 128 or (lane >= SPARE and group == 1):
                    position, spill = spill, spill + 1
                    assert group == 0
                else:
                    position, lane = lane, lane + 1
                axes = ((1, 0, 2), (2, 0, 1), (1, 2, 0))[face]
                select[axes[0], i, position] = 1.0
                select[axes[1], j, position] = 1.0
                select[axes[2], 17 + normal, position] = 1.0
                for slot in moments:
                    gather[slot, position] = step * sign * moments[slot][i, j]
            left = trig(prow, odd, circle)
            right = trig(pcol, odd, circle)
            left_unit = left / np.sum(left * left, axis=1, keepdims=True)
            right_unit = right / np.sum(right * right, axis=1, keepdims=True)
            base = group * 32 + face * 9
            for slot, (l, m, which) in enumerate(terms[group]):
                table, r = wave[face]
                values = r ** (ORDER - odd) * table[which][l, m]
                block = left_unit @ values @ right_unit.T
                weight = (1.0 if m == 0 else 2.0) / (4.0 * math.pi * radius * 1.1 ** (l + 1))
                block = block * weight * sign * span * span
                spread[slot, : block.shape[0], base : base + block.shape[1]] = block
            tail = trig(pcol, odd, angle)
            columns[base : base + tail.shape[0]] = tail
            head = trig(prow, odd, angle)
            rows[group, face, : head.shape[0]] = head
    assert spill <= 256
    root = 1.0 / np.sqrt(1.0 - np.outer(np.sin(angle) ** 2, np.sin(angle) ** 2))
    return sine_rows, eigen, basis, select, gather, spread, columns, rows, root, root**15

MESH = pl.DeviceIdType.MESH
SIDE = 16
WIDE = 24
EARLY = 0
UNROLL = 2
VMEM_LIMIT = 67043328 - 1024 * 1024
HALF = 128
F32 = jnp.float32
BF16 = jnp.bfloat16
NN = (((1,), (0,)), ((), ()))
NT = (((1,), (1,)), ((), ()))


def split(value):
    high = value.astype(BF16)
    return high, (value - high.astype(F32)).astype(BF16)


def dot(a, b, dims=NN):
    return lax.dot_general(a, b, dims, preferred_element_type=F32)


def dot3(a, b, dims=NN):
    return dot(a[0], b[0], dims) + (dot(a[0], b[1], dims) + dot(a[1], b[0], dims))


def regroup(load, store, roll):
    lane = lax.broadcasted_iota(jnp.int32, (4 * SIDE, HALF), 1)
    rows = [
        jnp.concatenate([load(8 * a + i, h) for a in range(2) for h in range(2)], axis=0)
        for i in range(8)
    ]
    for step in (4, 2, 1):
        keep = (lane // (SIDE * step)) % 2 == 0
        for i in range(8):
            if i & step == 0:
                one, two = rows[i], rows[i + step]
                rows[i] = jnp.where(keep, one, roll(two, SIDE * step))
                rows[i + step] = jnp.where(keep, roll(one, HALF - SIDE * step), two)
    for i in range(8):
        for a in range(2):
            for h in range(2):
                part = 2 * a + h
                store(8 * h + i, a, rows[i][part * SIDE : (part + 1) * SIDE])


def green_rows(sines, basis_rows):
    rows = [sines[x : x + 1, :] * basis_rows[:SIDE] for x in range(SIDE)]
    rows += [sines * basis_rows[f : f + 1] for f in range(SIDE, SIDE + 3)]
    return jnp.concatenate(rows, axis=0)


def weighted_rows(table, values):
    total = table[:SIDE] * values[0:1, :]
    for x in range(1, SIDE):
        total += table[x * SIDE : (x + 1) * SIDE] * values[x : x + 1, :]
    other = [
        jnp.sum(table[f * SIDE : (f + 1) * SIDE] * values, axis=0, keepdims=True)
        for f in range(SIDE, SIDE + 3)
    ]
    even = jnp.concatenate([total[:8], *other[:2], jnp.zeros((6, 256), F32)], axis=0)
    return even, jnp.concatenate([total[8:], other[2], jnp.zeros((7, 256), F32)], axis=0)


def local_entries(folded, expand_y, expand_z, select):
    pieces = [split(part) for part in folded]
    outcome = []
    for tile in range(4):
        lanes = slice(tile * 256, (tile + 1) * 256)
        mixed = dot3(pieces[tile // 2], (expand_y[0][:, lanes], expand_y[1][:, lanes]))
        total = mixed[:SIDE] * expand_z[0:1, lanes]
        for k in range(1, SIDE):
            total += mixed[k * SIDE : (k + 1) * SIDE] * expand_z[k : k + 1, lanes]
        start = SIDE * (tile // 2)
        chosen = select[tile][start : start + SIDE, :].astype(F32)
        summed = jnp.sum(total * chosen, axis=0, keepdims=True)
        outcome += [summed[:, :HALF], summed[:, HALF:]]
    return outcome


def owner_map():
    row = lax.broadcasted_iota(jnp.int32, (LANES, 256), 0)
    lane = lax.broadcasted_iota(jnp.int32, (LANES, 256), 1)
    owner = jnp.where((row >= SPARE) & (row < 256), 0, row // HALF)
    return jnp.where(owner == lane // 32, 1.0, 0.0).astype(BF16)


def surface_planes(entries, gather, spread, onehot, columns, heads, root, power):
    product = jnp.concatenate(
        [gather[r][...] * entries[r : r + 1, :] for r in range(8)], axis=1
    )
    high, rest = product.astype(BF16), None
    rest = product - high.astype(F32)
    middle = rest.astype(BF16)
    low = (rest - middle.astype(F32)).astype(BF16)
    moments = dot(jnp.concatenate([high, middle, low], axis=0), onehot)
    moments = moments[:SLOTS] + (moments[SLOTS : 2 * SLOTS] + moments[2 * SLOTS :])
    shape = moments[0:1, :] * spread[0][0:8, :]
    for slot in range(1, 45):
        shape += moments[slot : slot + 1, :] * spread[0][slot * 8 : slot * 8 + 8, :]
    ninth = jnp.sum(moments * spread[1][...], axis=0, keepdims=True)
    below = lax.broadcasted_iota(jnp.int32, (8, 256), 0) == 0
    shape = jnp.concatenate([shape, jnp.where(below, ninth, 0.0)], axis=0)
    lane = lax.broadcasted_iota(jnp.int32, (SIDE, 256), 1)
    blocks = []
    for face in range(3):
        for normal in range(2):
            for odd in range(2):
                for head in range(2):
                    tail = (odd + normal + head) % 2
                    px, py, pz = (
                        (tail, head, normal),
                        (tail, normal, head),
                        (normal, head, tail),
                    )[face]
                    base = (px * 4 + py * 2 + pz) * 32 + face * 9
                    blocks.append(jnp.where((lane >= base) & (lane < base + 9), shape, 0.0))
    right = dot3(split(jnp.concatenate(blocks, axis=0)), columns)
    planes = []
    for face in range(3):
        for normal in range(2):
            parts = []
            for odd in range(2):
                start = ((face * 2 + normal) * 2 + odd) * 32
                high, low = split(right[start : start + 32])
                stack = jnp.concatenate([high, low, high, low], axis=0)
                parts.append(dot(heads[odd][...], stack))
            planes.append(split(power * (root * parts[0] + parts[1])))
    return planes


def few_rows(rows, matrix, dims=NN):
    both = dot(jnp.concatenate(rows, axis=0), matrix[0], dims)
    return both[:SIDE] + (both[SIDE:] + dot(rows[0], matrix[1], dims))


def side_hats(planes, at_y, at_z, sines):
    half_y = split(jnp.concatenate([few_rows(at_z, planes[2 + n]) for n in range(2)], axis=0))
    hat_y = dot3(half_y, sines)
    half = [few_rows(at_z, planes[4 + n], NT) for n in range(2)]
    hat_x = dot3(split(jnp.concatenate(half, axis=0)), sines)
    near_x = [dot3(at_y, split(half[n]), NT) for n in range(2)]
    half_z = split(jnp.concatenate([few_rows(at_y, planes[n]) for n in range(2)], axis=0))
    return hat_y, hat_x, near_x, dot3(half_z, sines)


def corrected(shape, scale, hat_y, edge, hat_x, inverse, edge_green, at_x):
    even = lax.broadcasted_iota(jnp.int32, (256, 256), 0) % 2 == 0
    mixed = shape * scale + jnp.where(even, hat_y[0], hat_y[1]) * edge
    value = few_rows(at_x, split(mixed * inverse), NT)
    return value + hat_x[0] * edge_green[:SIDE] + hat_x[1] * edge_green[SIDE:]


def source_block(k, hat_z, hat_y, last, edge_y, edge_z, edge_lane):
    ky = lax.broadcasted_iota(jnp.int32, (SIDE, 256), 0)
    value = hat_z[(k % 2) * SIDE : (k % 2 + 1) * SIDE] * edge_z[k : k + 1, :]
    side = jnp.where(ky % 2 == 0, hat_y[k : k + 1, :], hat_y[SIDE + k : SIDE + k + 1, :])
    value += side * edge_y
    value += last[0][:, k : k + 1] * edge_lane[0] + last[1][:, k : k + 1] * edge_lane[1]
    return value


FAR = {
    "gx": (
        (4, 1), (3, 1), (5, 1), (4, 0), (2, 1), (6, 1), (3, 0), (5, 0), (1, 1), (7, 1), (2, 0),
        (6, 0), (0, 1), (1, 0), (7, 0),
    ),
    "gy": (
        (2, 3), (2, 2), (1, 3), (3, 3), (1, 2), (3, 2), (2, 1), (2, 0), (1, 1), (3, 1), (1, 0),
        (3, 0), (0, 3), (0, 2), (0, 1),
    ),
}


def peer_of(axis, me, step):
    if axis == "gx":
        return lax.rem(me // 8 + step[1], 2) * 8 + lax.rem(me % 8 + step[0], 8)
    cross = lax.rem(me % 4 // 2 + step[1] // 2, 2) * 2 + lax.rem(me % 2 + step[1] % 2, 2)
    return lax.rem(me // 4 + step[0], 4) * 4 + cross


def start_all(phase, source, target, axis, me, send_sem, recv_sem, rows):
    for step in FAR[axis]:
        peer = peer_of(axis, me, step)
        count = source.shape[0] if rows is None else rows
        src = source if rows is None else source.at[pl.ds(pl.multiple_of(peer * rows, rows), rows), :]
        pltpu.make_async_remote_copy(
            src_ref=src,
            dst_ref=target.at[pl.ds(pl.multiple_of(me * count, count), count), :],
            send_sem=send_sem.at[phase],
            recv_sem=recv_sem.at[phase],
            device_id={axis: peer},
            device_id_type=MESH,
        ).start()


def whole_of(phase, target, axis, me, send_sem, recv_sem):
    rows = target.shape[0] // SIDE * (SIDE - 1)
    return pltpu.make_async_remote_copy(
        src_ref=target.at[0:rows, :],
        dst_ref=target.at[0:rows, :],
        send_sem=send_sem.at[phase],
        recv_sem=recv_sem.at[phase],
        device_id={axis: lax.rem(me + 1, SIDE)},
        device_id_type=MESH,
    )


def sum_slots(ref):
    total = ref[0:8, :]
    for slot in range(1, SIDE):
        total += ref[slot * 8 : (slot + 1) * 8, :]
    return total


def unpack(plain, narrow, cut):
    return dict(
        eigen_wide=cut(plain, 0, 256, 0, 128),
        edge_wide=cut(plain, 0, 256, 128, 256),
        lane_rows=cut(plain, 256, 264, 0, 256),
        basis_rows=cut(plain, 264, 288, 0, 256),
        gather=[
            cut(plain, 288 + SLOTS * (r // 2), 288 + SLOTS * (r // 2 + 1), r % 2 * 128, r % 2 * 128 + 128)
            for r in range(8)
        ],
        spread=(cut(plain, 480, 864, 0, 256), cut(plain, 864, 912, 0, 256)),
        root=cut(plain, 912, 1168, 0, 256),
        sine_high=cut(narrow, 0, 256, 0, 256),
        sine_low=cut(narrow, 256, 512, 0, 256),
        basis_high=cut(narrow, 512, 768, 0, 128),
        basis_low=cut(narrow, 512, 768, 128, 256),
        select=[cut(narrow, 768 + 96 * t, 864 + 96 * t, 0, 256) for t in range(4)],
        column_high=cut(narrow, 1152, 1408, 0, 256),
        column_low=cut(narrow, 1408, 1664, 0, 256),
        heads=[cut(narrow, 1664, 1920, 128 * odd, 128 * odd + 128) for odd in range(2)],
    )


def kernel(charge_hbm, plain_hbm, narrow_hbm, out_ref, energy_ref, *scratch):
    charge, plain, narrow = scratch[:3]
    sends = scratch[3:7]
    lands = scratch[7:11]
    (
        mats, field_ref, inverse, shape_z, expand_high, expand_low, expand_z, pair_sum, half_rows,
        green, folded, hats, extra, power, own, onehot, small_send, small_land, local_sem,
        send_sem, recv_sem,
    ) = scratch[11:]
    table = unpack(plain, narrow, lambda ref, a, b, c, d: ref.at[a:b, c:d])
    eigen_wide, edge_wide, lane_rows = table["eigen_wide"], table["edge_wide"], table["lane_rows"]
    sine_high, sine_low, select = table["sine_high"], table["sine_low"], table["select"]
    p = lax.axis_index("gx")
    q = lax.axis_index("gy")

    pieces = (
        (charge_hbm, charge),
        (narrow_hbm.at[0:512, :], narrow.at[0:512, :]),
        (narrow_hbm.at[512:1920, :], narrow.at[512:1920, :]),
        (plain_hbm, plain),
    )
    copies = [
        pltpu.make_async_copy(source, target, local_sem.at[i])
        for i, (source, target) in enumerate(pieces)
    ]
    for copy in copies:
        copy.start()

    barrier = pltpu.get_barrier_semaphore()

    for axis, me in (("gx", p), ("gy", q)):
        for step in FAR[axis]:
            pl.semaphore_signal(
                barrier, inc=1, device_id={axis: peer_of(axis, me, step)}, device_id_type=MESH
            )

    def at(index):
        return pl.ds(pl.multiple_of(index * SIDE, SIDE), SIDE)

    def sines():
        return sine_high[...], sine_low[...]

    def launch(phase, value, axis, me, ready=None):
        sends[phase][...] = dot3(sines(), split(value), NT)
        if ready is not None:
            ready()
        start_all(phase, sends[phase], lands[phase], axis, me, send_sem, recv_sem, SIDE)
        lands[phase][at(me), :] = sends[phase][at(me), :]

    def collect(phase, axis, me, strided, added=None):
        whole_of(phase, lands[phase], axis, me, send_sem, recv_sem).wait_recv()
        land = lands[phase]

        def load(a, h):
            return land[a * SIDE : (a + 1) * SIDE, h * HALF : (h + 1) * HALF]

        def store(g, h, piece):
            if added is not None:
                piece += added[g * SIDE : (g + 1) * SIDE, h * HALF : (h + 1) * HALF]
            if strided:
                mats[h][pl.ds(g, SIDE, stride=SIDE), :] = piece
            else:
                mats[h][g * SIDE : (g + 1) * SIDE, :] = piece

        regroup(load, store, lambda v, amount: pltpu.roll(v, amount, 1))

    def mat():
        return jnp.concatenate([mats[0][...], mats[1][...]], axis=1)

    def small(phase, index, value, axis, me):
        small_send[index][...] = value
        start_all(phase, small_send[index], small_land[index], axis, me, send_sem, recv_sem, None)
        small_land[index][pl.ds(pl.multiple_of(me * 8, 8), 8), :] = value

    def small_total(phase, index, axis, me):
        whole_of(phase, small_land[index], axis, me, send_sem, recv_sem).wait_recv()
        return sum_slots(small_land[index])

    cube = ((N + 1) / 2.0) ** 3

    def lead_rows():
        near = sine_high[at(p), :].astype(F32) + sine_low[at(p), :].astype(F32)
        return split(green_rows(near, table["basis_rows"][...]))

    def fill(k, lead):
        whole = 1.0 / ((pair_sum[...] + own[pl.ds(k, 1), :]) * cube)
        inverse[k] = whole
        green[k] = dot3(lead, split(whole))
        return lead

    def prepare():
        copies[2].wait()
        copies[3].wait()
        for tile in range(4):
            lanes = slice(tile * 256, (tile + 1) * 256)
            chosen = select[tile]
            basis = (table["basis_high"][...][:, :32], table["basis_low"][...][:, :32])
            expand_high[:, lanes] = dot(basis[0], chosen[32:64, :]).astype(BF16)
            expand_low[:, lanes] = dot(basis[1], chosen[32:64, :]).astype(BF16)
            near = (table["basis_high"][at(q), :][:, :32], table["basis_low"][at(q), :][:, :32])
            expand_z[:, lanes] = dot(near[0], chosen[64:96, :]) + dot(near[1], chosen[64:96, :])
        for half in range(2):
            lanes = slice(half * HALF, (half + 1) * HALF)
            own[0:SIDE, lanes] = eigen_wide[at(q), :]
            own[SIDE : 2 * SIDE, lanes] = edge_wide[at(q), :]
        pair_sum[:, :HALF] = eigen_wide[...] + lane_rows[0:1, :HALF]
        pair_sum[:, HALF:] = eigen_wide[...] + lane_rows[0:1, HALF:]
        lax.fori_loop(0, EARLY, fill, lead_rows())
        pl.semaphore_wait(barrier, 2 * (SIDE - 1))

    def drain_big(phase, axis, me):
        whole_of(phase, lands[phase], axis, me, send_sem, recv_sem).wait_send()

    def drain_small(phase, index, axis, me):
        whole_of(phase, small_land[index], axis, me, send_sem, recv_sem).wait_send()

    copies[0].wait()
    copies[1].wait()
    launch(0, charge[...], "gy", q, prepare)
    lax.fori_loop(EARLY, SIDE, fill, lead_rows())

    collect(0, "gy", q, True)
    launch(1, mat(), "gx", p)
    half_rows[...] = dot3(split(mat()), sines())

    def fold(k, carry):
        folded[0, at(k), :], folded[1, at(k), :] = weighted_rows(green[k], half_rows[at(k), :])
        return carry

    lax.fori_loop(0, SIDE, fold, 0)
    entries = local_entries((folded[0], folded[1]), (expand_high, expand_low), expand_z, select)
    small(4, 0, jnp.concatenate(entries, axis=0), "gy", q)
    onehot[...] = owner_map()
    root = table["root"][...]
    square = root * root
    fourth = square * square
    power[...] = fourth * fourth * (fourth * (square * root))
    drain_big(0, "gy", q)
    small(5, 1, small_total(4, 0, "gy", q), "gx", p)

    collect(1, "gx", p, False)
    value = dot3(split(mat()), sines())
    field = value * jnp.concatenate([inverse[k, at(p), :] for k in range(SIDE)], axis=0)
    field_ref[...] = field
    launch(2, field, "gx", p)
    energy = jnp.sum(jnp.sum(value * field, axis=1, keepdims=True), axis=0, keepdims=True)
    entries = small_total(5, 1, "gx", p)

    at_x = at_y = (sine_high[at(p), :], sine_low[at(p), :])
    at_z = (sine_high[at(q), :], sine_low[at(q), :])
    planes = surface_planes(
        entries, table["gather"], table["spread"], onehot[...],
        (table["column_high"][...], table["column_low"][...]), table["heads"],
        table["root"][...], power[...],
    )
    hat_y, hat_x, near_x, near_z = side_hats(planes, at_y, at_z, sines())
    edge_y = edge_wide[at(p), :]
    edge_y = jnp.concatenate([edge_y, edge_y], axis=1)
    edge_z = own[SIDE : 2 * SIDE, :]
    edge_lane = (lane_rows[1:2, :], lane_rows[2:3, :])
    cross = jnp.zeros((SIDE, 256), F32)
    for k in range(SIDE):
        cross += field_ref[k * SIDE : (k + 1) * SIDE, :] * source_block(
            k, near_z, hat_y, near_x, edge_y, edge_z, edge_lane
        )
    second = energy + jnp.sum(jnp.sum(cross, axis=1, keepdims=True), axis=0, keepdims=True)
    lane = lax.broadcasted_iota(jnp.int32, (8, HALF), 1)
    small(6, 2, jnp.where(lane == 0, energy, second), "gx", p)

    for n in range(2):
        shape_z[n] = dot3(split(dot3(sines(), planes[n])), sines())
    hats[0] = hat_y
    hats[1] = hat_x
    edge = jnp.concatenate([edge_wide[...], edge_wide[...]], axis=1)

    def correct(k, carry):
        extra[at(k), :] = corrected(
            shape_z[lax.rem(k, 2)],
            own[pl.ds(SIDE + k, 1), :],
            (hats[0, pl.ds(k, 1), :], hats[0, pl.ds(SIDE + k, 1), :]),
            edge,
            (hats[1, pl.ds(k, 1), :], hats[1, pl.ds(SIDE + k, 1), :]),
            inverse[k],
            green[k, 17 * SIDE :, :],
            at_x,
        )
        return carry

    lax.fori_loop(0, SIDE, correct, 0, unroll=UNROLL)
    collect(2, "gx", p, True, extra)
    launch(3, mat(), "gy", q)
    drain_big(1, "gx", p)
    drain_big(2, "gx", p)
    drain_small(4, 0, "gy", q)
    drain_small(5, 1, "gx", p)
    small(7, 3, small_total(6, 2, "gx", p), "gy", q)
    drain_small(6, 2, "gx", p)
    collect(3, "gy", q, False)
    out_ref[...] = dot3(split(mat()), sines())
    drain_big(3, "gy", q)
    energy_ref[...] = small_total(7, 3, "gy", q) * (1.0 / (N + 1)) ** 3
    drain_small(7, 3, "gy", q)


def constants():
    sine_rows, eigen, basis, select, gather, spread, columns, rows, root, power = build_tables()

    def pair(table):
        table = table.astype(np.float32)
        high = table.astype(jnp.bfloat16)
        return high, (table - high.astype(np.float32)).astype(jnp.bfloat16)

    parity = np.arange(N) % 2
    lane_rows = np.zeros((8, N))
    lane_rows[0] = eigen
    lane_rows[1] = sine_rows[0] * (parity == 0)
    lane_rows[2] = sine_rows[0] * (parity == 1)
    lane_rows[3] = sine_rows[0]
    heads = []
    for odd in range(2):
        tables = [trig(parity_of, odd, np.arctan(2.0 * (np.arange(N) - (N - 1) / 2.0) / (N + 1))) for parity_of in range(2)]
        wide = np.zeros((N, 32))
        for k, table in enumerate(tables):
            wide[:, 16 * k : 16 * k + table.shape[0]] = table.T
        high, low = pair(wide)
        heads.append(np.concatenate([high, high, low, low], axis=1))
    plain = np.concatenate(
        [
            np.concatenate([np.repeat(v[:, None], HALF, 1) for v in (eigen, sine_rows[0])], axis=1),
            lane_rows,
            basis.T[[*range(0, 16, 2), *range(1, 16, 2), *range(16, WIDE)]],
            *[gather[:, 256 * t : 256 * (t + 1)] for t in range(4)],
            spread[:, :8].reshape(8 * SLOTS, 256),
            spread[:, 8],
            root,
        ],
        axis=0,
    ).astype(np.float32)
    wide = np.zeros((N, HALF - 32))
    chosen = np.zeros_like(select[0])
    chosen[[*range(10), *range(16, 25)]] = select[0][[*range(0, 17, 2), 17, *range(1, 16, 2), 18]]
    select[0] = chosen
    high, low = pair(basis)
    narrow = np.concatenate(
        [
            *pair(sine_rows),
            np.concatenate([high, wide.astype(high.dtype), low, wide.astype(high.dtype)], axis=1),
            *[
                np.concatenate(list(select), axis=0)[:, 256 * t : 256 * (t + 1)].astype(jnp.bfloat16)
                for t in range(4)
            ],
            *pair(columns),
            np.concatenate(heads, axis=1),
        ],
        axis=0,
    )
    return plain, narrow


def solution(mesh):
    tables = constants()

    def shards(charge_density):
        cells_a, cells_b, length = charge_density.shape
        flat = charge_density.reshape(cells_a * cells_b, length)
        grid = pltpu.VMEM((256, 256), F32)
        potential, energies = pl.pallas_call(
            kernel,
            out_shape=(
                pltpu.VMEM((256, 256), F32),
                pltpu.VMEM((8, HALF), F32),
            ),
            in_specs=[pl.BlockSpec(memory_space=pl.ANY)] * 3,
            out_specs=(
                pl.BlockSpec(memory_space=pltpu.VMEM),
                pl.BlockSpec(memory_space=pltpu.VMEM),
            ),
            scratch_shapes=[
                grid,
                *[pltpu.VMEM(table.shape, table.dtype) for table in tables],
                *[grid] * 8,
                [pltpu.VMEM((256, HALF), F32)] * 2,
                grid,
                pltpu.VMEM((SIDE, 256, 256), F32),
                pltpu.VMEM((2, 256, 256), F32),
                pltpu.VMEM((256, LANES), BF16),
                pltpu.VMEM((256, LANES), BF16),
                pltpu.VMEM((SIDE, LANES), F32),
                grid,
                grid,
                pltpu.VMEM((SIDE, 19 * SIDE, 256), F32),
                pltpu.VMEM((2, 256, 256), F32),
                pltpu.VMEM((2, 2 * SIDE, 256), F32),
                grid,
                grid,
                pltpu.VMEM((2 * SIDE, 256), F32),
                pltpu.VMEM((LANES, 256), BF16),
                [pltpu.VMEM((8, HALF), F32)] * 4,
                [pltpu.VMEM((8 * SIDE, HALF), F32)] * 4,
                pltpu.SemaphoreType.DMA((4,)),
                pltpu.SemaphoreType.DMA((8,)),
                pltpu.SemaphoreType.DMA((8,)),
            ],
            compiler_params=pltpu.CompilerParams(
                collective_id=0, has_side_effects=True, vmem_limit_bytes=VMEM_LIMIT
            ),
        )(flat, *[jnp.asarray(table) for table in tables])
        return potential.reshape(cells_a, cells_b, length), energies[0, :2]

    return jax.shard_map(
        shards,
        mesh=mesh,
        in_specs=(P("gx", "gy", None),),
        out_specs=(P("gx", "gy", None), P()),
        check_vma=False,
    )
```

```python
import math

import jax
import jax.numpy as jnp
import numpy as np
from jax import lax
from jax.experimental import pallas as pl
from jax.experimental.pallas import tpu as pltpu
from jax.sharding import PartitionSpec as P

ORDER = 16
N = 256
SLOTS = 48
LANES = 1024
SPARE = 128 + 112


def harmonics(x, y, z):
    cosine = {(0, 0): np.ones_like(x)}
    sine = {(0, 0): np.zeros_like(x)}
    for l in range(1, ORDER + 1):
        scale = 1.0 if l == 1 else math.sqrt((2 * l - 1) / (2.0 * l))
        c, s = cosine[l - 1, l - 1], sine[l - 1, l - 1]
        cosine[l, l] = scale * (x * c - y * s)
        sine[l, l] = scale * (x * s + y * c)
        for m in range(l):
            near = (2 * l - 1) / math.sqrt(l * l - m * m)
            far = math.sqrt((l - 1) ** 2 - m * m) / math.sqrt(l * l - m * m)
            for table in (cosine, sine):
                older = table[l - 2, m] if l - 2 >= m else 0.0
                table[l, m] = near * z * table[l - 1, m] - far * older
    return cosine, sine


def face_point(face, t, s):
    one = np.ones_like(t)
    return ((s, t, one), (s, one, t), (one, t, s))[face]


def face_parity(face, px, py, pz):
    return ((py, px, pz), (pz, px, py), (py, pz, px))[face]


def trig(parity, odd, angle):
    if odd:
        orders = np.arange(1, 16, 2)
    else:
        orders = np.arange(0, 17, 2) if parity == 0 else np.arange(2, 17, 2)
    wave = np.cos if parity == 0 else np.sin
    return wave(orders[:, None] * angle[None, :])


def build_tables():
    span = N + 1.0
    step = 1.0 / span
    radius = math.sqrt(3.0) / 2.0
    index = np.arange(N) + 1
    sine_rows = np.sin(np.pi * (index[:, None] * index[None, :] % (2 * N + 2)) / span)
    eigen = 4.0 * span * span * np.sin(np.pi * index / (2 * span)) ** 2
    scaled = 2.0 * (np.arange(N) - (N - 1) / 2.0) * step
    angle = np.arctan(scaled)

    terms = [[] for _ in range(8)]
    for l in range(ORDER + 1):
        for m in range(l + 1):
            terms[(m % 2) * 4 + (l - m) % 2].append((l, m, 0))
            if m:
                terms[((m - 1) % 2) * 4 + 2 + (l - m) % 2].append((l, m, 1))

    nodes, quad = np.polynomial.legendre.leggauss(24)
    legendre = np.polynomial.legendre.legvander(nodes, ORDER).T
    basis = np.zeros((N, 32))
    basis[:, : ORDER + 1] = sine_rows @ np.polynomial.legendre.legvander(scaled, ORDER)
    even = (np.arange(N) % 2 == 0).astype(np.float64)
    basis[:, 17] = sine_rows[0] * even
    basis[:, 18] = sine_rows[0] * (1.0 - even)
    project = legendre * quad[None, :] * (np.arange(ORDER + 1) + 0.5)[:, None]
    turns = 64
    circle = 2.0 * np.pi * np.arange(turns) / turns
    ones_t, ones_s = np.meshgrid(nodes, nodes, indexing="ij")
    alpha, beta = np.meshgrid(circle, circle, indexing="ij")
    solid, wave = [], []
    for face in range(3):
        x, y, z = face_point(face, ones_t, ones_s)
        r = np.sqrt(x * x + y * y + z * z)
        table = harmonics(x / r, y / r, z / r)
        solid.append((table, r / math.sqrt(3.0)))
        ca, sa, cb, sb = np.cos(alpha), np.sin(alpha), np.cos(beta), np.sin(beta)
        parts = (sa * cb, ca * sb, ca * cb)
        order = ((1, 0, 2), (1, 2, 0), (2, 0, 1))[face]
        x, y, z = (parts[k] for k in order)
        r = np.sqrt(x * x + y * y + z * z)
        safe = np.where(r < 1e-12, 1.0, r)
        wave.append((harmonics(x / safe, y / safe, z / safe), np.where(r < 1e-12, 0.0, r)))

    select = np.zeros((3, 32, LANES))
    gather = np.zeros((SLOTS, LANES))
    spread = np.zeros((SLOTS, 16, 256))
    columns = np.zeros((256, N))
    rows = np.zeros((8, 3, 16, N))
    spill = SPARE
    for group in range(8):
        px, py, pz = group >> 2 & 1, group >> 1 & 1, group & 1
        odd = (px + py + pz) % 2
        lane = group * 128
        for face in range(3):
            prow, pcol, normal = face_parity(face, px, py, pz)
            sign = 2.0 if normal == 0 else -2.0
            entries = [
                (i, j)
                for i in range(prow, ORDER + 1, 2)
                for j in range(pcol, ORDER + 1, 2)
                if i + j + normal <= ORDER - odd
            ]
            moments = {}
            for slot, (l, m, which) in enumerate(terms[group]):
                table, ratio = solid[face]
                values = ratio**l * table[which][l, m]
                moments[slot] = project @ values @ project.T
            for i, j in entries:
                if lane >= (group + 1) * 128 or (lane >= SPARE and group == 1):
                    position, spill = spill, spill + 1
                    assert group == 0
                else:
                    position, lane = lane, lane + 1
                axes = ((1, 0, 2), (2, 0, 1), (1, 2, 0))[face]
                select[axes[0], i, position] = 1.0
                select[axes[1], j, position] = 1.0
                select[axes[2], 17 + normal, position] = 1.0
                for slot in moments:
                    gather[slot, position] = step * sign * moments[slot][i, j]
            left = trig(prow, odd, circle)
            right = trig(pcol, odd, circle)
            left_unit = left / np.sum(left * left, axis=1, keepdims=True)
            right_unit = right / np.sum(right * right, axis=1, keepdims=True)
            base = group * 32 + face * 9
            for slot, (l, m, which) in enumerate(terms[group]):
                table, r = wave[face]
                values = r ** (ORDER - odd) * table[which][l, m]
                block = left_unit @ values @ right_unit.T
                weight = (1.0 if m == 0 else 2.0) / (4.0 * math.pi * radius * 1.1 ** (l + 1))
                block = block * weight * sign * span * span
                spread[slot, : block.shape[0], base : base + block.shape[1]] = block
            tail = trig(pcol, odd, angle)
            columns[base : base + tail.shape[0]] = tail
            head = trig(prow, odd, angle)
            rows[group, face, : head.shape[0]] = head
    assert spill <= 256
    root = 1.0 / np.sqrt(1.0 - np.outer(np.sin(angle) ** 2, np.sin(angle) ** 2))
    return sine_rows, eigen, basis, select, gather, spread, columns, rows, root, root**15

MESH = pl.DeviceIdType.MESH
SIDE = 16
WIDE = 24
EARLY = 1
UNROLL = 2
VMEM_LIMIT = 67043328 - 1024 * 1024
HALF = 128
F32 = jnp.float32
BF16 = jnp.bfloat16
NN = (((1,), (0,)), ((), ()))
NT = (((1,), (1,)), ((), ()))


def split(value):
    high = value.astype(BF16)
    return high, (value - high.astype(F32)).astype(BF16)


def dot(a, b, dims=NN):
    return lax.dot_general(a, b, dims, preferred_element_type=F32)


def dot3(a, b, dims=NN):
    return dot(a[0], b[0], dims) + (dot(a[0], b[1], dims) + dot(a[1], b[0], dims))


def regroup(load, store, roll):
    lane = lax.broadcasted_iota(jnp.int32, (4 * SIDE, HALF), 1)
    rows = [
        jnp.concatenate([load(8 * a + i, h) for a in range(2) for h in range(2)], axis=0)
        for i in range(8)
    ]
    for step in (4, 2, 1):
        keep = (lane // (SIDE * step)) % 2 == 0
        for i in range(8):
            if i & step == 0:
                one, two = rows[i], rows[i + step]
                rows[i] = jnp.where(keep, one, roll(two, SIDE * step))
                rows[i + step] = jnp.where(keep, roll(one, HALF - SIDE * step), two)
    for i in range(8):
        for a in range(2):
            for h in range(2):
                part = 2 * a + h
                store(8 * h + i, a, rows[i][part * SIDE : (part + 1) * SIDE])


def green_rows(sines, basis_rows):
    rows = [sines[x : x + 1, :] * basis_rows[:SIDE] for x in range(SIDE)]
    rows += [sines * basis_rows[f : f + 1] for f in range(SIDE, SIDE + 3)]
    return jnp.concatenate(rows, axis=0)


def weighted_rows(table, values):
    total = table[:SIDE] * values[0:1, :]
    for x in range(1, SIDE):
        total += table[x * SIDE : (x + 1) * SIDE] * values[x : x + 1, :]
    other = [
        jnp.sum(table[f * SIDE : (f + 1) * SIDE] * values, axis=0, keepdims=True)
        for f in range(SIDE, SIDE + 3)
    ]
    even = jnp.concatenate([total[:8], *other[:2], jnp.zeros((6, 256), F32)], axis=0)
    return even, jnp.concatenate([total[8:], other[2], jnp.zeros((7, 256), F32)], axis=0)


def local_entries(folded, expand_y, expand_z, select):
    pieces = [split(part) for part in folded]
    outcome = []
    for tile in range(4):
        lanes = slice(tile * 256, (tile + 1) * 256)
        mixed = dot3(pieces[tile // 2], (expand_y[0][:, lanes], expand_y[1][:, lanes]))
        total = mixed[:SIDE] * expand_z[0:1, lanes]
        for k in range(1, SIDE):
            total += mixed[k * SIDE : (k + 1) * SIDE] * expand_z[k : k + 1, lanes]
        start = SIDE * (tile // 2)
        chosen = select[tile][start : start + SIDE, :].astype(F32)
        summed = jnp.sum(total * chosen, axis=0, keepdims=True)
        outcome += [summed[:, :HALF], summed[:, HALF:]]
    return outcome


def owner_map():
    row = lax.broadcasted_iota(jnp.int32, (LANES, 256), 0)
    lane = lax.broadcasted_iota(jnp.int32, (LANES, 256), 1)
    owner = jnp.where((row >= SPARE) & (row < 256), 0, row // HALF)
    return jnp.where(owner == lane // 32, 1.0, 0.0).astype(BF16)


def surface_planes(entries, gather, spread, onehot, columns, heads, root, power):
    product = jnp.concatenate(
        [gather[r][...] * entries[r : r + 1, :] for r in range(8)], axis=1
    )
    high, rest = product.astype(BF16), None
    rest = product - high.astype(F32)
    middle = rest.astype(BF16)
    low = (rest - middle.astype(F32)).astype(BF16)
    moments = dot(jnp.concatenate([high, middle, low], axis=0), onehot)
    moments = moments[:SLOTS] + (moments[SLOTS : 2 * SLOTS] + moments[2 * SLOTS :])
    shape = moments[0:1, :] * spread[0][0:8, :]
    for slot in range(1, 45):
        shape += moments[slot : slot + 1, :] * spread[0][slot * 8 : slot * 8 + 8, :]
    ninth = jnp.sum(moments * spread[1][...], axis=0, keepdims=True)
    below = lax.broadcasted_iota(jnp.int32, (8, 256), 0) == 0
    shape = jnp.concatenate([shape, jnp.where(below, ninth, 0.0)], axis=0)
    lane = lax.broadcasted_iota(jnp.int32, (SIDE, 256), 1)
    blocks = []
    for face in range(3):
        for normal in range(2):
            for odd in range(2):
                for head in range(2):
                    tail = (odd + normal + head) % 2
                    px, py, pz = (
                        (tail, head, normal),
                        (tail, normal, head),
                        (normal, head, tail),
                    )[face]
                    base = (px * 4 + py * 2 + pz) * 32 + face * 9
                    blocks.append(jnp.where((lane >= base) & (lane < base + 9), shape, 0.0))
    right = dot3(split(jnp.concatenate(blocks, axis=0)), columns)
    planes = []
    for face in range(3):
        for normal in range(2):
            parts = []
            for odd in range(2):
                start = ((face * 2 + normal) * 2 + odd) * 32
                high, low = split(right[start : start + 32])
                stack = jnp.concatenate([high, low, high, low], axis=0)
                parts.append(dot(heads[odd][...], stack))
            planes.append(split(power * (root * parts[0] + parts[1])))
    return planes


def few_rows(rows, matrix, dims=NN):
    both = dot(jnp.concatenate(rows, axis=0), matrix[0], dims)
    return both[:SIDE] + (both[SIDE:] + dot(rows[0], matrix[1], dims))


def side_hats(planes, at_y, at_z, sines):
    half_y = split(jnp.concatenate([few_rows(at_z, planes[2 + n]) for n in range(2)], axis=0))
    hat_y = dot3(half_y, sines)
    half = [few_rows(at_z, planes[4 + n], NT) for n in range(2)]
    hat_x = dot3(split(jnp.concatenate(half, axis=0)), sines)
    near_x = [dot3(at_y, split(half[n]), NT) for n in range(2)]
    half_z = split(jnp.concatenate([few_rows(at_y, planes[n]) for n in range(2)], axis=0))
    return hat_y, hat_x, near_x, dot3(half_z, sines)


def corrected(shape, scale, hat_y, edge, hat_x, inverse, edge_green, at_x):
    even = lax.broadcasted_iota(jnp.int32, (256, 256), 0) % 2 == 0
    mixed = shape * scale + jnp.where(even, hat_y[0], hat_y[1]) * edge
    value = few_rows(at_x, split(mixed * inverse), NT)
    return value + hat_x[0] * edge_green[:SIDE] + hat_x[1] * edge_green[SIDE:]


def source_block(k, hat_z, hat_y, last, edge_y, edge_z, edge_lane):
    ky = lax.broadcasted_iota(jnp.int32, (SIDE, 256), 0)
    value = hat_z[(k % 2) * SIDE : (k % 2 + 1) * SIDE] * edge_z[k : k + 1, :]
    side = jnp.where(ky % 2 == 0, hat_y[k : k + 1, :], hat_y[SIDE + k : SIDE + k + 1, :])
    value += side * edge_y
    value += last[0][:, k : k + 1] * edge_lane[0] + last[1][:, k : k + 1] * edge_lane[1]
    return value


FAR = {
    "gx": (
        (4, 1), (3, 1), (5, 1), (4, 0), (2, 1), (6, 1), (3, 0), (5, 0), (1, 1), (7, 1), (2, 0),
        (6, 0), (0, 1), (1, 0), (7, 0),
    ),
    "gy": (
        (2, 3), (2, 2), (1, 3), (3, 3), (1, 2), (3, 2), (2, 1), (2, 0), (1, 1), (3, 1), (1, 0),
        (3, 0), (0, 3), (0, 2), (0, 1),
    ),
}


def peer_of(axis, me, step):
    if axis == "gx":
        return lax.rem(me // 8 + step[1], 2) * 8 + lax.rem(me % 8 + step[0], 8)
    cross = lax.rem(me % 4 // 2 + step[1] // 2, 2) * 2 + lax.rem(me % 2 + step[1] % 2, 2)
    return lax.rem(me // 4 + step[0], 4) * 4 + cross


def start_all(phase, source, target, axis, me, send_sem, recv_sem, rows):
    for step in FAR[axis]:
        peer = peer_of(axis, me, step)
        count = source.shape[0] if rows is None else rows
        src = source if rows is None else source.at[pl.ds(pl.multiple_of(peer * rows, rows), rows), :]
        pltpu.make_async_remote_copy(
            src_ref=src,
            dst_ref=target.at[pl.ds(pl.multiple_of(me * count, count), count), :],
            send_sem=send_sem.at[phase],
            recv_sem=recv_sem.at[phase],
            device_id={axis: peer},
            device_id_type=MESH,
        ).start()


def whole_of(phase, target, axis, me, send_sem, recv_sem):
    rows = target.shape[0] // SIDE * (SIDE - 1)
    return pltpu.make_async_remote_copy(
        src_ref=target.at[0:rows, :],
        dst_ref=target.at[0:rows, :],
        send_sem=send_sem.at[phase],
        recv_sem=recv_sem.at[phase],
        device_id={axis: lax.rem(me + 1, SIDE)},
        device_id_type=MESH,
    )


def sum_slots(ref):
    total = ref[0:8, :]
    for slot in range(1, SIDE):
        total += ref[slot * 8 : (slot + 1) * 8, :]
    return total


def unpack(plain, narrow, cut):
    return dict(
        eigen_wide=cut(plain, 0, 256, 0, 128),
        edge_wide=cut(plain, 0, 256, 128, 256),
        lane_rows=cut(plain, 256, 264, 0, 256),
        basis_rows=cut(plain, 264, 288, 0, 256),
        gather=[
            cut(plain, 288 + SLOTS * (r // 2), 288 + SLOTS * (r // 2 + 1), r % 2 * 128, r % 2 * 128 + 128)
            for r in range(8)
        ],
        spread=(cut(plain, 480, 864, 0, 256), cut(plain, 864, 912, 0, 256)),
        root=cut(plain, 912, 1168, 0, 256),
        sine_high=cut(narrow, 0, 256, 0, 256),
        sine_low=cut(narrow, 256, 512, 0, 256),
        basis_high=cut(narrow, 512, 768, 0, 128),
        basis_low=cut(narrow, 512, 768, 128, 256),
        select=[cut(narrow, 768 + 96 * t, 864 + 96 * t, 0, 256) for t in range(4)],
        column_high=cut(narrow, 1152, 1408, 0, 256),
        column_low=cut(narrow, 1408, 1664, 0, 256),
        heads=[cut(narrow, 1664, 1920, 128 * odd, 128 * odd + 128) for odd in range(2)],
    )


def kernel(charge_hbm, plain_hbm, narrow_hbm, out_ref, energy_ref, *scratch):
    charge, plain, narrow = scratch[:3]
    sends = scratch[3:7]
    lands = scratch[7:11]
    (
        mats, field_ref, inverse, shape_z, expand_high, expand_low, expand_z, pair_sum, half_rows,
        green, folded, hats, extra, power, own, onehot, small_send, small_land, local_sem,
        send_sem, recv_sem,
    ) = scratch[11:]
    table = unpack(plain, narrow, lambda ref, a, b, c, d: ref.at[a:b, c:d])
    eigen_wide, edge_wide, lane_rows = table["eigen_wide"], table["edge_wide"], table["lane_rows"]
    sine_high, sine_low, select = table["sine_high"], table["sine_low"], table["select"]
    p = lax.axis_index("gx")
    q = lax.axis_index("gy")

    pieces = (
        (charge_hbm, charge),
        (narrow_hbm.at[0:512, :], narrow.at[0:512, :]),
        (narrow_hbm.at[512:1920, :], narrow.at[512:1920, :]),
        (plain_hbm, plain),
    )
    copies = [
        pltpu.make_async_copy(source, target, local_sem.at[i])
        for i, (source, target) in enumerate(pieces)
    ]
    for copy in copies:
        copy.start()

    barrier = pltpu.get_barrier_semaphore()

    for axis, me in (("gx", p), ("gy", q)):
        for step in FAR[axis]:
            pl.semaphore_signal(
                barrier, inc=1, device_id={axis: peer_of(axis, me, step)}, device_id_type=MESH
            )

    def at(index):
        return pl.ds(pl.multiple_of(index * SIDE, SIDE), SIDE)

    def sines():
        return sine_high[...], sine_low[...]

    def launch(phase, value, axis, me, ready=None):
        sends[phase][...] = dot3(sines(), split(value), NT)
        if ready is not None:
            ready()
        start_all(phase, sends[phase], lands[phase], axis, me, send_sem, recv_sem, SIDE)
        lands[phase][at(me), :] = sends[phase][at(me), :]

    def collect(phase, axis, me, strided, added=None):
        whole_of(phase, lands[phase], axis, me, send_sem, recv_sem).wait_recv()
        land = lands[phase]

        def load(a, h):
            return land[a * SIDE : (a + 1) * SIDE, h * HALF : (h + 1) * HALF]

        def store(g, h, piece):
            if added is not None:
                piece += added[g * SIDE : (g + 1) * SIDE, h * HALF : (h + 1) * HALF]
            if strided:
                mats[h][pl.ds(g, SIDE, stride=SIDE), :] = piece
            else:
                mats[h][g * SIDE : (g + 1) * SIDE, :] = piece

        regroup(load, store, lambda v, amount: pltpu.roll(v, amount, 1))

    def mat():
        return jnp.concatenate([mats[0][...], mats[1][...]], axis=1)

    def small(phase, index, value, axis, me):
        small_send[index][...] = value
        start_all(phase, small_send[index], small_land[index], axis, me, send_sem, recv_sem, None)
        small_land[index][pl.ds(pl.multiple_of(me * 8, 8), 8), :] = value

    def small_total(phase, index, axis, me):
        whole_of(phase, small_land[index], axis, me, send_sem, recv_sem).wait_recv()
        return sum_slots(small_land[index])

    cube = ((N + 1) / 2.0) ** 3

    def lead_rows():
        near = sine_high[at(p), :].astype(F32) + sine_low[at(p), :].astype(F32)
        return split(green_rows(near, table["basis_rows"][...]))

    def fill(k, lead):
        whole = 1.0 / ((pair_sum[...] + own[pl.ds(k, 1), :]) * cube)
        inverse[k] = whole
        green[k] = dot3(lead, split(whole))
        return lead

    def prepare():
        copies[2].wait()
        copies[3].wait()
        for tile in range(4):
            lanes = slice(tile * 256, (tile + 1) * 256)
            chosen = select[tile]
            basis = (table["basis_high"][...][:, :32], table["basis_low"][...][:, :32])
            expand_high[:, lanes] = dot(basis[0], chosen[32:64, :]).astype(BF16)
            expand_low[:, lanes] = dot(basis[1], chosen[32:64, :]).astype(BF16)
            near = (table["basis_high"][at(q), :][:, :32], table["basis_low"][at(q), :][:, :32])
            expand_z[:, lanes] = dot(near[0], chosen[64:96, :]) + dot(near[1], chosen[64:96, :])
        for half in range(2):
            lanes = slice(half * HALF, (half + 1) * HALF)
            own[0:SIDE, lanes] = eigen_wide[at(q), :]
            own[SIDE : 2 * SIDE, lanes] = edge_wide[at(q), :]
        pair_sum[:, :HALF] = eigen_wide[...] + lane_rows[0:1, :HALF]
        pair_sum[:, HALF:] = eigen_wide[...] + lane_rows[0:1, HALF:]
        lax.fori_loop(0, EARLY, fill, lead_rows())
        pl.semaphore_wait(barrier, 2 * (SIDE - 1))

    def drain_big(phase, axis, me):
        whole_of(phase, lands[phase], axis, me, send_sem, recv_sem).wait_send()

    def drain_small(phase, index, axis, me):
        whole_of(phase, small_land[index], axis, me, send_sem, recv_sem).wait_send()

    copies[0].wait()
    copies[1].wait()
    launch(0, charge[...], "gy", q, prepare)
    lax.fori_loop(EARLY, SIDE, fill, lead_rows())

    collect(0, "gy", q, True)
    launch(1, mat(), "gx", p)
    half_rows[...] = dot3(split(mat()), sines())

    def fold(k, carry):
        folded[0, at(k), :], folded[1, at(k), :] = weighted_rows(green[k], half_rows[at(k), :])
        return carry

    lax.fori_loop(0, SIDE, fold, 0)
    entries = local_entries((folded[0], folded[1]), (expand_high, expand_low), expand_z, select)
    small(4, 0, jnp.concatenate(entries, axis=0), "gy", q)
    onehot[...] = owner_map()
    root = table["root"][...]
    square = root * root
    fourth = square * square
    power[...] = fourth * fourth * (fourth * (square * root))
    drain_big(0, "gy", q)
    small(5, 1, small_total(4, 0, "gy", q), "gx", p)

    collect(1, "gx", p, False)
    value = dot3(split(mat()), sines())
    field = value * jnp.concatenate([inverse[k, at(p), :] for k in range(SIDE)], axis=0)
    field_ref[...] = field
    launch(2, field, "gx", p)
    energy = jnp.sum(jnp.sum(value * field, axis=1, keepdims=True), axis=0, keepdims=True)
    entries = small_total(5, 1, "gx", p)

    at_x = at_y = (sine_high[at(p), :], sine_low[at(p), :])
    at_z = (sine_high[at(q), :], sine_low[at(q), :])
    planes = surface_planes(
        entries, table["gather"], table["spread"], onehot[...],
        (table["column_high"][...], table["column_low"][...]), table["heads"],
        table["root"][...], power[...],
    )
    hat_y, hat_x, near_x, near_z = side_hats(planes, at_y, at_z, sines())
    edge_y = edge_wide[at(p), :]
    edge_y = jnp.concatenate([edge_y, edge_y], axis=1)
    edge_z = own[SIDE : 2 * SIDE, :]
    edge_lane = (lane_rows[1:2, :], lane_rows[2:3, :])
    cross = jnp.zeros((SIDE, 256), F32)
    for k in range(SIDE):
        cross += field_ref[k * SIDE : (k + 1) * SIDE, :] * source_block(
            k, near_z, hat_y, near_x, edge_y, edge_z, edge_lane
        )
    second = energy + jnp.sum(jnp.sum(cross, axis=1, keepdims=True), axis=0, keepdims=True)
    lane = lax.broadcasted_iota(jnp.int32, (8, HALF), 1)
    small(6, 2, jnp.where(lane == 0, energy, second), "gx", p)

    for n in range(2):
        shape_z[n] = dot3(split(dot3(sines(), planes[n])), sines())
    hats[0] = hat_y
    hats[1] = hat_x
    edge = jnp.concatenate([edge_wide[...], edge_wide[...]], axis=1)

    def correct(k, carry):
        extra[at(k), :] = corrected(
            shape_z[lax.rem(k, 2)],
            own[pl.ds(SIDE + k, 1), :],
            (hats[0, pl.ds(k, 1), :], hats[0, pl.ds(SIDE + k, 1), :]),
            edge,
            (hats[1, pl.ds(k, 1), :], hats[1, pl.ds(SIDE + k, 1), :]),
            inverse[k],
            green[k, 17 * SIDE :, :],
            at_x,
        )
        return carry

    lax.fori_loop(0, SIDE, correct, 0, unroll=UNROLL)
    collect(2, "gx", p, True, extra)
    launch(3, mat(), "gy", q)
    drain_big(1, "gx", p)
    drain_big(2, "gx", p)
    drain_small(4, 0, "gy", q)
    drain_small(5, 1, "gx", p)
    small(7, 3, small_total(6, 2, "gx", p), "gy", q)
    drain_small(6, 2, "gx", p)
    collect(3, "gy", q, False)
    out_ref[...] = dot3(split(mat()), sines())
    drain_big(3, "gy", q)
    energy_ref[...] = small_total(7, 3, "gy", q) * (1.0 / (N + 1)) ** 3
    drain_small(7, 3, "gy", q)


def constants():
    sine_rows, eigen, basis, select, gather, spread, columns, rows, root, power = build_tables()

    def pair(table):
        table = table.astype(np.float32)
        high = table.astype(jnp.bfloat16)
        return high, (table - high.astype(np.float32)).astype(jnp.bfloat16)

    parity = np.arange(N) % 2
    lane_rows = np.zeros((8, N))
    lane_rows[0] = eigen
    lane_rows[1] = sine_rows[0] * (parity == 0)
    lane_rows[2] = sine_rows[0] * (parity == 1)
    lane_rows[3] = sine_rows[0]
    heads = []
    for odd in range(2):
        tables = [trig(parity_of, odd, np.arctan(2.0 * (np.arange(N) - (N - 1) / 2.0) / (N + 1))) for parity_of in range(2)]
        wide = np.zeros((N, 32))
        for k, table in enumerate(tables):
            wide[:, 16 * k : 16 * k + table.shape[0]] = table.T
        high, low = pair(wide)
        heads.append(np.concatenate([high, high, low, low], axis=1))
    plain = np.concatenate(
        [
            np.concatenate([np.repeat(v[:, None], HALF, 1) for v in (eigen, sine_rows[0])], axis=1),
            lane_rows,
            basis.T[[*range(0, 16, 2), *range(1, 16, 2), *range(16, WIDE)]],
            *[gather[:, 256 * t : 256 * (t + 1)] for t in range(4)],
            spread[:, :8].reshape(8 * SLOTS, 256),
            spread[:, 8],
            root,
        ],
        axis=0,
    ).astype(np.float32)
    wide = np.zeros((N, HALF - 32))
    chosen = np.zeros_like(select[0])
    chosen[[*range(10), *range(16, 25)]] = select[0][[*range(0, 17, 2), 17, *range(1, 16, 2), 18]]
    select[0] = chosen
    high, low = pair(basis)
    narrow = np.concatenate(
        [
            *pair(sine_rows),
            np.concatenate([high, wide.astype(high.dtype), low, wide.astype(high.dtype)], axis=1),
            *[
                np.concatenate(list(select), axis=0)[:, 256 * t : 256 * (t + 1)].astype(jnp.bfloat16)
                for t in range(4)
            ],
            *pair(columns),
            np.concatenate(heads, axis=1),
        ],
        axis=0,
    )
    return plain, narrow


def solution(mesh):
    tables = constants()

    def shards(charge_density):
        cells_a, cells_b, length = charge_density.shape
        flat = charge_density.reshape(cells_a * cells_b, length)
        grid = pltpu.VMEM((256, 256), F32)
        potential, energies = pl.pallas_call(
            kernel,
            out_shape=(
                pltpu.VMEM((256, 256), F32),
                pltpu.VMEM((8, HALF), F32),
            ),
            in_specs=[pl.BlockSpec(memory_space=pl.ANY)] * 3,
            out_specs=(
                pl.BlockSpec(memory_space=pltpu.VMEM),
                pl.BlockSpec(memory_space=pltpu.VMEM),
            ),
            scratch_shapes=[
                grid,
                *[pltpu.VMEM(table.shape, table.dtype) for table in tables],
                *[grid] * 8,
                [pltpu.VMEM((256, HALF), F32)] * 2,
                grid,
                pltpu.VMEM((SIDE, 256, 256), F32),
                pltpu.VMEM((2, 256, 256), F32),
                pltpu.VMEM((256, LANES), BF16),
                pltpu.VMEM((256, LANES), BF16),
                pltpu.VMEM((SIDE, LANES), F32),
                grid,
                grid,
                pltpu.VMEM((SIDE, 19 * SIDE, 256), F32),
                pltpu.VMEM((2, 256, 256), F32),
                pltpu.VMEM((2, 2 * SIDE, 256), F32),
                grid,
                grid,
                pltpu.VMEM((2 * SIDE, 256), F32),
                pltpu.VMEM((LANES, 256), BF16),
                [pltpu.VMEM((8, HALF), F32)] * 4,
                [pltpu.VMEM((8 * SIDE, HALF), F32)] * 4,
                pltpu.SemaphoreType.DMA((4,)),
                pltpu.SemaphoreType.DMA((8,)),
                pltpu.SemaphoreType.DMA((8,)),
            ],
            compiler_params=pltpu.CompilerParams(
                collective_id=0, has_side_effects=True, vmem_limit_bytes=VMEM_LIMIT
            ),
        )(flat, *[jnp.asarray(table) for table in tables])
        return potential.reshape(cells_a, cells_b, length), energies[0, :2]

    return jax.shard_map(
        shards,
        mesh=mesh,
        in_specs=(P("gx", "gy", None),),
        out_specs=(P("gx", "gy", None), P()),
        check_vma=False,
    )
```
